32 devices in a mesh: dp: 1 (over z), tp: 4 (over y), ep: 8 (over x, core).
Axes of the slice: x: 4, y: 4, z: 1, core: 2. Of those that a mesh axis runs over, the one named last changes fastest.
The devices are a block of a 4x4x8 slice.
Arguments:
- hidden_in: bfloat16 [1024, 2048], P(('dp', 'ep'))
- topk_idx: int32 [1024, 6], P(('dp', 'ep'))
- norm_gain: bfloat16 [2048], replicated
- router_w: bfloat16 [2048, 64], replicated
- shared_sig_w: bfloat16 [2048, 1], replicated
- exp_gate: bfloat16 [64, 2048, 1408], P('ep', None, 'tp')
- exp_up: bfloat16 [64, 2048, 1408], P('ep', None, 'tp')
- exp_down: bfloat16 [64, 1408, 2048], P('ep', 'tp')
- sh_gate: bfloat16 [2048, 2816], P(None, ('tp', 'ep'))
- sh_up: bfloat16 [2048, 2816], P(None, ('tp', 'ep'))
- sh_down: bfloat16 [2816, 2048], P(('tp', 'ep'))
Outputs:
- output: bfloat16 [1024, 2048], P(('dp', 'ep'))
All inputs are finite; a program needn't handle non-finite values.
Results may differ from the reference program's by a relative error of at most 0.0123824.
Values are sent between devices in bfloat16 or wider.
A program may use at most 768 MiB of HBM per device.

```python
import jax
import jax.numpy as jnp
from jax import lax

HIDDEN = 2048
EXPERTS = 64
TOP_K = 6
EXPERT_WIDTH = 1408
SHARED_WIDTH = 2816
TOKENS = 1024
ROW_BLOCK = 128
RMS_EPS = 1e-6


def setup_inputs(seed: int = 0, part: int = 0) -> dict:
    weight_keys = jax.random.split(jax.random.key(seed), 9)
    part_keys = jax.random.split(jax.random.fold_in(jax.random.key(seed + 1), part), 3)
    hidden_in = jax.random.normal(part_keys[0], (TOKENS, HIDDEN), jnp.float32)
    hot_bias = jax.random.randint(part_keys[1], (EXPERTS,), 0, 3) * 400
    noise_score = jax.random.randint(part_keys[2], (TOKENS, EXPERTS), 0, 1000)
    ranked = (noise_score + hot_bias[None, :]) * EXPERTS + jnp.arange(EXPERTS)[None, :]
    topk_idx = lax.top_k(ranked, TOP_K)[1].astype(jnp.int32)
    in_scale = HIDDEN ** -0.5
    down_scale = 0.7 * EXPERTS * TOP_K ** -0.5 * EXPERT_WIDTH ** -0.5
    shared_scale = 2.0 * SHARED_WIDTH ** -0.5
    norm_gain = jax.random.uniform(weight_keys[0], (HIDDEN,), jnp.float32, 0.5, 1.5)
    router_w = jax.random.normal(weight_keys[1], (HIDDEN, EXPERTS), jnp.float32) * in_scale
    shared_sig_w = jax.random.normal(weight_keys[2], (HIDDEN, 1), jnp.float32) * in_scale
    exp_gate = jax.random.normal(weight_keys[3], (EXPERTS, HIDDEN, EXPERT_WIDTH), jnp.float32) * in_scale
    exp_up = jax.random.normal(weight_keys[4], (EXPERTS, HIDDEN, EXPERT_WIDTH), jnp.float32) * in_scale
    exp_down = jax.random.normal(weight_keys[5], (EXPERTS, EXPERT_WIDTH, HIDDEN), jnp.float32) * down_scale
    sh_gate = jax.random.normal(weight_keys[6], (HIDDEN, SHARED_WIDTH), jnp.float32) * in_scale
    sh_up = jax.random.normal(weight_keys[7], (HIDDEN, SHARED_WIDTH), jnp.float32) * in_scale
    sh_down = jax.random.normal(weight_keys[8], (SHARED_WIDTH, HIDDEN), jnp.float32) * shared_scale
    return {
        'hidden_in': hidden_in.astype(jnp.bfloat16),
        'topk_idx': topk_idx,
        'norm_gain': norm_gain.astype(jnp.bfloat16),
        'router_w': router_w.astype(jnp.bfloat16),
        'shared_sig_w': shared_sig_w.astype(jnp.bfloat16),
        'exp_gate': exp_gate.astype(jnp.bfloat16),
        'exp_up': exp_up.astype(jnp.bfloat16),
        'exp_down': exp_down.astype(jnp.bfloat16),
        'sh_gate': sh_gate.astype(jnp.bfloat16),
        'sh_up': sh_up.astype(jnp.bfloat16),
        'sh_down': sh_down.astype(jnp.bfloat16),
    }


def rms_norm(rows, gain):
    rows_f32 = rows.astype(jnp.float32)
    inv_rms = lax.rsqrt(jnp.mean(rows_f32 * rows_f32, axis=-1, keepdims=True) + RMS_EPS)
    return (rows_f32 * inv_rms * gain.astype(jnp.float32)).astype(jnp.bfloat16)


def routed_sum(normed, topk_idx, chosen_wt, exp_gate, exp_up, exp_down):
    n_tok, n_top = topk_idx.shape
    n_rows = n_tok * n_top
    block_rows = min(ROW_BLOCK, n_rows)
    flat_exp = topk_idx.reshape(-1)
    order = jnp.argsort(flat_exp, stable=True)
    row_tok = order // n_top
    row_wt = chosen_wt.reshape(-1)[order]
    counts = jax.ops.segment_sum(jnp.ones_like(flat_exp), flat_exp, num_segments=EXPERTS)
    starts = jnp.cumsum(counts) - counts

    def per_expert(running, expert_xs):
        w_gate, w_up, w_down, first, count = expert_xs

        def body(step, acc_in):
            row_start = first + step * block_rows
            begin = jnp.minimum(row_start, n_rows - block_rows)
            positions = begin + jnp.arange(block_rows)
            keep = (positions >= row_start) & (positions < first + count)
            tok_ids = lax.dynamic_slice(row_tok, (begin,), (block_rows,))
            row_wts = jnp.where(keep, lax.dynamic_slice(row_wt, (begin,), (block_rows,)), 0.0)
            rows = normed[tok_ids]
            gate_val = jnp.dot(rows, w_gate, preferred_element_type=jnp.float32)
            up_val = jnp.dot(rows, w_up, preferred_element_type=jnp.float32)
            act_val = (jax.nn.silu(gate_val) * up_val).astype(jnp.bfloat16)
            down_val = jnp.dot(act_val, w_down, preferred_element_type=jnp.float32)
            return acc_in.at[tok_ids].add(down_val * row_wts[:, None])

        n_steps = (count + block_rows - 1) // block_rows
        return lax.fori_loop(0, n_steps, body, running), None

    zeros_init = jnp.zeros((n_tok, HIDDEN), jnp.float32)
    total, _ = lax.scan(per_expert, zeros_init, (exp_gate, exp_up, exp_down, starts, counts))
    return total


def reference(hidden_in, topk_idx, norm_gain, router_w, shared_sig_w, exp_gate, exp_up, exp_down, sh_gate, sh_up, sh_down):
    normed = rms_norm(hidden_in, norm_gain)
    router_prob = jax.nn.softmax(jnp.dot(normed, router_w, preferred_element_type=jnp.float32), axis=-1)
    chosen_wt = jnp.take_along_axis(router_prob, topk_idx, axis=1)
    routed = routed_sum(normed, topk_idx, chosen_wt, exp_gate, exp_up, exp_down)
    sig_gate = jax.nn.sigmoid(jnp.dot(normed, shared_sig_w, preferred_element_type=jnp.float32))
    sh_act = (jax.nn.silu(jnp.dot(normed, sh_gate, preferred_element_type=jnp.float32)) * jnp.dot(normed, sh_up, preferred_element_type=jnp.float32)).astype(jnp.bfloat16)
    shared = sig_gate * jnp.dot(sh_act, sh_down, preferred_element_type=jnp.float32)
    return (hidden_in.astype(jnp.float32) + routed + shared).astype(jnp.bfloat16)
```

```python
import functools

import jax
import jax.numpy as jnp
from jax import lax
from jax.experimental import pallas as pl
from jax.experimental.pallas import tpu as pltpu
from jax.sharding import PartitionSpec as P

RMS_EPS = 1e-6
LANES = 128
PITCH = 24
TILES = (64, 256, 320, 384, 512)
SLOTS = 3
F32 = jnp.float32
BF16 = jnp.bfloat16


def router_columns(rw_ref, sig_ref, out_ref):
    n_exp = rw_ref.shape[1]
    out_ref[...] = jnp.zeros_like(out_ref)
    out_ref[:, :n_exp] = rw_ref[...]
    lane = lax.broadcasted_iota(jnp.int32, (256, LANES), 1)

    def put(step, carry):
        rows = pl.ds(pl.multiple_of(step * 256, 256), 256)
        sig = sig_ref[rows, :].astype(F32)
        out_ref[rows, :] = jnp.where(lane == n_exp, sig, out_ref[rows, :].astype(F32)).astype(BF16)
        return carry

    lax.fori_loop(0, out_ref.shape[0] // 256, put, 0)


def token_block(x, gain, rcol_ref, shg_ref, shu_ref, n_exp):
    xf = x.astype(F32)
    inv = lax.rsqrt(jnp.mean(xf * xf, axis=-1, keepdims=True) + RMS_EPS)
    h = (xf * inv * gain.astype(F32)).astype(BF16)
    logits = jnp.dot(h, rcol_ref[...], preferred_element_type=F32)
    lane = lax.broadcasted_iota(jnp.int32, logits.shape, 1)
    masked = jnp.where(lane < n_exp, logits, -jnp.inf)
    top = jnp.max(masked, axis=-1, keepdims=True)
    ex = jnp.exp(masked - top)
    prob = ex / jnp.sum(ex, axis=-1, keepdims=True)
    sig = jax.nn.sigmoid(logits[:, n_exp:n_exp + 1])
    gate = jnp.dot(h, shg_ref[...], preferred_element_type=F32)
    up = jnp.dot(h, shu_ref[...], preferred_element_type=F32)
    act = (jax.nn.silu(gate) * up).astype(BF16)
    return h, prob.T, sig, act


def routing_lists(idx_t, wt, first, n_local, lst_ref, wl_ref, cnt_ref):
    n_tok = idx_t.shape[1]
    n_hi = n_tok // LANES
    sub = lax.broadcasted_iota(jnp.int32, (n_local, n_tok), 0)
    member = jnp.zeros((n_local, n_tok), F32)
    for e in range(n_local):
        hit = jnp.sum((idx_t == first + e).astype(F32), axis=0, keepdims=True)
        member = jnp.where(sub == e, hit, member)
    tri = (lax.broadcasted_iota(jnp.int32, (LANES, LANES), 0)
           < lax.broadcasted_iota(jnp.int32, (LANES, LANES), 1)).astype(BF16)
    base = jnp.zeros((n_local, 1), F32)
    parts = []
    for b in range(n_hi):
        m_b = member[:, b * LANES:(b + 1) * LANES]
        parts.append(jnp.dot(m_b.astype(BF16), tri, preferred_element_type=F32) + base)
        base = base + jnp.sum(m_b, axis=-1, keepdims=True)
    pos = jnp.concatenate(parts, axis=1).astype(jnp.int32)
    cnt_ref[...] = jnp.broadcast_to(base, cnt_ref.shape).astype(jnp.int32)
    tok = lax.broadcasted_iota(jnp.int32, (n_hi, n_tok), 1)
    hi_id = lax.broadcasted_iota(jnp.int32, (n_hi, n_tok), 0)
    lo_id = lax.broadcasted_iota(jnp.int32, (LANES, n_tok), 0)
    row_id = (lax.broadcasted_iota(jnp.int32, (n_hi, LANES), 0) * LANES
              + lax.broadcasted_iota(jnp.int32, (n_hi, LANES), 1))
    tok_hi = (tok // 8).astype(F32)
    tok_lo = (tok % 8).astype(F32)
    for e in range(n_local):
        p_e = pos[e:e + 1, :]
        here = ((p_e // LANES) == hi_id) & (member[e:e + 1, :] > 0.0)
        lo_hot = jnp.where((p_e % LANES) == lo_id, 1.0, 0.0).astype(BF16)
        w = wt[e:e + 1, :]
        w1 = w.astype(BF16).astype(F32)
        w2 = (w - w1).astype(BF16).astype(F32)
        w3 = w - w1 - w2
        rows = [jnp.where(here, v, 0.0) for v in (tok_hi, tok_lo, w1, w2, w3)]
        lhs = jnp.concatenate(rows, axis=0).astype(BF16)
        got = lax.dot_general(lhs, lo_hot, (((1,), (1,)), ((), ())), preferred_element_type=F32)
        t_of = got[:n_hi] * 8.0 + got[n_hi:2 * n_hi]
        w_of = (got[2 * n_hi:3 * n_hi] + got[3 * n_hi:4 * n_hi]) + got[4 * n_hi:]
        valid = row_id < base[e:e + 1, :].astype(jnp.int32)
        lst_ref[e * n_hi:(e + 1) * n_hi, :] = jnp.where(valid, t_of.astype(jnp.int32), n_tok)
        wl_ref[e * n_hi:(e + 1) * n_hi, :] = jnp.where(valid, w_of, 0.0)


def prep_kernel(n_local, x_ref, idx_ref, gain_ref, rw_ref, sig_ref, shg_ref, shu_ref,
                h_ref, act_ref, sigv_ref, lst_ref, wl_ref, cnt_ref, rcol, probs):
    n_exp = rw_ref.shape[1]
    router_columns(rw_ref, sig_ref, rcol)
    n_blocks = x_ref.shape[0] // LANES

    def block(b, carry):
        rows = pl.ds(pl.multiple_of(b * LANES, LANES), LANES)
        h, prob_t, sig, act = token_block(x_ref[rows, :], gain_ref[...], rcol, shg_ref, shu_ref, n_exp)
        h_ref[rows, :] = h
        probs[b] = prob_t
        sigv_ref[rows, :] = sig
        act_ref[rows, :] = act
        return carry

    lax.fori_loop(0, n_blocks, block, 0)
    first = pl.multiple_of(lax.axis_index("ep") * n_local, n_local)
    wt = jnp.concatenate([probs[b, pl.ds(first, n_local), :] for b in range(n_blocks)], axis=1)
    routing_lists(idx_ref[...], wt, first, n_local, lst_ref, wl_ref, cnt_ref)


def expert_kernel(lst, wl, cnt, h_hbm, act_ref, sig_ref, shd_ref, wg_hbm, wu_hbm, wd_hbm, out_hbm,
                  h_in, table, acc, wg, wu, wd, xt, xb, fb, ob, active, in_sem, w_sem, out_sem):
    n_tok, dim = h_hbm.shape
    n_local = wg_hbm.shape[0]
    n_chunk = dim // LANES
    n_blocks = n_tok // LANES

    def fetch_h(b):
        return pltpu.make_async_copy(h_hbm.at[pl.ds(b * LANES, LANES), :], h_in.at[b], in_sem.at[b])

    def weight_copies(e, s):
        return (pltpu.make_async_copy(wg_hbm.at[e], wg.at[s], w_sem.at[s, 0]),
                pltpu.make_async_copy(wu_hbm.at[e], wu.at[s], w_sem.at[s, 1]),
                pltpu.make_async_copy(wd_hbm.at[e], wd.at[s], w_sem.at[s, 2]))

    for b in range(n_blocks):
        fetch_h(b).start()

    def note(e, n):
        has = cnt[e, 0] > 0

        @pl.when(has)
        def _():
            active[n] = e

        return n + jnp.where(has, 1, 0)

    n_active = lax.fori_loop(0, n_local, note, 0)
    for s in range(SLOTS - 1):
        @pl.when(s < n_active)
        def _():
            for c in weight_copies(active[s], s):
                c.start()

    def clear(i, carry):
        acc[pl.ds(pl.multiple_of(i * 128, 128), 128), :] = jnp.zeros((128, LANES), F32)
        return carry

    lax.fori_loop(0, (n_tok * PITCH) // 128, clear, 0)
    acc[n_tok * PITCH:, :] = jnp.zeros((acc.shape[0] - n_tok * PITCH, LANES), F32)
    table[n_tok * PITCH:, :] = jnp.zeros((table.shape[0] - n_tok * PITCH, LANES), F32)

    def spread(b, carry):
        fetch_h(b).wait()
        for c in range(n_chunk):
            table[pl.ds(b * LANES * PITCH + c, LANES, stride=PITCH), :] = (
                h_in[b, :, c * LANES:(c + 1) * LANES].astype(F32))
        return carry

    lax.fori_loop(0, n_blocks, spread, 0)

    def rows_of(e, r):
        return lst[e * n_blocks + r // LANES, r % LANES]

    def ffn(m, e, s, r0, n):
        stride = m + 8
        groups = (n + 7) // 8

        def gather(g, carry):
            for i in range(8):
                r = g * 8 + i
                t = rows_of(e, r0 + r)
                slab = table[pl.ds(pl.multiple_of(t * PITCH, 8), n_chunk), :]
                xt[pl.ds(r, n_chunk, stride=stride), :] = slab
            return carry

        lax.fori_loop(0, groups, gather, 0)
        for c in range(n_chunk):
            xb[:m, c * LANES:(c + 1) * LANES] = xt[c * stride:c * stride + m, :].astype(BF16)
        gate = jnp.dot(xb[:m, :], wg[s], preferred_element_type=F32)
        up = jnp.dot(xb[:m, :], wu[s], preferred_element_type=F32)
        act = (jax.nn.silu(gate) * up).astype(BF16)
        for c in range(0, n_chunk, 2):
            f = jnp.dot(act, wd[s, :, c * LANES:(c + 2) * LANES], preferred_element_type=F32)
            fb[c * stride:c * stride + m, :] = f[:, :LANES]
            fb[(c + 1) * stride:(c + 1) * stride + m, :] = f[:, LANES:]

        def scatter(g, carry):
            where, old, new = [], [], []
            for i in range(8):
                r = g * 8 + i
                t = rows_of(e, r0 + r)
                where.append(pl.multiple_of(t * PITCH, 8))
                old.append(acc[pl.ds(where[i], n_chunk), :])
            for i in range(8):
                r = g * 8 + i
                w = wl[e * n_blocks + (r0 + r) // LANES, (r0 + r) % LANES]
                new.append(old[i] + w * fb[pl.ds(r, n_chunk, stride=stride), :])
            for i in range(8):
                acc[pl.ds(where[i], n_chunk), :] = new[i]
            return carry

        lax.fori_loop(0, groups, scatter, 0)

    big = TILES[-1]

    def expert(i, carry):
        e = active[i]
        s = lax.rem(i, SLOTS)
        ahead = i + SLOTS - 1

        @pl.when(ahead < n_active)
        def _():
            for c in weight_copies(active[ahead], lax.rem(ahead, SLOTS)):
                c.start()

        for c in weight_copies(e, s):
            c.wait()
        total = cnt[e, 0]

        def piece(j, carry2):
            r0 = j * big
            n = jnp.minimum(total - r0, big)
            below = 0
            for m in TILES:
                @pl.when((n > below) & (n <= m))
                def _(m=m):
                    ffn(m, e, s, r0, n)
                below = m
            return carry2

        lax.fori_loop(0, (total + big - 1) // big, piece, 0)
        return carry

    lax.fori_loop(0, n_active, expert, 0)

    def write_out(b, slot):
        return pltpu.make_async_copy(ob.at[slot], out_hbm.at[pl.ds(b * LANES, LANES), :], out_sem.at[slot])

    def finish(b, carry):
        slot = lax.rem(b, 2)

        @pl.when(b >= 2)
        def _():
            write_out(b - 2, slot).wait()

        rows = pl.ds(pl.multiple_of(b * LANES, LANES), LANES)
        sig = sig_ref[rows, :]
        for c in range(0, n_chunk, 2):
            sh = sig * jnp.dot(act_ref[rows, :], shd_ref[:, c * LANES:(c + 2) * LANES], preferred_element_type=F32)
            for d in range(2):
                routed = acc[pl.ds(b * LANES * PITCH + c + d, LANES, stride=PITCH), :]
                ob[slot, :, (c + d) * LANES:(c + d + 1) * LANES] = (
                    routed + sh[:, d * LANES:(d + 1) * LANES]).astype(BF16)
        write_out(b, slot).start()
        return carry

    lax.fori_loop(0, n_blocks, finish, 0)
    for b in (n_blocks - 2, n_blocks - 1):
        write_out(b, b % 2).wait()


def run_experts(lst, wl, cnt, h, act, sig, shd, wg, wu, wd):
    n_tok, dim = h.shape
    n_local, _, width = wg.shape
    n_chunk = dim // LANES
    big = TILES[-1]
    smem = pl.BlockSpec(memory_space=pltpu.SMEM)
    vmem = pl.BlockSpec(memory_space=pltpu.VMEM)
    hbm = pl.BlockSpec(memory_space=pl.ANY)
    return pl.pallas_call(
        expert_kernel,
        out_shape=jax.ShapeDtypeStruct((n_tok, dim), BF16),
        in_specs=[smem] * 3 + [hbm] + [vmem] * 3 + [hbm] * 3,
        out_specs=hbm,
        scratch_shapes=[
            pltpu.VMEM((n_tok // LANES, LANES, dim), BF16),
            pltpu.VMEM(((n_tok + 1) * PITCH, LANES), F32),
            pltpu.VMEM(((n_tok + 1) * PITCH, LANES), F32),
            pltpu.VMEM((SLOTS, dim, width), BF16),
            pltpu.VMEM((SLOTS, dim, width), BF16),
            pltpu.VMEM((SLOTS, width, dim), BF16),
            pltpu.VMEM((n_chunk * (big + 8), LANES), F32),
            pltpu.VMEM((big, dim), BF16),
            pltpu.VMEM((n_chunk * (big + 8), LANES), F32),
            pltpu.VMEM((2, LANES, dim), BF16),
            pltpu.SMEM((n_local,), jnp.int32),
            pltpu.SemaphoreType.DMA((n_tok // LANES,)),
            pltpu.SemaphoreType.DMA((SLOTS, 3)),
            pltpu.SemaphoreType.DMA((2,)),
        ],
        compiler_params=pltpu.CompilerParams(vmem_limit_bytes=64 * 1000 * 1000),
        name="experts",
    )(lst, wl, cnt, h, act, sig, shd, wg, wu, wd)


def solution(mesh):
    tok_spec = P(('dp', 'ep'), None)
    in_specs = (tok_spec, tok_spec, P(None), P(None, None), P(None, None),
                P('ep', None, 'tp'), P('ep', None, 'tp'), P('ep', 'tp', None),
                P(None, ('tp', 'ep')), P(None, ('tp', 'ep')), P(('tp', 'ep'), None))

    def local_step(hidden_in, topk_idx, norm_gain, router_w, shared_sig_w, exp_gate, exp_up, exp_down,
                   sh_gate, sh_up, sh_down):
        n_local = exp_gate.shape[0]
        dim = hidden_in.shape[1]
        all_x = lax.all_gather(hidden_in, 'ep', axis=0, tiled=True)
        idx_t = jnp.pad(topk_idx.T, ((0, 8 - topk_idx.shape[1]), (0, 0)), constant_values=-1)
        all_idx = lax.all_gather(idx_t, 'ep', axis=1, tiled=True)
        n_tok = all_x.shape[0]
        n_hi = n_tok // LANES
        h, act, sig, lst, wl, cnt = pl.pallas_call(
            functools.partial(prep_kernel, n_local),
            out_shape=(jax.ShapeDtypeStruct((n_tok, dim), BF16),
                       jax.ShapeDtypeStruct((n_tok, sh_gate.shape[1]), BF16),
                       jax.ShapeDtypeStruct((n_tok, 1), F32),
                       jax.ShapeDtypeStruct((n_local * n_hi, LANES), jnp.int32),
                       jax.ShapeDtypeStruct((n_local * n_hi, LANES), F32),
                       jax.ShapeDtypeStruct((n_local, LANES), jnp.int32)),
            in_specs=[pl.BlockSpec(memory_space=pltpu.VMEM)] * 7,
            out_specs=[pl.BlockSpec(memory_space=pltpu.VMEM)] * 6,
            scratch_shapes=[pltpu.VMEM((dim, LANES), BF16), pltpu.VMEM((n_hi, LANES, LANES), F32)],
            name="prep",
        )(all_x, all_idx, norm_gain.reshape(1, -1), router_w, shared_sig_w, sh_gate, sh_up)
        partial = run_experts(lst, wl, cnt, h, act, sig, sh_down, exp_gate, exp_up, exp_down)
        own_rows = lax.psum_scatter(partial, 'ep', scatter_dimension=0, tiled=True)
        total = lax.psum(own_rows, 'tp')
        return (hidden_in.astype(F32) + total.astype(F32)).astype(BF16)

    return jax.shard_map(local_step, mesh=mesh, in_specs=in_specs, out_specs=tok_spec, check_vma=False)
```

```python
import functools

import jax
import jax.numpy as jnp
from jax import lax
from jax.experimental import pallas as pl
from jax.experimental.pallas import tpu as pltpu
from jax.sharding import PartitionSpec as P

RMS_EPS = 1e-6
LANES = 128
PITCH = 24
TILES = (64, 256, 320, 384, 512)
SLOTS = 3
F32 = jnp.float32
BF16 = jnp.bfloat16
NT = (((1,), (1,)), ((), ()))
TN = (((0,), (0,)), ((), ()))
MESH = pl.DeviceIdType.MESH


def place():
    ep, y = lax.axis_index("ep"), lax.axis_index("tp")
    return ep // 2, ep % 2, y, lax.axis_size("ep") // 2, lax.axis_size("tp")


def peer(x, core, y):
    return {"ep": 2 * x + core, "tp": y}


def remote(src, dst, send, recv, where):
    return pltpu.make_async_remote_copy(src_ref=src, dst_ref=dst, send_sem=send, recv_sem=recv,
                                        device_id=where, device_id_type=MESH)


def meet(peers):
    barrier = pltpu.get_barrier_semaphore()
    for p in peers:
        pl.semaphore_signal(barrier, inc=1, device_id=p, device_id_type=MESH)
    pl.semaphore_wait(barrier, len(peers))


def token_pair(x, gain, sigw, cols_ref, n_exp, width, up_at):
    xf = x.astype(F32)
    inv = lax.rsqrt(jnp.mean(xf * xf, axis=-1, keepdims=True) + RMS_EPS)
    h = (xf * inv * gain.astype(F32)).astype(BF16)
    sig = jax.nn.sigmoid(jnp.sum(h.astype(F32) * sigw.astype(F32), axis=-1, keepdims=True))
    return h, sig


def pair_dots(h, cols_ref, n_exp, width, up_at):
    out = lax.dot_general(cols_ref[...], h, NT, preferred_element_type=F32)
    logits = out[:n_exp]
    ex = jnp.exp(logits - jnp.max(logits, axis=0, keepdims=True))
    prob = ex / jnp.sum(ex, axis=0, keepdims=True)
    act = (jax.nn.silu(out[n_exp:n_exp + width]) * out[up_at:up_at + width]).astype(BF16)
    return prob, act


def routing_lists(idx_t, wt, first, n_local, lst_ref, wl_ref, cnt_ref):
    n_tok = idx_t.shape[1]
    n_hi = n_tok // LANES
    sub = lax.broadcasted_iota(jnp.int32, (n_local, n_tok), 0)
    member = jnp.zeros((n_local, n_tok), F32)
    for e in range(n_local):
        hit = jnp.sum((idx_t == first + e).astype(F32), axis=0, keepdims=True)
        member = jnp.where(sub == e, hit, member)
    tri = (lax.broadcasted_iota(jnp.int32, (LANES, LANES), 0)
           < lax.broadcasted_iota(jnp.int32, (LANES, LANES), 1)).astype(F32).astype(BF16)
    base = jnp.zeros((n_local, 1), F32)
    parts = []
    for b in range(n_hi):
        m_b = member[:, b * LANES:(b + 1) * LANES]
        parts.append(jnp.dot(m_b.astype(BF16), tri, preferred_element_type=F32) + base)
        base = base + jnp.sum(m_b, axis=-1, keepdims=True)
    pos = jnp.concatenate(parts, axis=1).astype(jnp.int32)
    cnt_ref[...] = jnp.broadcast_to(base, cnt_ref.shape).astype(jnp.int32)
    tok = lax.broadcasted_iota(jnp.int32, (n_hi, n_tok), 1)
    hi_id = lax.broadcasted_iota(jnp.int32, (n_hi, n_tok), 0)
    lo_id = lax.broadcasted_iota(jnp.int32, (LANES, n_tok), 0)
    row_id = (lax.broadcasted_iota(jnp.int32, (n_hi, LANES), 0) * LANES
              + lax.broadcasted_iota(jnp.int32, (n_hi, LANES), 1))
    tok_hi = (tok >> 3).astype(F32)
    tok_lo = (tok & 7).astype(F32)
    for e in range(n_local):
        p_e = pos[e:e + 1, :]
        here = ((p_e >> 7) == hi_id) & (member[e:e + 1, :] > 0.0)
        lo_hot = jnp.where((p_e & (LANES - 1)) == lo_id, 1.0, 0.0).astype(BF16)
        w = wt[e:e + 1, :]
        w1 = w.astype(BF16).astype(F32)
        w2 = (w - w1).astype(BF16).astype(F32)
        w3 = w - w1 - w2
        rows = [jnp.where(here, v, 0.0) for v in (tok_hi, tok_lo, w1, w2, w3)]
        lhs = jnp.concatenate(rows, axis=0).astype(BF16)
        got = lax.dot_general(lhs, lo_hot, NT, preferred_element_type=F32)
        t_of = got[:n_hi] * 8.0 + got[n_hi:2 * n_hi]
        w_of = (got[2 * n_hi:3 * n_hi] + got[3 * n_hi:4 * n_hi]) + got[4 * n_hi:]
        valid = row_id < base[e:e + 1, :].astype(jnp.int32)
        lst_ref[e * n_hi:(e + 1) * n_hi, :] = jnp.where(valid, t_of.astype(jnp.int32), n_tok) * PITCH
        wl_ref[e * n_hi:(e + 1) * n_hi, :] = jnp.where(valid, w_of, 0.0)


def gather_kernel(n_local, x_hbm, idx_hbm, gain_ref, rw_ref, sigw_ref, shg_ref, shu_ref,
                  h_hbm, act_ref, sigv_ref, lst_ref, wl_ref, cnt_ref,
                  tok, idx, cols, prob, hbuf, in_sem, send, recv, isend, irecv, out_sem):
    x, core, y, n_x, n_y = place()
    n_exp, width = rw_ref.shape[0], shg_ref.shape[0]
    up_at = n_exp + (width + 15) // 16 * 16
    rows = x_hbm.shape[0]
    half, piece = rows // 2, rows // 4
    own = 2 * x + core
    load_x = pltpu.make_async_copy(x_hbm, tok.at[own], in_sem.at[0])
    load_i = pltpu.make_async_copy(idx_hbm, idx.at[own], in_sem.at[1])
    load_x.start()
    load_i.start()

    def at(v, n):
        return lax.rem(v + n, n)

    right, left, far = at(x + 1, n_x), at(x - 1, n_x), at(x + 2, n_x)
    up, down = at(y + 1, n_y), at(y - 1, n_y)
    others = [peer(x, 1 - core, y)]
    for d in (right, left, far):
        for c in (core, 1 - core):
            others.append(peer(d, c, y))
    meet(others + [peer(x, core, up), peer(x, core, down)])
    load_x.wait()
    load_i.wait()

    started = []
    count = [0]

    def copy(block, row, n_rows, where):
        k = count[0]
        count[0] += 1
        row = pl.multiple_of(row, piece)
        ref = tok.at[block, pl.ds(row, n_rows), :]
        c = remote(ref, ref, send.at[k], recv.at[k], where)
        return c

    def go(c):
        c.start()
        started.append(c)
        return c

    mine = (y % 2) * half
    m0, m1 = mine, mine + piece
    to_right, to_left = peer(right, core, y), peer(left, core, y)
    to_up, to_down, to_mate = peer(x, core, up), peer(x, core, down), peer(x, 1 - core, y)
    s_r0 = go(copy(own, m0, piece, to_right))
    s_l1 = go(copy(own, m1, piece, to_left))
    s_mate = go(copy(own, 0, rows, to_mate))
    s_r1 = go(copy(own, m1, piece, to_right))
    s_l0 = go(copy(own, m0, piece, to_left))
    icopies = []
    for k, p in enumerate(others):
        c = remote(idx.at[own], idx.at[own], isend.at[k], irecv.at[k], p)
        c.start()
        icopies.append(c)

    cols[...] = jnp.zeros_like(cols)
    cols[:n_exp, :] = rw_ref[...]
    cols[n_exp:n_exp + width, :] = shg_ref[...]
    cols[up_at:up_at + width, :] = shu_ref[...]

    outs = []

    def pair(slot, px):
        for c in range(2):
            h, sig = token_pair(tok[2 * px + c], gain_ref[...], sigw_ref[...], cols, n_exp, width, up_at)
            hbuf[slot, c * rows:(c + 1) * rows, :] = h
            sigv_ref[pl.ds(pl.multiple_of((2 * px + c) * rows, rows), rows), :] = sig
        out = pltpu.make_async_copy(hbuf.at[slot], h_hbm.at[pl.ds(pl.multiple_of(2 * px * rows, 2 * rows), 2 * rows), :],
                                    out_sem.at[slot])
        p, a = pair_dots(hbuf[slot], cols, n_exp, width, up_at)
        prob[px] = p
        act_ref[:, pl.ds(pl.multiple_of(px * 2 * rows, 2 * rows), 2 * rows)] = a
        out.start()
        outs.append(out)

    def relay(arrived, block, row, vertical, forward=None):
        arrived.wait_recv()
        res = []
        if forward is not None:
            res.append(go(copy(block, row, piece, forward)))
        res.append(go(copy(block, row, piece, vertical)))
        res.append(go(copy(block, row, piece, to_mate)))
        return res

    lb, rb, fb = 2 * left + core, 2 * right + core, 2 * far + core
    f_r, v_l0, d1 = relay(s_r0, lb, m0, to_up, to_right)
    f_l, v_r1, d2 = relay(s_l1, rb, m1, to_down, to_left)
    s_mate.wait_recv()
    pair(0, x)
    v_l1, d3 = relay(s_r1, lb, m1, to_down)
    v_r0, d4 = relay(s_l0, rb, m0, to_up)
    o0 = half - mine
    o1 = o0 + piece

    def pass_on(arrived, block, row):
        arrived.wait_recv()
        return go(copy(block, row, piece, to_mate))

    e1 = pass_on(v_l0, lb, o0)
    e2 = pass_on(v_r1, rb, o1)
    v_f0, d5 = relay(f_r, fb, m0, to_up)
    v_f1, d6 = relay(f_l, fb, m1, to_down)
    e3 = pass_on(v_l1, lb, o1)
    e4 = pass_on(v_r0, rb, o0)
    for c in (d1, d3, e1, e3):
        c.wait_recv()
    pair(1, left)
    for c in (d2, d4, e2, e4):
        c.wait_recv()
    e5 = pass_on(v_f0, fb, o0)
    e6 = pass_on(v_f1, fb, o1)
    pair(2, right)
    for c in icopies:
        c.wait_recv()
    for c in (d5, d6, e5, e6):
        c.wait_recv()
    pair(3, far)

    first = pl.multiple_of(own * n_local, n_local)
    wt = jnp.concatenate([prob[b, pl.ds(first, n_local), :] for b in range(n_x)], axis=1)
    idx_t = jnp.concatenate([idx[b] for b in range(2 * n_x)], axis=1)
    routing_lists(idx_t, wt, first, n_local, lst_ref, wl_ref, cnt_ref)
    for c in started + icopies:
        c.wait_send()
    for c in outs:
        c.wait()


def run_gather(hidden, idx_t, gain, rw_t, sig_t, shg_t, shu_t, n_local, n_x):
    rows, dim = hidden.shape
    n_tok = rows * 2 * n_x
    n_hi = n_tok // LANES
    n_exp, width = rw_t.shape[0], shg_t.shape[0]
    pad = (width + 15) // 16 * 16
    n_copy = 5 + 2 * 3 + 2 * 2 + 2 * 2 + 6
    n_peer = 2 * n_x - 1
    vmem = pl.BlockSpec(memory_space=pltpu.VMEM)
    hbm = pl.BlockSpec(memory_space=pl.ANY)
    return pl.pallas_call(
        functools.partial(gather_kernel, n_local),
        out_shape=(jax.ShapeDtypeStruct((n_tok, dim), BF16),
                   jax.ShapeDtypeStruct((width, n_tok), BF16),
                   jax.ShapeDtypeStruct((n_tok, 1), F32),
                   jax.ShapeDtypeStruct((n_local * n_hi, LANES), jnp.int32),
                   jax.ShapeDtypeStruct((n_local * n_hi, LANES), F32),
                   jax.ShapeDtypeStruct((n_local, LANES), jnp.int32)),
        in_specs=[hbm, hbm] + [vmem] * 5,
        out_specs=[hbm] + [vmem] * 5,
        scratch_shapes=[
            pltpu.VMEM((2 * n_x, rows, dim), BF16),
            pltpu.VMEM((2 * n_x,) + idx_t.shape, jnp.int32),
            pltpu.VMEM((n_exp + 2 * pad, dim), BF16),
            pltpu.VMEM((n_x, n_exp, 2 * rows), F32),
            pltpu.VMEM((n_x, 2 * rows, dim), BF16),
            pltpu.SemaphoreType.DMA((2,)),
            pltpu.SemaphoreType.DMA((n_copy,)),
            pltpu.SemaphoreType.DMA((n_copy,)),
            pltpu.SemaphoreType.DMA((n_peer,)),
            pltpu.SemaphoreType.DMA((n_peer,)),
            pltpu.SemaphoreType.DMA((n_x,)),
        ],
        compiler_params=pltpu.CompilerParams(collective_id=0, has_side_effects=True, vmem_limit_bytes=32 * 1000 * 1000),
        name="gather",
    )(hidden, idx_t, gain, rw_t, sig_t, shg_t, shu_t)


def expert_kernel(lst, wl, cnt, h_hbm, act_ref, sig_ref, shd_ref, wg_hbm, wu_hbm, wd_hbm, out_hbm,
                  h_in, table, acc, wg, wu, wd, xt, xb, fb, ob, active, in_sem, w_sem, out_sem):
    n_tok, dim = h_hbm.shape
    n_local = wg_hbm.shape[0]
    n_chunk = dim // LANES
    n_blocks = n_tok // LANES

    def fetch_h(b):
        return pltpu.make_async_copy(h_hbm.at[pl.ds(b * LANES, LANES), :], h_in.at[b], in_sem.at[b])

    def weight_copies(e, s):
        return (pltpu.make_async_copy(wg_hbm.at[e], wg.at[s], w_sem.at[s, 0]),
                pltpu.make_async_copy(wu_hbm.at[e], wu.at[s], w_sem.at[s, 1]),
                pltpu.make_async_copy(wd_hbm.at[e], wd.at[s], w_sem.at[s, 2]))

    for b in range(n_blocks):
        fetch_h(b).start()

    def note(e, n):
        has = cnt[e, 0] > 0

        @pl.when(has)
        def _():
            active[n] = e

        return n + jnp.where(has, 1, 0)

    n_active = lax.fori_loop(0, n_local, note, 0)
    for s in range(SLOTS - 1):
        @pl.when(s < n_active)
        def _():
            for c in weight_copies(active[s], s):
                c.start()

    def clear(i, carry):
        acc[pl.ds(pl.multiple_of(i * 128, 128), 128), :] = jnp.zeros((128, LANES), F32)
        return carry

    lax.fori_loop(0, (n_tok * PITCH) // 128, clear, 0)
    acc[n_tok * PITCH:, :] = jnp.zeros((acc.shape[0] - n_tok * PITCH, LANES), F32)
    table[n_tok * PITCH:, :] = jnp.zeros((table.shape[0] - n_tok * PITCH, LANES), F32)

    def spread(b, carry):
        fetch_h(b).wait()
        for c in range(n_chunk):
            table[pl.ds(b * LANES * PITCH + c, LANES, stride=PITCH), :] = (
                h_in[b, :, c * LANES:(c + 1) * LANES].astype(F32))
        return carry

    lax.fori_loop(0, n_blocks, spread, 0)

    def list_at(e, r):
        return e * n_blocks + (r >> 7), r & (LANES - 1)

    def ffn(m, e, s, r0, n):
        stride = m + 8
        groups = (n + 7) // 8

        def gather(g, carry):
            hi, lo = list_at(e, r0 + g * 8)
            for i in range(8):
                r = g * 8 + i
                t = lst[hi, lo + i]
                slab = table[pl.ds(pl.multiple_of(t, 8), n_chunk), :]
                xt[pl.ds(r, n_chunk, stride=stride), :] = slab
            return carry

        lax.fori_loop(0, groups, gather, 0)
        for c in range(n_chunk):
            xb[:m, c * LANES:(c + 1) * LANES] = xt[c * stride:c * stride + m, :].astype(BF16)
        gate = lax.dot_general(wg[s], xb[:m, :], NT, preferred_element_type=F32)
        up = lax.dot_general(wu[s], xb[:m, :], NT, preferred_element_type=F32)
        act = (jax.nn.silu(gate) * up).astype(BF16)
        for c in range(0, n_chunk, 2):
            f = lax.dot_general(act, wd[s, :, c * LANES:(c + 2) * LANES], TN, preferred_element_type=F32)
            fb[c * stride:c * stride + m, :] = f[:, :LANES]
            fb[(c + 1) * stride:(c + 1) * stride + m, :] = f[:, LANES:]

        def scatter(g, carry):
            where, old, new = [], [], []
            hi, lo = list_at(e, r0 + g * 8)
            for i in range(8):
                t = lst[hi, lo + i]
                where.append(pl.multiple_of(t, 8))
                old.append(acc[pl.ds(where[i], n_chunk), :])
            for i in range(8):
                r = g * 8 + i
                w = wl[hi, lo + i]
                new.append(old[i] + w * fb[pl.ds(r, n_chunk, stride=stride), :])
            for i in range(8):
                acc[pl.ds(where[i], n_chunk), :] = new[i]
            return carry

        lax.fori_loop(0, groups, scatter, 0)

    big = TILES[-1]

    def expert(i, carry):
        e = active[i]
        s = lax.rem(i, SLOTS)
        ahead = i + SLOTS - 1

        @pl.when(ahead < n_active)
        def _():
            for c in weight_copies(active[ahead], lax.rem(ahead, SLOTS)):
                c.start()

        for c in weight_copies(e, s):
            c.wait()
        total = cnt[e, 0]

        def piece(j, carry2):
            r0 = j * big
            n = jnp.minimum(total - r0, big)
            below = 0
            for m in TILES:
                @pl.when((n > below) & (n <= m))
                def _(m=m):
                    ffn(m, e, s, r0, n)
                below = m
            return carry2

        lax.fori_loop(0, (total + big - 1) // big, piece, 0)
        return carry

    lax.fori_loop(0, n_active, expert, 0)

    def write_out(b, slot):
        return pltpu.make_async_copy(ob.at[slot], out_hbm.at[pl.ds(b * LANES, LANES), :], out_sem.at[slot])

    def finish(b, carry):
        slot = lax.rem(b, 2)

        @pl.when(b >= 2)
        def _():
            write_out(b - 2, slot).wait()

        rows = pl.ds(pl.multiple_of(b * LANES, LANES), LANES)
        sig = sig_ref[rows, :]
        for c in range(0, n_chunk, 2):
            sh = sig * lax.dot_general(act_ref[:, rows], shd_ref[:, c * LANES:(c + 2) * LANES], TN,
                                       preferred_element_type=F32)
            for d in range(2):
                routed = acc[pl.ds(b * LANES * PITCH + c + d, LANES, stride=PITCH), :]
                ob[slot, :, (c + d) * LANES:(c + d + 1) * LANES] = (
                    routed + sh[:, d * LANES:(d + 1) * LANES]).astype(BF16)
        write_out(b, slot).start()
        return carry

    lax.fori_loop(0, n_blocks, finish, 0)
    for b in (n_blocks - 2, n_blocks - 1):
        write_out(b, b % 2).wait()


def run_experts(lst, wl, cnt, h, act, sig, shd, wg, wu, wd):
    n_tok, dim = h.shape
    n_local, width, _ = wg.shape
    n_chunk = dim // LANES
    big = TILES[-1]
    smem = pl.BlockSpec(memory_space=pltpu.SMEM)
    vmem = pl.BlockSpec(memory_space=pltpu.VMEM)
    hbm = pl.BlockSpec(memory_space=pl.ANY)
    return pl.pallas_call(
        expert_kernel,
        out_shape=jax.ShapeDtypeStruct((n_tok, dim), BF16),
        in_specs=[smem] * 3 + [hbm] + [vmem] * 3 + [hbm] * 3,
        out_specs=hbm,
        scratch_shapes=[
            pltpu.VMEM((n_tok // LANES, LANES, dim), BF16),
            pltpu.VMEM(((n_tok + 1) * PITCH, LANES), F32),
            pltpu.VMEM(((n_tok + 1) * PITCH, LANES), F32),
            pltpu.VMEM((SLOTS, width, dim), BF16),
            pltpu.VMEM((SLOTS, width, dim), BF16),
            pltpu.VMEM((SLOTS, width, dim), BF16),
            pltpu.VMEM((n_chunk * (big + 8), LANES), F32),
            pltpu.VMEM((big, dim), BF16),
            pltpu.VMEM((n_chunk * (big + 8), LANES), F32),
            pltpu.VMEM((2, LANES, dim), BF16),
            pltpu.SMEM((n_local,), jnp.int32),
            pltpu.SemaphoreType.DMA((n_tok // LANES,)),
            pltpu.SemaphoreType.DMA((SLOTS, 3)),
            pltpu.SemaphoreType.DMA((2,)),
        ],
        compiler_params=pltpu.CompilerParams(vmem_limit_bytes=64 * 1000 * 1000),
        name="experts",
    )(lst, wl, cnt, h, act, sig, shd, wg, wu, wd)


def reduce_kernel(groups, p_hbm, x_ref, out_ref, mate, own, ra, rb, rc, s_in, s_d, r_d, s_a, r_a, s_b, r_b, s_c, r_c,
                  s_e, r_e):
    x, core, y, n_x, n_y = place()
    rows, dim = x_ref.shape
    wide = dim // len(groups)
    part = rows // n_y

    def at(v, n):
        return lax.rem(v + n, n)

    xs = [at(x + d, n_x) for d in range(4)]
    ys = [at(y + d, n_y) for d in range(4)]
    to_mate = peer(x, 1 - core, y)
    x_peers = [None] + [peer(xs[d], core, y) for d in range(1, 4)]
    y_peers = [None] + [peer(x, core, ys[d]) for d in range(1, 4)]

    loads, mates = [], []
    for g in range(len(groups)):
        c = pltpu.make_async_copy(p_hbm.at[:, core, :, g * wide:(g + 1) * wide], own.at[g], s_in.at[g])
        c.start()
        loads.append(c)
    meet([to_mate] + x_peers[1:] + y_peers[1:])
    started = []

    def go(c):
        c.start()
        started.append(c)
        return c

    for g in range(len(groups)):
        mates.append(go(remote(p_hbm.at[:, 1 - core, :, g * wide:(g + 1) * wide], mate.at[g], s_d.at[g], r_d.at[g],
                               to_mate)))

    def unit(g, d, lo, n):
        if groups[g] == "x":
            return own.at[g, xs[d], lo:lo + n, :]
        return own.at[g, :, pl.ds(pl.multiple_of(ys[d] * part, part) + lo, n), :]

    a, b_ind, b_dep = {}, {}, {}
    for g, kind in enumerate(groups):
        loads[g].wait()
        mates[g].wait_recv()
        own[g] = (own[g].astype(F32) + mate[g].astype(F32)).astype(BF16)
        peers = x_peers if kind == "x" else y_peers
        full = rows if kind == "x" else part
        h = full // 2
        land = (lambda r: r) if kind == "x" else (lambda r: r)
        for k, (lo, d) in enumerate(((0, 1), (h, 3))):
            a[g, k] = go(remote(unit(g, 2, lo, h), ra[kind].at[groups[:g].count(kind), k], s_a.at[g, k], r_a.at[g, k],
                                peers[d]))
        for k, (lo, d) in enumerate(((h, 1), (0, 3))):
            dst = rb[kind].at[groups[:g].count(kind), k]
            dst = dst.at[lo:lo + h, :] if kind == "x" else dst.at[:, lo:lo + h, :]
            b_ind[g, k] = go(remote(unit(g, d, lo, h), dst, s_b.at[g, k, 0], r_b.at[g, k, 0], peers[d]))
    for g, kind in enumerate(groups):
        peers = x_peers if kind == "x" else y_peers
        full = rows if kind == "x" else part
        h = full // 2
        n = groups[:g].count(kind)
        for k, (lo, d) in enumerate(((0, 1), (h, 3))):
            a[g, k].wait_recv()
            ref = unit(g, d, lo, h)
            ref[...] = (ref[...].astype(F32) + ra[kind][n, k].astype(F32)).astype(BF16)
        for k, (lo, d) in enumerate(((0, 1), (h, 3))):
            dst = rb[kind].at[n, k]
            dst = dst.at[lo:lo + h, :] if kind == "x" else dst.at[:, lo:lo + h, :]
            b_dep[g, k] = go(remote(unit(g, d, lo, h), dst, s_b.at[g, k, 1], r_b.at[g, k, 1], peers[d]))
    c_sent = {}
    for g, kind in enumerate(groups):
        n = groups[:g].count(kind)
        for k in range(2):
            b_ind[g, k].wait_recv()
            b_dep[g, k].wait_recv()
        full = rows if kind == "x" else part
        ref = unit(g, 0, 0, full)
        ref[...] = (ref[...].astype(F32) + rb[kind][n, 0].astype(F32) + rb[kind][n, 1].astype(F32)).astype(BF16)
        for d in range(1, 4):
            if kind == "x":
                src = own.at[g, x, pl.ds(pl.multiple_of(ys[d] * part, part), part), :]
                where = y_peers[d]
            else:
                src = own.at[g, xs[d], pl.ds(pl.multiple_of(y * part, part), part), :]
                where = x_peers[d]
            c_sent[g, d] = go(remote(src, rc.at[g, d - 1], s_c.at[g, d - 1], r_c.at[g, d - 1], where))
    e_sent = {}
    mine = pl.ds(pl.multiple_of(y * part, part), part)
    for g, kind in enumerate(groups):
        cols = slice(g * wide, (g + 1) * wide)
        total = own[g, x, mine, :].astype(F32)
        for d in range(1, 4):
            c_sent[g, d].wait_recv()
            total = total + rc[g, d - 1].astype(F32)
        out_ref[mine, cols] = (x_ref[mine, cols].astype(F32) + total).astype(BF16)
        for d in range(1, 4):
            ref = out_ref.at[mine, cols]
            e_sent[g, d] = go(remote(ref, ref, s_e.at[g, d - 1], r_e.at[g, d - 1], y_peers[d]))
    for g in range(len(groups)):
        for d in range(1, 4):
            e_sent[g, d].wait_recv()
    for c in started:
        c.wait_send()


def run_reduce(partial, hidden, n_x, n_y):
    rows, dim = hidden.shape
    groups = ("y", "x", "x", "x")
    n_g = len(groups)
    wide = dim // n_g
    part = rows // n_y
    dma = pltpu.SemaphoreType.DMA
    n_kind = {k: groups.count(k) for k in ("x", "y")}

    def kernel(p, xr, o, mate, own, ra_x, ra_y, rb_x, rb_y, *rest):
        reduce_kernel(groups, p, xr, o, mate, own, {"x": ra_x, "y": ra_y}, {"x": rb_x, "y": rb_y}, *rest)

    return pl.pallas_call(
        kernel,
        out_shape=jax.ShapeDtypeStruct((rows, dim), BF16),
        in_specs=[pl.BlockSpec(memory_space=pl.ANY), pl.BlockSpec(memory_space=pltpu.VMEM)],
        out_specs=pl.BlockSpec(memory_space=pltpu.VMEM),
        scratch_shapes=[
            pltpu.VMEM((n_g, n_x, rows, wide), BF16),
            pltpu.VMEM((n_g, n_x, rows, wide), BF16),
            pltpu.VMEM((n_kind["x"], 2, rows // 2, wide), BF16),
            pltpu.VMEM((n_kind["y"], 2, n_x, part // 2, wide), BF16),
            pltpu.VMEM((n_kind["x"], 2, rows, wide), BF16),
            pltpu.VMEM((n_kind["y"], 2, n_x, part, wide), BF16),
            pltpu.VMEM((n_g, 3, part, wide), BF16),
            dma((n_g,)), dma((n_g,)), dma((n_g,)),
            dma((n_g, 2)), dma((n_g, 2)),
            dma((n_g, 2, 2)), dma((n_g, 2, 2)),
            dma((n_g, 3)), dma((n_g, 3)),
            dma((n_g, 3)), dma((n_g, 3)),
        ],
        compiler_params=pltpu.CompilerParams(collective_id=1, has_side_effects=True, vmem_limit_bytes=32 * 1000 * 1000),
        name="reduce",
    )(partial.reshape(n_x, 2, rows, dim), hidden)


def solution(mesh):
    tok_spec = P(('dp', 'ep'), None)
    in_specs = (tok_spec, tok_spec, P(None), P(None, None), P(None, None),
                P('ep', None, 'tp'), P('ep', None, 'tp'), P('ep', 'tp', None),
                P(None, ('tp', 'ep')), P(None, ('tp', 'ep')), P(('tp', 'ep'), None))
    n_x, n_y = mesh.shape['ep'] // 2, mesh.shape['tp']
    assert n_x == 4 and n_y == 4

    def local_step(hidden_in, topk_idx, norm_gain, router_w, shared_sig_w, exp_gate, exp_up, exp_down,
                   sh_gate, sh_up, sh_down):
        h, act, sig, lst, wl, cnt = run_gather(
            hidden_in, topk_idx.T, norm_gain.reshape(1, -1), router_w.T, shared_sig_w.T, sh_gate.T, sh_up.T,
            exp_gate.shape[0], n_x)
        partial = run_experts(lst, wl, cnt, h, act, sig, sh_down,
                              jnp.swapaxes(exp_gate, 1, 2), jnp.swapaxes(exp_up, 1, 2), exp_down)
        return run_reduce(partial, hidden_in, n_x, n_y)

    return jax.shard_map(local_step, mesh=mesh, in_specs=in_specs, out_specs=tok_spec, check_vma=False)
```

```python
import functools

import jax
import jax.numpy as jnp
from jax import lax
from jax.experimental import pallas as pl
from jax.experimental.pallas import tpu as pltpu
from jax.sharding import PartitionSpec as P

RMS_EPS = 1e-6
LANES = 128
PITCH = 24
TILES = (64, 256, 320, 384, 512)
SLOTS = 3
F32 = jnp.float32
BF16 = jnp.bfloat16
NT = (((1,), (1,)), ((), ()))
TN = (((0,), (0,)), ((), ()))
MESH = pl.DeviceIdType.MESH


def place():
    ep, y = lax.axis_index("ep"), lax.axis_index("tp")
    return ep // 2, ep % 2, y, lax.axis_size("ep") // 2, lax.axis_size("tp")


def peer(x, core, y):
    return {"ep": 2 * x + core, "tp": y}


def remote(src, dst, send, recv, where):
    return pltpu.make_async_remote_copy(src_ref=src, dst_ref=dst, send_sem=send, recv_sem=recv,
                                        device_id=where, device_id_type=MESH)


def meet(peers):
    barrier = pltpu.get_barrier_semaphore()
    for p in peers:
        pl.semaphore_signal(barrier, inc=1, device_id=p, device_id_type=MESH)
    pl.semaphore_wait(barrier, len(peers))


def token_pair(x, gain, sigw, cols_ref, n_exp, width, up_at):
    xf = x.astype(F32)
    inv = lax.rsqrt(jnp.mean(xf * xf, axis=-1, keepdims=True) + RMS_EPS)
    h = (xf * inv * gain.astype(F32)).astype(BF16)
    sig = jax.nn.sigmoid(jnp.sum(h.astype(F32) * sigw.astype(F32), axis=-1, keepdims=True))
    return h, sig


def pair_dots(h, cols_ref, n_exp, width, up_at):
    out = lax.dot_general(cols_ref[...], h, NT, preferred_element_type=F32)
    logits = out[:n_exp]
    ex = jnp.exp(logits - jnp.max(logits, axis=0, keepdims=True))
    prob = ex / jnp.sum(ex, axis=0, keepdims=True)
    act = (jax.nn.silu(out[n_exp:n_exp + width]) * out[up_at:up_at + width]).astype(BF16)
    return prob, act


def routing_lists(idx_t, wt, first, n_local, lst_ref, wl_ref, cnt_ref):
    n_tok = idx_t.shape[1]
    n_hi = n_tok // LANES
    sub = lax.broadcasted_iota(jnp.int32, (n_local, n_tok), 0)
    member = jnp.zeros((n_local, n_tok), F32)
    for e in range(n_local):
        hit = jnp.sum((idx_t == first + e).astype(F32), axis=0, keepdims=True)
        member = jnp.where(sub == e, hit, member)
    tri = (lax.broadcasted_iota(jnp.int32, (LANES, LANES), 0)
           < lax.broadcasted_iota(jnp.int32, (LANES, LANES), 1)).astype(F32).astype(BF16)
    base = jnp.zeros((n_local, 1), F32)
    parts = []
    for b in range(n_hi):
        m_b = member[:, b * LANES:(b + 1) * LANES]
        parts.append(jnp.dot(m_b.astype(BF16), tri, preferred_element_type=F32) + base)
        base = base + jnp.sum(m_b, axis=-1, keepdims=True)
    pos = jnp.concatenate(parts, axis=1).astype(jnp.int32)
    cnt_ref[...] = jnp.broadcast_to(base, cnt_ref.shape).astype(jnp.int32)
    tok = lax.broadcasted_iota(jnp.int32, (n_hi, n_tok), 1)
    hi_id = lax.broadcasted_iota(jnp.int32, (n_hi, n_tok), 0)
    lo_id = lax.broadcasted_iota(jnp.int32, (LANES, n_tok), 0)
    row_id = (lax.broadcasted_iota(jnp.int32, (n_hi, LANES), 0) * LANES
              + lax.broadcasted_iota(jnp.int32, (n_hi, LANES), 1))
    tok_hi = (tok >> 3).astype(F32)
    tok_lo = (tok & 7).astype(F32)
    for e in range(n_local):
        p_e = pos[e:e + 1, :]
        here = ((p_e >> 7) == hi_id) & (member[e:e + 1, :] > 0.0)
        lo_hot = jnp.where((p_e & (LANES - 1)) == lo_id, 1.0, 0.0).astype(BF16)
        w = wt[e:e + 1, :]
        w1 = w.astype(BF16).astype(F32)
        w2 = (w - w1).astype(BF16).astype(F32)
        w3 = w - w1 - w2
        rows = [jnp.where(here, v, 0.0) for v in (tok_hi, tok_lo, w1, w2, w3)]
        lhs = jnp.concatenate(rows, axis=0).astype(BF16)
        got = lax.dot_general(lhs, lo_hot, NT, preferred_element_type=F32)
        t_of = got[:n_hi] * 8.0 + got[n_hi:2 * n_hi]
        w_of = (got[2 * n_hi:3 * n_hi] + got[3 * n_hi:4 * n_hi]) + got[4 * n_hi:]
        valid = row_id < base[e:e + 1, :].astype(jnp.int32)
        lst_ref[e * n_hi:(e + 1) * n_hi, :] = jnp.where(valid, t_of.astype(jnp.int32), n_tok) * PITCH
        wl_ref[e * n_hi:(e + 1) * n_hi, :] = jnp.where(valid, w_of, 0.0)


def gather_kernel(n_local, x_hbm, idx_hbm, gain_ref, rw_ref, sigw_ref, shg_ref, shu_ref,
                  h_hbm, act_ref, sigv_ref, lst_ref, wl_ref, cnt_ref,
                  tok, idx, cols, prob, hbuf, in_sem, send, recv, isend, irecv, out_sem):
    x, core, y, n_x, n_y = place()
    n_exp, width = rw_ref.shape[0], shg_ref.shape[0]
    up_at = n_exp + (width + 15) // 16 * 16
    rows = x_hbm.shape[0]
    half, piece = rows // 2, rows // 4
    own = 2 * x + core
    load_x = pltpu.make_async_copy(x_hbm, tok.at[own], in_sem.at[0])
    load_i = pltpu.make_async_copy(idx_hbm, idx.at[own], in_sem.at[1])
    load_x.start()
    load_i.start()

    def at(v, n):
        return lax.rem(v + n, n)

    right, left, far = at(x + 1, n_x), at(x - 1, n_x), at(x + 2, n_x)
    up, down = at(y + 1, n_y), at(y - 1, n_y)
    others = [peer(x, 1 - core, y)]
    for d in (right, left, far):
        for c in (core, 1 - core):
            others.append(peer(d, c, y))
    meet(others + [peer(x, core, up), peer(x, core, down)])
    load_x.wait()
    load_i.wait()

    started = []
    count = [0]

    def copy(block, row, n_rows, where):
        k = count[0]
        count[0] += 1
        row = pl.multiple_of(row, piece)
        ref = tok.at[block, pl.ds(row, n_rows), :]
        c = remote(ref, ref, send.at[k], recv.at[k], where)
        return c

    def go(c):
        c.start()
        started.append(c)
        return c

    mine = (y % 2) * half
    m0, m1 = mine, mine + piece
    to_right, to_left = peer(right, core, y), peer(left, core, y)
    to_up, to_down, to_mate = peer(x, core, up), peer(x, core, down), peer(x, 1 - core, y)
    s_r0 = go(copy(own, m0, piece, to_right))
    s_l1 = go(copy(own, m1, piece, to_left))
    s_mate = go(copy(own, 0, rows, to_mate))
    s_r1 = go(copy(own, m1, piece, to_right))
    s_l0 = go(copy(own, m0, piece, to_left))
    icopies = []
    for k, p in enumerate(others):
        c = remote(idx.at[own], idx.at[own], isend.at[k], irecv.at[k], p)
        c.start()
        icopies.append(c)

    cols[...] = jnp.zeros_like(cols)
    cols[:n_exp, :] = rw_ref[...]
    cols[n_exp:n_exp + width, :] = shg_ref[...]
    cols[up_at:up_at + width, :] = shu_ref[...]

    outs = []

    def pair(slot, px):
        for c in range(2):
            h, sig = token_pair(tok[2 * px + c], gain_ref[...], sigw_ref[...], cols, n_exp, width, up_at)
            hbuf[slot, c * rows:(c + 1) * rows, :] = h
            sigv_ref[pl.ds(pl.multiple_of((2 * px + c) * rows, rows), rows), :] = sig
        out = pltpu.make_async_copy(hbuf.at[slot], h_hbm.at[pl.ds(pl.multiple_of(2 * px * rows, 2 * rows), 2 * rows), :],
                                    out_sem.at[slot])
        p, a = pair_dots(hbuf[slot], cols, n_exp, width, up_at)
        prob[px] = p
        act_ref[:, pl.ds(pl.multiple_of(px * 2 * rows, 2 * rows), 2 * rows)] = a
        out.start()
        outs.append(out)

    def relay(arrived, block, row, vertical, forward=None):
        arrived.wait_recv()
        res = []
        if forward is not None:
            res.append(go(copy(block, row, piece, forward)))
        res.append(go(copy(block, row, piece, vertical)))
        res.append(go(copy(block, row, piece, to_mate)))
        return res

    lb, rb, fb = 2 * left + core, 2 * right + core, 2 * far + core
    f_r, v_l0, d1 = relay(s_r0, lb, m0, to_up, to_right)
    f_l, v_r1, d2 = relay(s_l1, rb, m1, to_down, to_left)
    s_mate.wait_recv()
    pair(0, x)
    v_l1, d3 = relay(s_r1, lb, m1, to_down)
    v_r0, d4 = relay(s_l0, rb, m0, to_up)
    o0 = half - mine
    o1 = o0 + piece

    def pass_on(arrived, block, row):
        arrived.wait_recv()
        return go(copy(block, row, piece, to_mate))

    e1 = pass_on(v_l0, lb, o0)
    e2 = pass_on(v_r1, rb, o1)
    v_f0, d5 = relay(f_r, fb, m0, to_up)
    v_f1, d6 = relay(f_l, fb, m1, to_down)
    e3 = pass_on(v_l1, lb, o1)
    e4 = pass_on(v_r0, rb, o0)
    for c in (d1, d3, e1, e3):
        c.wait_recv()
    pair(1, left)
    for c in (d2, d4, e2, e4):
        c.wait_recv()
    e5 = pass_on(v_f0, fb, o0)
    e6 = pass_on(v_f1, fb, o1)
    pair(2, right)
    for c in icopies:
        c.wait_recv()
    for c in (d5, d6, e5, e6):
        c.wait_recv()
    pair(3, far)

    first = pl.multiple_of(own * n_local, n_local)
    wt = jnp.concatenate([prob[b, pl.ds(first, n_local), :] for b in range(n_x)], axis=1)
    idx_t = jnp.concatenate([idx[b] for b in range(2 * n_x)], axis=1)
    routing_lists(idx_t, wt, first, n_local, lst_ref, wl_ref, cnt_ref)
    for c in started + icopies:
        c.wait_send()
    for c in outs:
        c.wait()


def run_gather(hidden, idx_t, gain, rw_t, sig_t, shg_t, shu_t, n_local, n_x):
    rows, dim = hidden.shape
    n_tok = rows * 2 * n_x
    n_hi = n_tok // LANES
    n_exp, width = rw_t.shape[0], shg_t.shape[0]
    pad = (width + 15) // 16 * 16
    n_copy = 5 + 2 * 3 + 2 * 2 + 2 * 2 + 6
    n_peer = 2 * n_x - 1
    vmem = pl.BlockSpec(memory_space=pltpu.VMEM)
    hbm = pl.BlockSpec(memory_space=pl.ANY)
    return pl.pallas_call(
        functools.partial(gather_kernel, n_local),
        out_shape=(jax.ShapeDtypeStruct((n_tok, dim), BF16),
                   jax.ShapeDtypeStruct((width, n_tok), BF16),
                   jax.ShapeDtypeStruct((n_tok, 1), F32),
                   jax.ShapeDtypeStruct((n_local * n_hi, LANES), jnp.int32),
                   jax.ShapeDtypeStruct((n_local * n_hi, LANES), F32),
                   jax.ShapeDtypeStruct((n_local, LANES), jnp.int32)),
        in_specs=[hbm, hbm] + [vmem] * 5,
        out_specs=[hbm] + [vmem] * 5,
        scratch_shapes=[
            pltpu.VMEM((2 * n_x, rows, dim), BF16),
            pltpu.VMEM((2 * n_x,) + idx_t.shape, jnp.int32),
            pltpu.VMEM((n_exp + 2 * pad, dim), BF16),
            pltpu.VMEM((n_x, n_exp, 2 * rows), F32),
            pltpu.VMEM((n_x, 2 * rows, dim), BF16),
            pltpu.SemaphoreType.DMA((2,)),
            pltpu.SemaphoreType.DMA((n_copy,)),
            pltpu.SemaphoreType.DMA((n_copy,)),
            pltpu.SemaphoreType.DMA((n_peer,)),
            pltpu.SemaphoreType.DMA((n_peer,)),
            pltpu.SemaphoreType.DMA((n_x,)),
        ],
        compiler_params=pltpu.CompilerParams(collective_id=0, has_side_effects=True, vmem_limit_bytes=67_000_000),
        name="gather",
    )(hidden, idx_t, gain, rw_t, sig_t, shg_t, shu_t)


def expert_kernel(lst, wl, cnt, h_hbm, act_ref, sig_ref, shd_ref, wg_hbm, wu_hbm, wd_hbm, out_hbm,
                  h_in, table, acc, wg, wu, wd, xt, xb, fb, ob, active, in_sem, w_sem, out_sem):
    n_tok, dim = h_hbm.shape
    n_local = wg_hbm.shape[0]
    n_chunk = dim // LANES
    n_blocks = n_tok // LANES

    def fetch_h(b):
        return pltpu.make_async_copy(h_hbm.at[pl.ds(b * LANES, LANES), :], h_in.at[b], in_sem.at[b])

    def weight_copies(e, s):
        return (pltpu.make_async_copy(wg_hbm.at[e], wg.at[s], w_sem.at[s, 0]),
                pltpu.make_async_copy(wu_hbm.at[e], wu.at[s], w_sem.at[s, 1]),
                pltpu.make_async_copy(wd_hbm.at[e], wd.at[s], w_sem.at[s, 2]))

    for b in range(n_blocks):
        fetch_h(b).start()

    def note(e, n):
        has = cnt[e, 0] > 0

        @pl.when(has)
        def _():
            active[n] = e

        return n + jnp.where(has, 1, 0)

    n_active = lax.fori_loop(0, n_local, note, 0)
    for s in range(SLOTS - 1):
        @pl.when(s < n_active)
        def _():
            for c in weight_copies(active[s], s):
                c.start()

    def clear(i, carry):
        acc[pl.ds(pl.multiple_of(i * 128, 128), 128), :] = jnp.zeros((128, LANES), F32)
        return carry

    lax.fori_loop(0, (n_tok * PITCH) // 128, clear, 0)
    acc[n_tok * PITCH:, :] = jnp.zeros((acc.shape[0] - n_tok * PITCH, LANES), F32)
    table[n_tok * PITCH:, :] = jnp.zeros((table.shape[0] - n_tok * PITCH, LANES), F32)

    def spread(b, carry):
        fetch_h(b).wait()
        for c in range(n_chunk):
            table[pl.ds(b * LANES * PITCH + c, LANES, stride=PITCH), :] = (
                h_in[b, :, c * LANES:(c + 1) * LANES].astype(F32))
        return carry

    lax.fori_loop(0, n_blocks, spread, 0)

    def list_at(e, r):
        return e * n_blocks + (r >> 7), r & (LANES - 1)

    def ffn(m, e, s, r0, n):
        stride = m + 8
        groups = (n + 7) // 8

        def gather(g, carry):
            hi, lo = list_at(e, r0 + g * 8)
            for i in range(8):
                r = g * 8 + i
                t = lst[hi, lo + i]
                slab = table[pl.ds(pl.multiple_of(t, 8), n_chunk), :]
                xt[pl.ds(r, n_chunk, stride=stride), :] = slab
            return carry

        lax.fori_loop(0, groups, gather, 0)
        for c in range(n_chunk):
            xb[:m, c * LANES:(c + 1) * LANES] = xt[c * stride:c * stride + m, :].astype(BF16)
        gate = lax.dot_general(wg[s], xb[:m, :], NT, preferred_element_type=F32)
        up = lax.dot_general(wu[s], xb[:m, :], NT, preferred_element_type=F32)
        act = (jax.nn.silu(gate) * up).astype(BF16)
        for c in range(0, n_chunk, 2):
            f = lax.dot_general(act, wd[s, :, c * LANES:(c + 2) * LANES], TN, preferred_element_type=F32)
            fb[c * stride:c * stride + m, :] = f[:, :LANES]
            fb[(c + 1) * stride:(c + 1) * stride + m, :] = f[:, LANES:]

        def scatter(g, carry):
            where, old, new = [], [], []
            hi, lo = list_at(e, r0 + g * 8)
            for i in range(8):
                t = lst[hi, lo + i]
                where.append(pl.multiple_of(t, 8))
                old.append(acc[pl.ds(where[i], n_chunk), :])
            for i in range(8):
                r = g * 8 + i
                w = wl[hi, lo + i]
                new.append(old[i] + w * fb[pl.ds(r, n_chunk, stride=stride), :])
            for i in range(8):
                acc[pl.ds(where[i], n_chunk), :] = new[i]
            return carry

        lax.fori_loop(0, groups, scatter, 0)

    big = TILES[-1]

    def expert(i, carry):
        e = active[i]
        s = lax.rem(i, SLOTS)
        ahead = i + SLOTS - 1

        @pl.when(ahead < n_active)
        def _():
            for c in weight_copies(active[ahead], lax.rem(ahead, SLOTS)):
                c.start()

        for c in weight_copies(e, s):
            c.wait()
        total = cnt[e, 0]

        def piece(j, carry2):
            r0 = j * big
            n = jnp.minimum(total - r0, big)
            below = 0
            for m in TILES:
                @pl.when((n > below) & (n <= m))
                def _(m=m):
                    ffn(m, e, s, r0, n)
                below = m
            return carry2

        lax.fori_loop(0, (total + big - 1) // big, piece, 0)
        return carry

    lax.fori_loop(0, n_active, expert, 0)

    def write_out(b, slot):
        return pltpu.make_async_copy(ob.at[slot], out_hbm.at[pl.ds(b * LANES, LANES), :], out_sem.at[slot])

    def finish(b, carry):
        slot = lax.rem(b, 2)

        @pl.when(b >= 2)
        def _():
            write_out(b - 2, slot).wait()

        rows = pl.ds(pl.multiple_of(b * LANES, LANES), LANES)
        sig = sig_ref[rows, :]
        for c in range(0, n_chunk, 2):
            sh = sig * lax.dot_general(act_ref[:, rows], shd_ref[:, c * LANES:(c + 2) * LANES], TN,
                                       preferred_element_type=F32)
            for d in range(2):
                routed = acc[pl.ds(b * LANES * PITCH + c + d, LANES, stride=PITCH), :]
                ob[slot, :, (c + d) * LANES:(c + d + 1) * LANES] = (
                    routed + sh[:, d * LANES:(d + 1) * LANES]).astype(BF16)
        write_out(b, slot).start()
        return carry

    lax.fori_loop(0, n_blocks, finish, 0)
    for b in (n_blocks - 2, n_blocks - 1):
        write_out(b, b % 2).wait()


def run_experts(lst, wl, cnt, h, act, sig, shd, wg, wu, wd):
    n_tok, dim = h.shape
    n_local, width, _ = wg.shape
    n_chunk = dim // LANES
    big = TILES[-1]
    smem = pl.BlockSpec(memory_space=pltpu.SMEM)
    vmem = pl.BlockSpec(memory_space=pltpu.VMEM)
    hbm = pl.BlockSpec(memory_space=pl.ANY)
    return pl.pallas_call(
        expert_kernel,
        out_shape=jax.ShapeDtypeStruct((n_tok, dim), BF16),
        in_specs=[smem] * 3 + [hbm] + [vmem] * 3 + [hbm] * 3,
        out_specs=hbm,
        scratch_shapes=[
            pltpu.VMEM((n_tok // LANES, LANES, dim), BF16),
            pltpu.VMEM(((n_tok + 1) * PITCH, LANES), F32),
            pltpu.VMEM(((n_tok + 1) * PITCH, LANES), F32),
            pltpu.VMEM((SLOTS, width, dim), BF16),
            pltpu.VMEM((SLOTS, width, dim), BF16),
            pltpu.VMEM((SLOTS, width, dim), BF16),
            pltpu.VMEM((n_chunk * (big + 8), LANES), F32),
            pltpu.VMEM((big, dim), BF16),
            pltpu.VMEM((n_chunk * (big + 8), LANES), F32),
            pltpu.VMEM((2, LANES, dim), BF16),
            pltpu.SMEM((n_local,), jnp.int32),
            pltpu.SemaphoreType.DMA((n_tok // LANES,)),
            pltpu.SemaphoreType.DMA((SLOTS, 3)),
            pltpu.SemaphoreType.DMA((2,)),
        ],
        compiler_params=pltpu.CompilerParams(vmem_limit_bytes=67_000_000),
        name="experts",
    )(lst, wl, cnt, h, act, sig, shd, wg, wu, wd)


def reduce_kernel(groups, p_hbm, x_ref, out_ref, mate, own, ra, rb, rc, s_in, s_d, r_d, s_a, r_a, s_b, r_b, s_c, r_c,
                  s_e, r_e):
    x, core, y, n_x, n_y = place()
    rows, dim = x_ref.shape
    wide = dim // len(groups)
    part = rows // n_y

    def at(v, n):
        return lax.rem(v + n, n)

    xs = [at(x + d, n_x) for d in range(4)]
    ys = [at(y + d, n_y) for d in range(4)]
    to_mate = peer(x, 1 - core, y)
    x_peers = [None] + [peer(xs[d], core, y) for d in range(1, 4)]
    y_peers = [None] + [peer(x, core, ys[d]) for d in range(1, 4)]

    loads, mates = [], []
    for g in range(len(groups)):
        c = pltpu.make_async_copy(p_hbm.at[:, core, :, g * wide:(g + 1) * wide], own.at[g], s_in.at[g])
        c.start()
        loads.append(c)
    meet([to_mate] + x_peers[1:] + y_peers[1:])
    started = []

    def go(c):
        c.start()
        started.append(c)
        return c

    for g in range(len(groups)):
        mates.append(go(remote(p_hbm.at[:, 1 - core, :, g * wide:(g + 1) * wide], mate.at[g], s_d.at[g], r_d.at[g],
                               to_mate)))

    def unit(g, d, lo, n):
        if groups[g] == "x":
            return own.at[g, xs[d], lo:lo + n, :]
        return own.at[g, :, pl.ds(pl.multiple_of(ys[d] * part, part) + lo, n), :]

    a, b_ind, b_dep = {}, {}, {}
    for g, kind in enumerate(groups):
        loads[g].wait()
        mates[g].wait_recv()
        own[g] = (own[g].astype(F32) + mate[g].astype(F32)).astype(BF16)
        peers = x_peers if kind == "x" else y_peers
        full = rows if kind == "x" else part
        h = full // 2
        land = (lambda r: r) if kind == "x" else (lambda r: r)
        for k, (lo, d) in enumerate(((0, 1), (h, 3))):
            a[g, k] = go(remote(unit(g, 2, lo, h), ra[kind].at[groups[:g].count(kind), k], s_a.at[g, k], r_a.at[g, k],
                                peers[d]))
        for k, (lo, d) in enumerate(((h, 1), (0, 3))):
            dst = rb[kind].at[groups[:g].count(kind), k]
            dst = dst.at[lo:lo + h, :] if kind == "x" else dst.at[:, lo:lo + h, :]
            b_ind[g, k] = go(remote(unit(g, d, lo, h), dst, s_b.at[g, k, 0], r_b.at[g, k, 0], peers[d]))
    for g, kind in enumerate(groups):
        peers = x_peers if kind == "x" else y_peers
        full = rows if kind == "x" else part
        h = full // 2
        n = groups[:g].count(kind)
        for k, (lo, d) in enumerate(((0, 1), (h, 3))):
            a[g, k].wait_recv()
            ref = unit(g, d, lo, h)
            ref[...] = (ref[...].astype(F32) + ra[kind][n, k].astype(F32)).astype(BF16)
        for k, (lo, d) in enumerate(((0, 1), (h, 3))):
            dst = rb[kind].at[n, k]
            dst = dst.at[lo:lo + h, :] if kind == "x" else dst.at[:, lo:lo + h, :]
            b_dep[g, k] = go(remote(unit(g, d, lo, h), dst, s_b.at[g, k, 1], r_b.at[g, k, 1], peers[d]))
    c_sent = {}
    for g, kind in enumerate(groups):
        n = groups[:g].count(kind)
        for k in range(2):
            b_ind[g, k].wait_recv()
            b_dep[g, k].wait_recv()
        full = rows if kind == "x" else part
        ref = unit(g, 0, 0, full)
        ref[...] = (ref[...].astype(F32) + rb[kind][n, 0].astype(F32) + rb[kind][n, 1].astype(F32)).astype(BF16)
        for d in range(1, 4):
            if kind == "x":
                src = own.at[g, x, pl.ds(pl.multiple_of(ys[d] * part, part), part), :]
                where = y_peers[d]
            else:
                src = own.at[g, xs[d], pl.ds(pl.multiple_of(y * part, part), part), :]
                where = x_peers[d]
            c_sent[g, d] = go(remote(src, rc.at[g, d - 1], s_c.at[g, d - 1], r_c.at[g, d - 1], where))
    e_sent = {}
    mine = pl.ds(pl.multiple_of(y * part, part), part)
    for g, kind in enumerate(groups):
        cols = slice(g * wide, (g + 1) * wide)
        total = own[g, x, mine, :].astype(F32)
        for d in range(1, 4):
            c_sent[g, d].wait_recv()
            total = total + rc[g, d - 1].astype(F32)
        out_ref[mine, cols] = (x_ref[mine, cols].astype(F32) + total).astype(BF16)
        for d in range(1, 4):
            ref = out_ref.at[mine, cols]
            e_sent[g, d] = go(remote(ref, ref, s_e.at[g, d - 1], r_e.at[g, d - 1], y_peers[d]))
    for g in range(len(groups)):
        for d in range(1, 4):
            e_sent[g, d].wait_recv()
    for c in started:
        c.wait_send()


def run_reduce(partial, hidden, n_x, n_y):
    rows, dim = hidden.shape
    groups = ("y", "x", "x", "x")
    n_g = len(groups)
    wide = dim // n_g
    part = rows // n_y
    dma = pltpu.SemaphoreType.DMA
    n_kind = {k: groups.count(k) for k in ("x", "y")}

    def kernel(p, xr, o, mate, own, ra_x, ra_y, rb_x, rb_y, *rest):
        reduce_kernel(groups, p, xr, o, mate, own, {"x": ra_x, "y": ra_y}, {"x": rb_x, "y": rb_y}, *rest)

    return pl.pallas_call(
        kernel,
        out_shape=jax.ShapeDtypeStruct((rows, dim), BF16),
        in_specs=[pl.BlockSpec(memory_space=pl.ANY), pl.BlockSpec(memory_space=pltpu.VMEM)],
        out_specs=pl.BlockSpec(memory_space=pltpu.VMEM),
        scratch_shapes=[
            pltpu.VMEM((n_g, n_x, rows, wide), BF16),
            pltpu.VMEM((n_g, n_x, rows, wide), BF16),
            pltpu.VMEM((n_kind["x"], 2, rows // 2, wide), BF16),
            pltpu.VMEM((n_kind["y"], 2, n_x, part // 2, wide), BF16),
            pltpu.VMEM((n_kind["x"], 2, rows, wide), BF16),
            pltpu.VMEM((n_kind["y"], 2, n_x, part, wide), BF16),
            pltpu.VMEM((n_g, 3, part, wide), BF16),
            dma((n_g,)), dma((n_g,)), dma((n_g,)),
            dma((n_g, 2)), dma((n_g, 2)),
            dma((n_g, 2, 2)), dma((n_g, 2, 2)),
            dma((n_g, 3)), dma((n_g, 3)),
            dma((n_g, 3)), dma((n_g, 3)),
        ],
        compiler_params=pltpu.CompilerParams(collective_id=1, has_side_effects=True, vmem_limit_bytes=67_000_000),
        name="reduce",
    )(partial.reshape(n_x, 2, rows, dim), hidden)


def solution(mesh):
    tok_spec = P(('dp', 'ep'), None)
    in_specs = (tok_spec, tok_spec, P(None), P(None, None), P(None, None),
                P('ep', None, 'tp'), P('ep', None, 'tp'), P('ep', 'tp', None),
                P(None, ('tp', 'ep')), P(None, ('tp', 'ep')), P(('tp', 'ep'), None))
    n_x, n_y = mesh.shape['ep'] // 2, mesh.shape['tp']
    assert n_x == 4 and n_y == 4

    def local_step(hidden_in, topk_idx, norm_gain, router_w, shared_sig_w, exp_gate, exp_up, exp_down,
                   sh_gate, sh_up, sh_down):
        h, act, sig, lst, wl, cnt = run_gather(
            hidden_in, topk_idx.T, norm_gain.reshape(1, -1), router_w.T, shared_sig_w.T, sh_gate.T, sh_up.T,
            exp_gate.shape[0], n_x)
        partial = run_experts(lst, wl, cnt, h, act, sig, sh_down,
                              jnp.swapaxes(exp_gate, 1, 2), jnp.swapaxes(exp_up, 1, 2), exp_down)
        return run_reduce(partial, hidden_in, n_x, n_y)

    return jax.shard_map(local_step, mesh=mesh, in_specs=in_specs, out_specs=tok_spec, check_vma=False)
```

```python
import functools

import jax
import jax.numpy as jnp
from jax import lax
from jax.experimental import pallas as pl
from jax.experimental.pallas import tpu as pltpu
from jax.sharding import PartitionSpec as P

RMS_EPS = 1e-6
LANES = 128
PITCH = 20
PAD = 4
TILES = (64, 256, 320, 384, 512)
SLOTS = 3
F32 = jnp.float32
BF16 = jnp.bfloat16
NT = (((1,), (1,)), ((), ()))
TN = (((0,), (0,)), ((), ()))
MESH = pl.DeviceIdType.MESH


def place():
    ep, y = lax.axis_index("ep"), lax.axis_index("tp")
    return ep // 2, ep % 2, y, lax.axis_size("ep") // 2, lax.axis_size("tp")


def peer(x, core, y):
    return {"ep": 2 * x + core, "tp": y}


def remote(src, dst, send, recv, where):
    return pltpu.make_async_remote_copy(src_ref=src, dst_ref=dst, send_sem=send, recv_sem=recv,
                                        device_id=where, device_id_type=MESH)


def meet(peers):
    barrier = pltpu.get_barrier_semaphore()
    for p in peers:
        pl.semaphore_signal(barrier, inc=1, device_id=p, device_id_type=MESH)
    pl.semaphore_wait(barrier, len(peers))


def token_pair(x, gain, sigw, cols_ref, n_exp, width, up_at):
    xf = x.astype(F32)
    inv = lax.rsqrt(jnp.mean(xf * xf, axis=-1, keepdims=True) + RMS_EPS)
    h = (xf * inv * gain.astype(F32)).astype(BF16)
    sig = jax.nn.sigmoid(jnp.sum(h.astype(F32) * sigw.astype(F32), axis=-1, keepdims=True))
    return h, sig


def pair_dots(h, cols_ref, n_exp, width, up_at):
    out = lax.dot_general(cols_ref[...], h, NT, preferred_element_type=F32)
    logits = out[:n_exp]
    ex = jnp.exp(logits - jnp.max(logits, axis=0, keepdims=True))
    prob = ex / jnp.sum(ex, axis=0, keepdims=True)
    act = (jax.nn.silu(out[n_exp:n_exp + width]) * out[up_at:up_at + width]).astype(BF16)
    return prob, act


def routing_lists(idx_t, first, n_local, lst_ref, cnt_ref):
    n_tok = idx_t.shape[1]
    n_hi = n_tok // LANES
    sub = lax.broadcasted_iota(jnp.int32, (n_local, n_tok), 0)
    member = jnp.zeros((n_local, n_tok), F32)
    for e in range(n_local):
        hit = jnp.sum((idx_t == first + e).astype(F32), axis=0, keepdims=True)
        member = jnp.where(sub == e, hit, member)
    tri = (lax.broadcasted_iota(jnp.int32, (LANES, LANES), 0)
           < lax.broadcasted_iota(jnp.int32, (LANES, LANES), 1)).astype(F32).astype(BF16)
    base = jnp.zeros((n_local, 1), F32)
    parts = []
    for b in range(n_hi):
        m_b = member[:, b * LANES:(b + 1) * LANES]
        parts.append(jnp.dot(m_b.astype(BF16), tri, preferred_element_type=F32) + base)
        base = base + jnp.sum(m_b, axis=-1, keepdims=True)
    pos = jnp.concatenate(parts, axis=1).astype(jnp.int32)
    cnt_ref[...] = jnp.broadcast_to(base, cnt_ref.shape).astype(jnp.int32)
    tok = lax.broadcasted_iota(jnp.int32, (n_hi, n_tok), 1)
    hi_id = lax.broadcasted_iota(jnp.int32, (n_hi, n_tok), 0)
    lo_id = lax.broadcasted_iota(jnp.int32, (LANES, n_tok), 0)
    row_id = (lax.broadcasted_iota(jnp.int32, (n_hi, LANES), 0) * LANES
              + lax.broadcasted_iota(jnp.int32, (n_hi, LANES), 1))
    tok_hi = (tok >> 3).astype(F32)
    tok_lo = (tok & 7).astype(F32)
    for e in range(n_local):
        p_e = pos[e:e + 1, :]
        here = ((p_e >> 7) == hi_id) & (member[e:e + 1, :] > 0.0)
        lo_hot = jnp.where((p_e & (LANES - 1)) == lo_id, 1.0, 0.0).astype(BF16)
        lhs = jnp.concatenate([jnp.where(here, v, 0.0) for v in (tok_hi, tok_lo)], axis=0).astype(BF16)
        got = lax.dot_general(lhs, lo_hot, NT, preferred_element_type=F32)
        t_of = (got[:n_hi] * 8.0 + got[n_hi:]).astype(jnp.int32)
        valid = row_id < base[e:e + 1, :].astype(jnp.int32)
        lst_ref[e * n_hi:(e + 1) * n_hi, :] = jnp.where(valid, t_of, n_tok)


def gather_kernel(n_local, x_hbm, idx_hbm, gain_ref, rw_ref, sigw_ref, shg_ref, shu_ref,
                  h_hbm, act_ref, sigv_ref, lst_ref, wl_ref, cnt_ref,
                  tok, idx, cols, prob, hbuf, in_sem, send, recv, isend, irecv, out_sem):
    x, core, y, n_x, n_y = place()
    n_exp, width = rw_ref.shape[0], shg_ref.shape[0]
    up_at = n_exp + (width + 15) // 16 * 16
    rows = x_hbm.shape[0]
    half, piece = rows // 2, rows // 8
    own = 2 * x + core
    load_x = pltpu.make_async_copy(x_hbm, tok.at[own], in_sem.at[0])
    load_i = pltpu.make_async_copy(idx_hbm, idx.at[own], in_sem.at[1])
    load_x.start()
    load_i.start()

    def at(v, n):
        return lax.rem(v + n, n)

    right, left, far = at(x + 1, n_x), at(x - 1, n_x), at(x + 2, n_x)
    up, down = at(y + 1, n_y), at(y - 1, n_y)
    others = [peer(x, 1 - core, y)]
    for d in (right, left, far):
        for c in (core, 1 - core):
            others.append(peer(d, c, y))
    meet(others + [peer(x, core, up), peer(x, core, down)])
    load_x.wait()
    load_i.wait()

    started = []
    count = [0]

    def copy(block, row, n_rows, where):
        k = count[0]
        count[0] += 1
        row = pl.multiple_of(row, piece)
        ref = tok.at[block, pl.ds(row, n_rows), :]
        c = remote(ref, ref, send.at[k], recv.at[k], where)
        return c

    def go(c):
        c.start()
        started.append(c)
        return c

    mine = (y % 2) * half
    m = [mine + k * piece for k in range(4)]
    o = [half - mine + k * piece for k in range(4)]
    to_right, to_left = peer(right, core, y), peer(left, core, y)
    to_up, to_down, to_mate = peer(x, core, up), peer(x, core, down), peer(x, 1 - core, y)
    from_left, from_right = {}, {}
    for k in range(4):
        from_left[k] = go(copy(own, m[k], piece, to_right))
        from_right[k ^ 2] = go(copy(own, m[k ^ 2], piece, to_left))
    s_mate = go(copy(own, 0, rows, to_mate))
    icopies = []
    for k, p in enumerate(others):
        c = remote(idx.at[own], idx.at[own], isend.at[k], irecv.at[k], p)
        c.start()
        icopies.append(c)

    cols[...] = jnp.zeros_like(cols)
    cols[:n_exp, :] = rw_ref[...]
    cols[n_exp:n_exp + width, :] = shg_ref[...]
    cols[up_at:up_at + width, :] = shu_ref[...]

    outs = []

    def pair(slot, px):
        for c in range(2):
            h, sig = token_pair(tok[2 * px + c], gain_ref[...], sigw_ref[...], cols, n_exp, width, up_at)
            hbuf[slot, c * rows:(c + 1) * rows, :] = h
            sigv_ref[pl.ds(pl.multiple_of((2 * px + c) * rows, rows), rows), :] = sig
        out = pltpu.make_async_copy(hbuf.at[slot], h_hbm.at[pl.ds(pl.multiple_of(2 * px * rows, 2 * rows), 2 * rows), :],
                                    out_sem.at[slot])
        p, a = pair_dots(hbuf[slot], cols, n_exp, width, up_at)
        prob[px] = p
        act_ref[:, pl.ds(pl.multiple_of(px * 2 * rows, 2 * rows), 2 * rows)] = a
        out.start()
        outs.append(out)

    lb, rb, fb = 2 * left + core, 2 * right + core, 2 * far + core
    mate = {lb_name: [] for lb_name in "lrf"}
    along_y, forward = {}, {}

    def relay(name, block, k, arrived, onward=None):
        arrived.wait_recv()
        if onward is not None:
            forward[k] = go(copy(block, m[k], piece, onward))
        along_y[name, k] = go(copy(block, m[k], piece, to_up if k < 2 else to_down))
        mate[name].append(go(copy(block, m[k], piece, to_mate)))

    def pass_on(name, block, k):
        along_y[name, k].wait_recv()
        mate[name].append(go(copy(block, o[k], piece, to_mate)))

    def arrived_all(name):
        for c in mate[name]:
            c.wait_recv()

    relay("l", lb, 0, from_left[0], to_right)
    relay("r", rb, 2, from_right[2], to_left)
    relay("l", lb, 1, from_left[1], to_right)
    relay("r", rb, 3, from_right[3], to_left)
    s_mate.wait_recv()
    pair(0, x)
    relay("l", lb, 2, from_left[2])
    relay("r", rb, 0, from_right[0])
    pass_on("l", lb, 0)
    pass_on("r", rb, 2)
    relay("l", lb, 3, from_left[3])
    relay("r", rb, 1, from_right[1])
    pass_on("l", lb, 1)
    pass_on("r", rb, 3)
    relay("f", fb, 0, forward[0])
    relay("f", fb, 2, forward[2])
    pass_on("l", lb, 2)
    pass_on("r", rb, 0)
    relay("f", fb, 1, forward[1])
    relay("f", fb, 3, forward[3])
    pass_on("l", lb, 3)
    pass_on("r", rb, 1)
    arrived_all("l")
    pair(1, left)
    pass_on("f", fb, 0)
    pass_on("f", fb, 2)
    arrived_all("r")
    pair(2, right)
    pass_on("f", fb, 1)
    pass_on("f", fb, 3)
    first = pl.multiple_of(own * n_local, n_local)
    for c in icopies:
        c.wait_recv()
    routing_lists(jnp.concatenate([idx[b] for b in range(2 * n_x)], axis=1), first, n_local, lst_ref, cnt_ref)
    arrived_all("f")
    pair(3, far)
    n_hi = 2 * n_x * rows // LANES
    wl_ref[...] = jnp.zeros_like(wl_ref)
    for b in range(n_x):
        wt = prob[b, pl.ds(first, n_local), :]
        for e in range(n_local):
            for c in range(2):
                wl_ref[e * (n_hi + 1) + 2 * b + c:e * (n_hi + 1) + 2 * b + c + 1, :] = (
                    wt[e:e + 1, c * LANES:(c + 1) * LANES])
    for c in started + icopies:
        c.wait_send()
    for c in outs:
        c.wait()


def run_gather(hidden, idx_t, gain, rw_t, sig_t, shg_t, shu_t, n_local, n_x):
    rows, dim = hidden.shape
    n_tok = rows * 2 * n_x
    n_hi = n_tok // LANES
    n_exp, width = rw_t.shape[0], shg_t.shape[0]
    pad = (width + 15) // 16 * 16
    n_copy = 8 + 1 + 4 + 2 * 12 + 12
    n_peer = 2 * n_x - 1
    vmem = pl.BlockSpec(memory_space=pltpu.VMEM)
    hbm = pl.BlockSpec(memory_space=pl.ANY)
    return pl.pallas_call(
        functools.partial(gather_kernel, n_local),
        out_shape=(jax.ShapeDtypeStruct((n_tok, dim), BF16),
                   jax.ShapeDtypeStruct((width, n_tok), BF16),
                   jax.ShapeDtypeStruct((n_tok, 1), F32),
                   jax.ShapeDtypeStruct((n_local * n_hi, LANES), jnp.int32),
                   jax.ShapeDtypeStruct((n_local * (n_hi + 1), LANES), F32),
                   jax.ShapeDtypeStruct((n_local, LANES), jnp.int32)),
        in_specs=[hbm, hbm] + [vmem] * 5,
        out_specs=[hbm] + [vmem] * 5,
        scratch_shapes=[
            pltpu.VMEM((2 * n_x, rows, dim), BF16),
            pltpu.VMEM((2 * n_x,) + idx_t.shape, jnp.int32),
            pltpu.VMEM((n_exp + 2 * pad, dim), BF16),
            pltpu.VMEM((n_x, n_exp, 2 * rows), F32),
            pltpu.VMEM((n_x, 2 * rows, dim), BF16),
            pltpu.SemaphoreType.DMA((2,)),
            pltpu.SemaphoreType.DMA((n_copy,)),
            pltpu.SemaphoreType.DMA((n_copy,)),
            pltpu.SemaphoreType.DMA((n_peer,)),
            pltpu.SemaphoreType.DMA((n_peer,)),
            pltpu.SemaphoreType.DMA((n_x,)),
        ],
        compiler_params=pltpu.CompilerParams(collective_id=0, has_side_effects=True, vmem_limit_bytes=67_000_000),
        name="gather",
    )(hidden, idx_t, gain, rw_t, sig_t, shg_t, shu_t)


def expert_kernel(lst, wl, cnt, h_hbm, act_ref, sig_ref, shd_ref, wg_hbm, wu_hbm, wd_hbm, out_hbm,
                  h_in, table, acc, wg, wu, wd, xt, xb, fb, active, tile_e, tile_s, tile_r, tile_n,
                  in_sem, w_sem, out_sem):
    n_tok, dim = h_hbm.shape
    n_local = wg_hbm.shape[0]
    n_chunk = dim // LANES
    n_blocks = n_tok // LANES
    big = TILES[-1]
    stride = big + PAD

    def fetch_h(b):
        return pltpu.make_async_copy(h_hbm.at[pl.ds(b * LANES, LANES), :], h_in.at[b], in_sem.at[b])

    def weight_copies(e, s):
        return (pltpu.make_async_copy(wg_hbm.at[e], wg.at[s], w_sem.at[s, 0]),
                pltpu.make_async_copy(wu_hbm.at[e], wu.at[s], w_sem.at[s, 1]),
                pltpu.make_async_copy(wd_hbm.at[e], wd.at[s], w_sem.at[s, 2]))

    for b in range(n_blocks):
        fetch_h(b).start()

    def note(e, carry):
        n, tiles = carry
        total = cnt[e, 0]

        @pl.when(total > 0)
        def _():
            active[n] = e

        def tile(k, t):
            tile_e[t] = e
            tile_s[t] = n
            tile_r[t] = k * big
            tile_n[t] = jnp.minimum(total - k * big, big)
            return t + 1

        return n + jnp.where(total > 0, 1, 0), lax.fori_loop(0, (total + big - 1) // big, tile, tiles)

    n_active, n_tiles = lax.fori_loop(0, n_local, note, (0, 0))
    for s in range(SLOTS - 1):
        @pl.when(s < n_active)
        def _():
            for c in weight_copies(active[s], s):
                c.start()

    acc[n_tok * PITCH:, :] = jnp.zeros((acc.shape[0] - n_tok * PITCH, LANES), F32)
    table[n_tok * PITCH:, :] = jnp.zeros((table.shape[0] - n_tok * PITCH, LANES), F32)

    def shared(b, carry):
        rows = pl.ds(pl.multiple_of(b * LANES, LANES), LANES)
        sig = sig_ref[rows, :]
        for c in range(0, n_chunk, 2):
            sh = sig * lax.dot_general(act_ref[:, rows], shd_ref[:, c * LANES:(c + 2) * LANES], TN,
                                       preferred_element_type=F32)
            for d in range(2):
                acc[pl.ds(b * LANES * PITCH + c + d, LANES, stride=PITCH), :] = sh[:, d * LANES:(d + 1) * LANES]
        return carry

    lax.fori_loop(0, n_blocks, shared, 0)

    def spread(b, carry):
        fetch_h(b).wait()
        for c in range(n_chunk):
            table[pl.ds(b * LANES * PITCH + c, LANES, stride=PITCH), :] = (
                h_in[b, :, c * LANES:(c + 1) * LANES].astype(F32))
        return carry

    lax.fori_loop(0, n_blocks, spread, 0)

    def gather8(e, r0, g):
        base = e * n_tok + r0 + g * 8
        for i in range(8):
            t = lst[base + i]
            row = pl.multiple_of(t * PITCH, 4)
            xt[pl.ds(g * 8 + i, n_chunk, stride=stride), :] = table[pl.ds(row, n_chunk), :]

    def scatter8(e, r0, g):
        where, weight, old, new = [], [], [], []
        base = e * n_tok + r0 + g * 8
        for i in range(8):
            t = lst[base + i]
            where.append(pl.multiple_of(t * PITCH, 4))
            weight.append(wl[e * (n_tok + LANES) + t])
            old.append(acc[pl.ds(where[i], n_chunk), :])
        for i in range(8):
            new.append(old[i] + weight[i] * fb[pl.ds(g * 8 + i, n_chunk, stride=stride), :])
        for i in range(8):
            acc[pl.ds(where[i], n_chunk), :] = new[i]

    def ffn(m, s):
        for c in range(n_chunk):
            xb[:m, c * LANES:(c + 1) * LANES] = xt[c * stride:c * stride + m, :].astype(BF16)
        gate = lax.dot_general(wg[s], xb[:m, :], NT, preferred_element_type=F32)
        up = lax.dot_general(wu[s], xb[:m, :], NT, preferred_element_type=F32)
        act = (jax.nn.silu(gate) * up).astype(BF16)
        for c in range(0, n_chunk, 2):
            f = lax.dot_general(act, wd[s, :, c * LANES:(c + 2) * LANES], TN, preferred_element_type=F32)
            fb[c * stride:c * stride + m, :] = f[:, :LANES]
            fb[(c + 1) * stride:(c + 1) * stride + m, :] = f[:, LANES:]

    @pl.when(n_tiles > 0)
    def _():
        def first(g, carry):
            gather8(tile_e[0], tile_r[0], g)
            return carry

        lax.fori_loop(0, (tile_n[0] + 7) // 8, first, 0)

    def tile_step(i, carry):
        e, k, r0, n = tile_e[i], tile_s[i], tile_r[i], tile_n[i]
        s = lax.rem(k, SLOTS)

        @pl.when(r0 == 0)
        def _():
            ahead = k + SLOTS - 1

            @pl.when(ahead < n_active)
            def _():
                for c in weight_copies(active[ahead], lax.rem(ahead, SLOTS)):
                    c.start()

            for c in weight_copies(e, s):
                c.wait()

        below = 0
        for m in TILES:
            @pl.when((n > below) & (n <= m))
            def _(m=m):
                ffn(m, s)
            below = m

        last = i + 1 >= n_tiles
        nxt = jnp.where(last, i, i + 1)
        e2, r2 = tile_e[nxt], tile_r[nxt]
        n2 = jnp.where(last, 0, tile_n[nxt])
        both = (jnp.minimum(n, n2) + 7) // 8

        def mix(g, c2):
            gather8(e2, r2, g)
            scatter8(e, r0, g)
            return c2

        def more_in(g, c2):
            gather8(e2, r2, g)
            return c2

        def more_out(g, c2):
            scatter8(e, r0, g)
            return c2

        lax.fori_loop(0, both, mix, 0)
        lax.fori_loop(both, (n2 + 7) // 8, more_in, 0)
        lax.fori_loop(both, (n + 7) // 8, more_out, 0)
        return carry

    lax.fori_loop(0, n_tiles, tile_step, 0)

    def write_out(b):
        return pltpu.make_async_copy(h_in.at[b], out_hbm.at[pl.ds(b * LANES, LANES), :], out_sem.at[b])

    def finish(b, carry):
        for c in range(n_chunk):
            h_in[b, :, c * LANES:(c + 1) * LANES] = (
                acc[pl.ds(b * LANES * PITCH + c, LANES, stride=PITCH), :].astype(BF16))
        write_out(b).start()
        return carry

    lax.fori_loop(0, n_blocks, finish, 0)
    for b in range(n_blocks):
        write_out(b).wait()


def run_experts(lst, wl, cnt, h, act, sig, shd, wg, wu, wd):
    n_tok, dim = h.shape
    n_local, width, _ = wg.shape
    n_chunk = dim // LANES
    big = TILES[-1]
    max_tiles = n_local * ((n_tok + big - 1) // big)
    smem = pl.BlockSpec(memory_space=pltpu.SMEM)
    vmem = pl.BlockSpec(memory_space=pltpu.VMEM)
    hbm = pl.BlockSpec(memory_space=pl.ANY)
    return pl.pallas_call(
        expert_kernel,
        out_shape=jax.ShapeDtypeStruct((n_tok, dim), BF16),
        in_specs=[smem] * 3 + [hbm] + [vmem] * 3 + [hbm] * 3,
        out_specs=hbm,
        scratch_shapes=[
            pltpu.VMEM((n_tok // LANES, LANES, dim), BF16),
            pltpu.VMEM(((n_tok + 1) * PITCH, LANES), F32),
            pltpu.VMEM(((n_tok + 1) * PITCH, LANES), F32),
            pltpu.VMEM((SLOTS, width, dim), BF16),
            pltpu.VMEM((SLOTS, width, dim), BF16),
            pltpu.VMEM((SLOTS, width, dim), BF16),
            pltpu.VMEM((n_chunk * (big + PAD), LANES), F32),
            pltpu.VMEM((big, dim), BF16),
            pltpu.VMEM((n_chunk * (big + PAD), LANES), F32),
            pltpu.SMEM((n_local,), jnp.int32),
            pltpu.SMEM((max_tiles,), jnp.int32),
            pltpu.SMEM((max_tiles,), jnp.int32),
            pltpu.SMEM((max_tiles,), jnp.int32),
            pltpu.SMEM((max_tiles,), jnp.int32),
            pltpu.SemaphoreType.DMA((n_tok // LANES,)),
            pltpu.SemaphoreType.DMA((SLOTS, 3)),
            pltpu.SemaphoreType.DMA((n_tok // LANES,)),
        ],
        compiler_params=pltpu.CompilerParams(vmem_limit_bytes=67_000_000),
        name="experts",
    )(lst.reshape(-1), wl.reshape(-1), cnt, h, act, sig, shd, wg, wu, wd)


def reduce_kernel(groups, p_hbm, x_ref, out_ref, mate, own, ra, rb, rc, sems):
    x, core, y, n_x, n_y = place()
    rows, dim = x_ref.shape
    part = rows // n_y
    s_in, s_d, r_d, s_a, r_a, s_b, r_b, s_c, r_c, s_e, r_e = sems

    def at(v, n):
        return lax.rem(v + n, n)

    xs = [at(x + d, n_x) for d in range(4)]
    ys = [at(y + d, n_y) for d in range(4)]
    to_mate = peer(x, 1 - core, y)
    x_peers = [None] + [peer(xs[d], core, y) for d in range(1, 4)]
    y_peers = [None] + [peer(x, core, ys[d]) for d in range(1, 4)]
    mine = pl.ds(pl.multiple_of(y * part, part), part)
    started = []

    def go(c):
        c.start()
        started.append(c)
        return c

    loads, mates = [], []
    for g, (kind, lo, w) in enumerate(groups):
        c = pltpu.make_async_copy(p_hbm.at[:, core, :, lo:lo + w], own[g], s_in.at[g])
        c.start()
        loads.append(c)
    meet([to_mate] + x_peers[1:] + y_peers[1:])
    for g, (kind, lo, w) in enumerate(groups):
        mates.append(go(remote(p_hbm.at[:, 1 - core, :, lo:lo + w], mate[g], s_d.at[g], r_d.at[g], to_mate)))

    def unit(g, d, lo, n):
        if groups[g][0] == "x":
            return own[g].at[xs[d], lo:lo + n, :]
        return own[g].at[:, pl.ds(pl.multiple_of(ys[d] * part, part) + lo, n), :]

    def land(g, k, lo, n):
        return rb[g].at[k, lo:lo + n, :] if groups[g][0] == "x" else rb[g].at[k, :, lo:lo + n, :]

    def first_peers(g):
        return x_peers if groups[g][0] == "x" else y_peers

    def half(g):
        return (rows if groups[g][0] == "x" else part) // 2

    a, b_ind, b_dep, c_sent, e_sent = {}, {}, {}, {}, {}

    def add_mate(g):
        loads[g].wait()
        mates[g].wait_recv()
        own[g][...] = (own[g][...].astype(F32) + mate[g][...].astype(F32)).astype(BF16)
        h = half(g)
        for k, (lo, d) in enumerate(((0, 1), (h, 3))):
            a[g, k] = go(remote(unit(g, 2, lo, h), ra[g].at[k], s_a.at[g, k], r_a.at[g, k], first_peers(g)[d]))

    def send_near(g):
        h = half(g)
        for k, (lo, d) in enumerate(((h, 1), (0, 3))):
            b_ind[g, k] = go(remote(unit(g, d, lo, h), land(g, k, lo, h), s_b.at[g, k, 0], r_b.at[g, k, 0],
                                    first_peers(g)[d]))

    def add_far(g):
        h = half(g)
        for k, (lo, d) in enumerate(((0, 1), (h, 3))):
            a[g, k].wait_recv()
            ref = unit(g, d, lo, h)
            ref[...] = (ref[...].astype(F32) + ra[g][k].astype(F32)).astype(BF16)
            b_dep[g, k] = go(remote(ref, land(g, k, lo, h), s_b.at[g, k, 1], r_b.at[g, k, 1], first_peers(g)[d]))

    def second_axis(g):
        for k in range(2):
            b_ind[g, k].wait_recv()
            b_dep[g, k].wait_recv()
        ref = unit(g, 0, 0, 2 * half(g))
        ref[...] = (ref[...].astype(F32) + rb[g][0].astype(F32) + rb[g][1].astype(F32)).astype(BF16)
        for d in (2, 1, 3):
            if groups[g][0] == "x":
                src = own[g].at[x, pl.ds(pl.multiple_of(ys[d] * part, part), part), :]
                where = y_peers[d]
            else:
                src = own[g].at[xs[d], mine, :]
                where = x_peers[d]
            c_sent[g, d] = go(remote(src, rc[g].at[d - 1], s_c.at[g, d - 1], r_c.at[g, d - 1], where))

    def finish(g):
        kind, lo, w = groups[g]
        total = own[g][x, mine, :].astype(F32)
        for d in (1, 3, 2):
            c_sent[g, d].wait_recv()
            total = total + rc[g][d - 1].astype(F32)
        cols = slice(lo, lo + w)
        out_ref[mine, cols] = (x_ref[mine, cols].astype(F32) + total).astype(BF16)
        for d in (2, 1, 3):
            ref = out_ref.at[mine, cols]
            e_sent[g, d] = go(remote(ref, ref, s_e.at[g, d - 1], r_e.at[g, d - 1], y_peers[d]))

    order = ((add_mate, 0), (send_near, 0), (add_mate, 1), (send_near, 1), (add_mate, 2), (add_far, 0), (send_near, 2),
             (add_far, 1), (add_mate, 3), (add_far, 2), (second_axis, 1), (send_near, 3), (second_axis, 0),
             (add_mate, 4), (add_far, 3), (finish, 1), (send_near, 4), (second_axis, 2), (finish, 0), (add_far, 4),
             (second_axis, 3), (finish, 2), (second_axis, 4), (finish, 3), (finish, 4))
    for step, g in order:
        step(g)
    for g in range(len(groups)):
        for d in range(1, 4):
            e_sent[g, d].wait_recv()
    for c in started:
        c.wait_send()


def run_reduce(partial, hidden, n_x, n_y):
    rows, dim = hidden.shape
    q = dim // 8
    groups = (("x", 0, 2 * q), ("y", 2 * q, 2 * q), ("x", 4 * q, 2 * q), ("x", 6 * q, q), ("x", 7 * q, q))
    n_g = len(groups)
    part = rows // n_y
    dma = pltpu.SemaphoreType.DMA

    def per_group(of):
        return [pltpu.VMEM(of(kind, w), BF16) for kind, _, w in groups]

    def kernel(p, xr, o, *rest):
        lists = [rest[k * n_g:(k + 1) * n_g] for k in range(5)]
        reduce_kernel(groups, p, xr, o, *lists, rest[5 * n_g:])

    return pl.pallas_call(
        kernel,
        out_shape=jax.ShapeDtypeStruct((rows, dim), BF16),
        in_specs=[pl.BlockSpec(memory_space=pl.ANY), pl.BlockSpec(memory_space=pltpu.VMEM)],
        out_specs=pl.BlockSpec(memory_space=pltpu.VMEM),
        scratch_shapes=(
            per_group(lambda kind, w: (n_x, rows, w)) + per_group(lambda kind, w: (n_x, rows, w))
            + per_group(lambda kind, w: (2, rows // 2, w) if kind == "x" else (2, n_x, part // 2, w))
            + per_group(lambda kind, w: (2, rows, w) if kind == "x" else (2, n_x, part, w))
            + per_group(lambda kind, w: (3, part, w))
            + [dma((n_g,)), dma((n_g,)), dma((n_g,)), dma((n_g, 2)), dma((n_g, 2)), dma((n_g, 2, 2)),
               dma((n_g, 2, 2)), dma((n_g, 3)), dma((n_g, 3)), dma((n_g, 3)), dma((n_g, 3))]),
        compiler_params=pltpu.CompilerParams(collective_id=1, has_side_effects=True, vmem_limit_bytes=67_000_000),
        name="reduce",
    )(partial.reshape(n_x, 2, rows, dim), hidden)


def solution(mesh):
    tok_spec = P(('dp', 'ep'), None)
    in_specs = (tok_spec, tok_spec, P(None), P(None, None), P(None, None),
                P('ep', None, 'tp'), P('ep', None, 'tp'), P('ep', 'tp', None),
                P(None, ('tp', 'ep')), P(None, ('tp', 'ep')), P(('tp', 'ep'), None))
    n_x, n_y = mesh.shape['ep'] // 2, mesh.shape['tp']
    assert n_x == 4 and n_y == 4

    def local_step(hidden_in, topk_idx, norm_gain, router_w, shared_sig_w, exp_gate, exp_up, exp_down,
                   sh_gate, sh_up, sh_down):
        h, act, sig, lst, wl, cnt = run_gather(
            hidden_in, topk_idx.T, norm_gain.reshape(1, -1), router_w.T, shared_sig_w.T, sh_gate.T, sh_up.T,
            exp_gate.shape[0], n_x)
        partial = run_experts(lst, wl, cnt, h, act, sig, sh_down,
                              jnp.swapaxes(exp_gate, 1, 2), jnp.swapaxes(exp_up, 1, 2), exp_down)
        return run_reduce(partial, hidden_in, n_x, n_y)

    return jax.shard_map(local_step, mesh=mesh, in_specs=in_specs, out_specs=tok_spec, check_vma=False)
```

```python
import functools

import jax
import jax.numpy as jnp
from jax import lax
from jax.experimental import pallas as pl
from jax.experimental.pallas import tpu as pltpu
from jax.sharding import PartitionSpec as P

RMS_EPS = 1e-6
LANES = 128
PITCH = 20
PAD = 4
TILES = (64, 256, 320, 384, 512)
SLOTS = 3
F32 = jnp.float32
BF16 = jnp.bfloat16
NT = (((1,), (1,)), ((), ()))
TN = (((0,), (0,)), ((), ()))
MESH = pl.DeviceIdType.MESH


def place():
    ep, y = lax.axis_index("ep"), lax.axis_index("tp")
    return ep // 2, ep % 2, y, lax.axis_size("ep") // 2, lax.axis_size("tp")


def peer(x, core, y):
    return {"ep": 2 * x + core, "tp": y}


def remote(src, dst, send, recv, where):
    return pltpu.make_async_remote_copy(src_ref=src, dst_ref=dst, send_sem=send, recv_sem=recv,
                                        device_id=where, device_id_type=MESH)


def meet(peers):
    barrier = pltpu.get_barrier_semaphore()
    for p in peers:
        pl.semaphore_signal(barrier, inc=1, device_id=p, device_id_type=MESH)
    pl.semaphore_wait(barrier, len(peers))


def token_pair(x, gain, sigw, cols_ref, n_exp, width, up_at):
    xf = x.astype(F32)
    inv = lax.rsqrt(jnp.mean(xf * xf, axis=-1, keepdims=True) + RMS_EPS)
    h = (xf * inv * gain.astype(F32)).astype(BF16)
    sig = jax.nn.sigmoid(jnp.sum(h.astype(F32) * sigw.astype(F32), axis=-1, keepdims=True))
    return h, sig


def pair_dots(h, cols_ref, n_exp, width, up_at):
    out = lax.dot_general(cols_ref[...], h, NT, preferred_element_type=F32)
    logits = out[:n_exp]
    ex = jnp.exp(logits - jnp.max(logits, axis=0, keepdims=True))
    prob = ex / jnp.sum(ex, axis=0, keepdims=True)
    act = (jax.nn.silu(out[n_exp:n_exp + width]) * out[up_at:up_at + width]).astype(BF16)
    return prob, act


def routing_lists(idx_t, first, n_local, lst_ref, cnt_ref):
    n_tok = idx_t.shape[1]
    n_hi = n_tok // LANES
    sub = lax.broadcasted_iota(jnp.int32, (n_local, n_tok), 0)
    member = jnp.zeros((n_local, n_tok), F32)
    for e in range(n_local):
        hit = jnp.sum((idx_t == first + e).astype(F32), axis=0, keepdims=True)
        member = jnp.where(sub == e, hit, member)
    tri = (lax.broadcasted_iota(jnp.int32, (LANES, LANES), 0)
           < lax.broadcasted_iota(jnp.int32, (LANES, LANES), 1)).astype(F32).astype(BF16)
    base = jnp.zeros((n_local, 1), F32)
    parts = []
    for b in range(n_hi):
        m_b = member[:, b * LANES:(b + 1) * LANES]
        parts.append(jnp.dot(m_b.astype(BF16), tri, preferred_element_type=F32) + base)
        base = base + jnp.sum(m_b, axis=-1, keepdims=True)
    pos = jnp.concatenate(parts, axis=1).astype(jnp.int32)
    cnt_ref[...] = jnp.broadcast_to(base, cnt_ref.shape).astype(jnp.int32)
    tok = lax.broadcasted_iota(jnp.int32, (n_hi, n_tok), 1)
    hi_id = lax.broadcasted_iota(jnp.int32, (n_hi, n_tok), 0)
    lo_id = lax.broadcasted_iota(jnp.int32, (LANES, n_tok), 0)
    row_id = (lax.broadcasted_iota(jnp.int32, (n_hi, LANES), 0) * LANES
              + lax.broadcasted_iota(jnp.int32, (n_hi, LANES), 1))
    tok_hi = (tok >> 3).astype(F32)
    tok_lo = (tok & 7).astype(F32)
    for e in range(n_local):
        p_e = pos[e:e + 1, :]
        here = ((p_e >> 7) == hi_id) & (member[e:e + 1, :] > 0.0)
        lo_hot = jnp.where((p_e & (LANES - 1)) == lo_id, 1.0, 0.0).astype(BF16)
        lhs = jnp.concatenate([jnp.where(here, v, 0.0) for v in (tok_hi, tok_lo)], axis=0).astype(BF16)
        got = lax.dot_general(lhs, lo_hot, NT, preferred_element_type=F32)
        t_of = (got[:n_hi] * 8.0 + got[n_hi:]).astype(jnp.int32)
        valid = row_id < base[e:e + 1, :].astype(jnp.int32)
        lst_ref[e * n_hi:(e + 1) * n_hi, :] = jnp.where(valid, t_of, n_tok)


def gather_kernel(n_local, x_hbm, idx_hbm, gain_ref, rw_ref, sigw_ref, shg_ref, shu_ref,
                  h_hbm, act_ref, sigv_ref, lst_ref, wl_ref, cnt_ref,
                  tok, idx, cols, prob, hbuf, in_sem, send, recv, isend, irecv, out_sem):
    x, core, y, n_x, n_y = place()
    n_exp, width = rw_ref.shape[0], shg_ref.shape[0]
    up_at = n_exp + (width + 15) // 16 * 16
    rows = x_hbm.shape[0]
    half, piece = rows // 2, rows // 8
    own = 2 * x + core
    load_x = pltpu.make_async_copy(x_hbm, tok.at[own], in_sem.at[0])
    load_i = pltpu.make_async_copy(idx_hbm, idx.at[own], in_sem.at[1])
    load_x.start()
    load_i.start()

    def at(v, n):
        return lax.rem(v + n, n)

    right, left, far = at(x + 1, n_x), at(x - 1, n_x), at(x + 2, n_x)
    up, down = at(y + 1, n_y), at(y - 1, n_y)
    others = [peer(x, 1 - core, y)]
    for d in (right, left, far):
        for c in (core, 1 - core):
            others.append(peer(d, c, y))
    meet(others + [peer(x, core, up), peer(x, core, down)])
    load_x.wait()
    load_i.wait()

    started = []
    count = [0]

    def copy(block, row, n_rows, where):
        k = count[0]
        count[0] += 1
        row = pl.multiple_of(row, piece)
        ref = tok.at[block, pl.ds(row, n_rows), :]
        c = remote(ref, ref, send.at[k], recv.at[k], where)
        return c

    def go(c):
        c.start()
        started.append(c)
        return c

    mine = (y % 2) * half
    m = [mine + k * piece for k in range(4)]
    o = [half - mine + k * piece for k in range(4)]
    to_right, to_left = peer(right, core, y), peer(left, core, y)
    to_up, to_down, to_mate = peer(x, core, up), peer(x, core, down), peer(x, 1 - core, y)
    from_left, from_right = {}, {}
    for k in range(4):
        from_left[k] = go(copy(own, m[k], piece, to_right))
        from_right[k ^ 2] = go(copy(own, m[k ^ 2], piece, to_left))
    s_mate = go(copy(own, 0, rows, to_mate))
    icopies = []
    for k, p in enumerate(others):
        c = remote(idx.at[own], idx.at[own], isend.at[k], irecv.at[k], p)
        c.start()
        icopies.append(c)

    cols[...] = jnp.zeros_like(cols)
    cols[:n_exp, :] = rw_ref[...]
    cols[n_exp:n_exp + width, :] = shg_ref[...]
    cols[up_at:up_at + width, :] = shu_ref[...]

    outs = []

    def pair(slot, px):
        for c in range(2):
            h, sig = token_pair(tok[2 * px + c], gain_ref[...].astype(F32).reshape(1, -1), sigw_ref[...], cols, n_exp, width, up_at)
            hbuf[slot, c * rows:(c + 1) * rows, :] = h
            sigv_ref[pl.ds(pl.multiple_of((2 * px + c) * rows, rows), rows), :] = sig
        out = pltpu.make_async_copy(hbuf.at[slot], h_hbm.at[pl.ds(pl.multiple_of(2 * px * rows, 2 * rows), 2 * rows), :],
                                    out_sem.at[slot])
        p, a = pair_dots(hbuf[slot], cols, n_exp, width, up_at)
        prob[px] = p
        act_ref[:, pl.ds(pl.multiple_of(px * 2 * rows, 2 * rows), 2 * rows)] = a
        out.start()
        outs.append(out)

    lb, rb, fb = 2 * left + core, 2 * right + core, 2 * far + core
    mate = {lb_name: [] for lb_name in "lrf"}
    along_y, forward = {}, {}

    def relay(name, block, k, arrived, onward=None):
        arrived.wait_recv()
        if onward is not None:
            forward[k] = go(copy(block, m[k], piece, onward))
        along_y[name, k] = go(copy(block, m[k], piece, to_up if k < 2 else to_down))
        mate[name].append(go(copy(block, m[k], piece, to_mate)))

    def pass_on(name, block, k):
        along_y[name, k].wait_recv()
        mate[name].append(go(copy(block, o[k], piece, to_mate)))

    def arrived_all(name):
        for c in mate[name]:
            c.wait_recv()

    relay("l", lb, 0, from_left[0], to_right)
    relay("r", rb, 2, from_right[2], to_left)
    relay("l", lb, 1, from_left[1], to_right)
    relay("r", rb, 3, from_right[3], to_left)
    s_mate.wait_recv()
    pair(0, x)
    relay("l", lb, 2, from_left[2])
    relay("r", rb, 0, from_right[0])
    pass_on("l", lb, 0)
    pass_on("r", rb, 2)
    relay("l", lb, 3, from_left[3])
    relay("r", rb, 1, from_right[1])
    pass_on("l", lb, 1)
    pass_on("r", rb, 3)
    relay("f", fb, 0, forward[0])
    relay("f", fb, 2, forward[2])
    pass_on("l", lb, 2)
    pass_on("r", rb, 0)
    relay("f", fb, 1, forward[1])
    relay("f", fb, 3, forward[3])
    pass_on("l", lb, 3)
    pass_on("r", rb, 1)
    arrived_all("l")
    pair(1, left)
    pass_on("f", fb, 0)
    pass_on("f", fb, 2)
    arrived_all("r")
    pair(2, right)
    pass_on("f", fb, 1)
    pass_on("f", fb, 3)
    first = pl.multiple_of(own * n_local, n_local)
    lst_rows = 2 * n_x * rows // LANES
    lst_ref[n_local * lst_rows:, :] = jnp.full((lst_ref.shape[0] - n_local * lst_rows, LANES), 2 * n_x * rows, jnp.int32)
    for c in icopies:
        c.wait_recv()
    routing_lists(jnp.concatenate([idx[b] for b in range(2 * n_x)], axis=1), first, n_local, lst_ref, cnt_ref)
    arrived_all("f")
    pair(3, far)
    n_hi = 2 * n_x * rows // LANES
    wl_ref[...] = jnp.zeros_like(wl_ref)
    for b in range(n_x):
        wt = prob[b, pl.ds(first, n_local), :]
        for e in range(n_local):
            for c in range(2):
                wl_ref[e * (n_hi + 1) + 2 * b + c:e * (n_hi + 1) + 2 * b + c + 1, :] = (
                    wt[e:e + 1, c * LANES:(c + 1) * LANES])
    for c in started + icopies:
        c.wait_send()
    for c in outs:
        c.wait()


def run_gather(hidden, idx_t, gain, rw_t, sig_t, shg_t, shu_t, n_local, n_x):
    rows, dim = hidden.shape
    n_tok = rows * 2 * n_x
    n_hi = n_tok // LANES
    n_exp, width = rw_t.shape[0], shg_t.shape[0]
    pad = (width + 15) // 16 * 16
    n_copy = 8 + 1 + 4 + 2 * 12 + 12
    n_peer = 2 * n_x - 1
    vmem = pl.BlockSpec(memory_space=pltpu.VMEM)
    hbm = pl.BlockSpec(memory_space=pl.ANY)
    return pl.pallas_call(
        functools.partial(gather_kernel, n_local),
        out_shape=(jax.ShapeDtypeStruct((n_tok, dim), BF16),
                   jax.ShapeDtypeStruct((width, n_tok), BF16),
                   jax.ShapeDtypeStruct((n_tok, 1), F32),
                   jax.ShapeDtypeStruct(((n_local + 1) * n_hi, LANES), jnp.int32),
                   jax.ShapeDtypeStruct((n_local * (n_hi + 1), LANES), F32),
                   jax.ShapeDtypeStruct((n_local, LANES), jnp.int32)),
        in_specs=[hbm, hbm] + [vmem] * 5,
        out_specs=[hbm] + [vmem] * 5,
        scratch_shapes=[
            pltpu.VMEM((2 * n_x, rows, dim), BF16),
            pltpu.VMEM((2 * n_x,) + idx_t.shape, jnp.int32),
            pltpu.VMEM((n_exp + 2 * pad, dim), BF16),
            pltpu.VMEM((n_x, n_exp, 2 * rows), F32),
            pltpu.VMEM((n_x, 2 * rows, dim), BF16),
            pltpu.SemaphoreType.DMA((2,)),
            pltpu.SemaphoreType.DMA((n_copy,)),
            pltpu.SemaphoreType.DMA((n_copy,)),
            pltpu.SemaphoreType.DMA((n_peer,)),
            pltpu.SemaphoreType.DMA((n_peer,)),
            pltpu.SemaphoreType.DMA((n_x,)),
        ],
        compiler_params=pltpu.CompilerParams(collective_id=0, has_side_effects=True, vmem_limit_bytes=67_000_000),
        name="gather",
    )(hidden, idx_t, gain, rw_t, sig_t, shg_t, shu_t)


def expert_kernel(lst, wl, cnt, h_hbm, act_ref, sig_ref, shd_ref, wg_hbm, wu_hbm, wd_hbm, out_hbm,
                  h_in, table, acc, wg, wu, wd, xt, xb, fb, active, tile_e, tile_s, tile_r, tile_n,
                  in_sem, w_sem, out_sem):
    n_tok, dim = h_hbm.shape
    n_local = wg_hbm.shape[0]
    n_chunk = dim // LANES
    n_blocks = n_tok // LANES
    big = TILES[-1]
    stride = big + PAD

    def fetch_h(b):
        return pltpu.make_async_copy(h_hbm.at[pl.ds(b * LANES, LANES), :], h_in.at[b], in_sem.at[b])

    def weight_copies(e, s):
        return (pltpu.make_async_copy(wg_hbm.at[e], wg.at[s], w_sem.at[s, 0]),
                pltpu.make_async_copy(wu_hbm.at[e], wu.at[s], w_sem.at[s, 1]),
                pltpu.make_async_copy(wd_hbm.at[e], wd.at[s], w_sem.at[s, 2]))

    for b in range(n_blocks):
        fetch_h(b).start()

    def note(e, carry):
        n, tiles = carry
        total = cnt[e, 0]

        @pl.when(total > 0)
        def _():
            active[n] = e

        def tile(k, t):
            tile_e[t] = e
            tile_s[t] = n
            tile_r[t] = k * big
            tile_n[t] = jnp.minimum(total - k * big, big)
            return t + 1

        return n + jnp.where(total > 0, 1, 0), lax.fori_loop(0, (total + big - 1) // big, tile, tiles)

    n_active, n_tiles = lax.fori_loop(0, n_local, note, (0, 0))
    for s in range(SLOTS - 1):
        @pl.when(s < n_active)
        def _():
            for c in weight_copies(active[s], s):
                c.start()

    acc[n_tok * PITCH:, :] = jnp.zeros((acc.shape[0] - n_tok * PITCH, LANES), F32)
    table[n_tok * PITCH:, :] = jnp.zeros((table.shape[0] - n_tok * PITCH, LANES), F32)

    def shared(b, carry):
        rows = pl.ds(pl.multiple_of(b * LANES, LANES), LANES)
        sig = sig_ref[rows, :]
        for c in range(0, n_chunk, 2):
            sh = sig * lax.dot_general(act_ref[:, rows], shd_ref[:, c * LANES:(c + 2) * LANES], TN,
                                       preferred_element_type=F32)
            for d in range(2):
                acc[pl.ds(b * LANES * PITCH + c + d, LANES, stride=PITCH), :] = sh[:, d * LANES:(d + 1) * LANES]
        return carry

    lax.fori_loop(0, n_blocks, shared, 0)

    def spread(b, carry):
        fetch_h(b).wait()
        for c in range(n_chunk):
            table[pl.ds(b * LANES * PITCH + c, LANES, stride=PITCH), :] = (
                h_in[b, :, c * LANES:(c + 1) * LANES].astype(F32))
        return carry

    lax.fori_loop(0, n_blocks, spread, 0)

    def gather8(base, g):
        for i in range(8):
            row = pl.multiple_of(lst[base + g * 8 + i] * PITCH, 4)
            xt[pl.ds(g * 8 + i, n_chunk, stride=stride), :] = table[pl.ds(row, n_chunk), :]

    def scatter8(f_at, w_at, base, g):
        where, weight, old, new = [], [], [], []
        for i in range(8):
            t = lst[base + g * 8 + i]
            where.append(pl.multiple_of(t * PITCH, 4))
            weight.append(wl[w_at + t])
            old.append(acc[pl.ds(where[i], n_chunk), :])
        for i in range(8):
            new.append(old[i] + weight[i] * fb[pl.ds(f_at + g * 8 + i, n_chunk, stride=stride), :])
        for i in range(8):
            acc[pl.ds(where[i], n_chunk), :] = new[i]

    def ffn(m, s, f_at, moves):
        for c in range(n_chunk):
            xb[:m, c * LANES:(c + 1) * LANES] = xt[c * stride:c * stride + m, :].astype(BF16)
        n_move = len(moves)
        done = 0

        def some(upto):
            nonlocal done
            while done < upto:
                moves[done]()
                done += 1

        gate = lax.dot_general(wg[s], xb[:m, :], NT, preferred_element_type=F32)
        some(n_move * 3 // 10)
        up = lax.dot_general(wu[s], xb[:m, :], NT, preferred_element_type=F32)
        some(n_move * 6 // 10)
        act = (jax.nn.silu(gate) * up).astype(BF16)
        for c in range(0, n_chunk, 2):
            f = lax.dot_general(act, wd[s, :, c * LANES:(c + 2) * LANES], TN, preferred_element_type=F32)
            yield_at = n_move * 6 // 10 + (n_move - n_move * 6 // 10) * (c + 2) // n_chunk
            for d in range(2):
                fb[pl.ds(f_at + (c + d) * stride, m), :] = f[:, d * LANES:(d + 1) * LANES]
            some(yield_at)

    @pl.when(n_tiles > 0)
    def _():
        def first(g, carry):
            gather8(tile_e[0] * n_tok + tile_r[0], g)
            return carry

        lax.fori_loop(0, (tile_n[0] + 7) // 8, first, 0)

    def tile_step(i, carry):
        e, k, r0, n = tile_e[i], tile_s[i], tile_r[i], tile_n[i]
        s = lax.rem(k, SLOTS)

        @pl.when(r0 == 0)
        def _():
            ahead = k + SLOTS - 1

            @pl.when(ahead < n_active)
            def _():
                for c in weight_copies(active[ahead], lax.rem(ahead, SLOTS)):
                    c.start()

            for c in weight_copies(e, s):
                c.wait()

        f_size = n_chunk * stride
        f_at = pl.multiple_of(lax.rem(i, 2) * f_size, 8)
        f_prev = pl.multiple_of(lax.rem(i + 1, 2) * f_size, 8)
        before, after = jnp.maximum(i - 1, 0), jnp.minimum(i + 1, n_tiles - 1)
        e1 = tile_e[before]
        w1 = e1 * (n_tok + LANES)
        base1 = jnp.where(i > 0, e1 * n_tok + tile_r[before], n_local * n_tok)
        n1 = jnp.where(i > 0, tile_n[before], 0)
        base2 = tile_e[after] * n_tok + tile_r[after]
        n2 = jnp.where(i + 1 < n_tiles, tile_n[after], 0)
        below = 0
        for m in TILES:
            @pl.when((n > below) & (n <= m))
            def _(m=m):
                moves = []
                for g in range(m // 8):
                    moves.append(functools.partial(gather8, base2, g))
                    moves.append(functools.partial(scatter8, f_prev, w1, base1, g))
                ffn(m, s, f_at, moves)

                def more_in(g, c2):
                    gather8(base2, g)
                    return c2

                def more_out(g, c2):
                    scatter8(f_prev, w1, base1, g)
                    return c2

                lax.fori_loop(m // 8, (n2 + 7) // 8, more_in, 0)
                lax.fori_loop(m // 8, (n1 + 7) // 8, more_out, 0)
            below = m

        return carry

    lax.fori_loop(0, n_tiles, tile_step, 0)

    @pl.when(n_tiles > 0)
    def _():
        i = n_tiles - 1
        f_at = pl.multiple_of(lax.rem(i, 2) * (n_chunk * stride), 8)

        def last(g, carry):
            scatter8(f_at, tile_e[i] * (n_tok + LANES), tile_e[i] * n_tok + tile_r[i], g)
            return carry

        lax.fori_loop(0, (tile_n[i] + 7) // 8, last, 0)

    def write_out(b):
        return pltpu.make_async_copy(h_in.at[b], out_hbm.at[pl.ds(b * LANES, LANES), :], out_sem.at[b])

    def finish(b, carry):
        for c in range(n_chunk):
            h_in[b, :, c * LANES:(c + 1) * LANES] = (
                acc[pl.ds(b * LANES * PITCH + c, LANES, stride=PITCH), :].astype(BF16))
        write_out(b).start()
        return carry

    lax.fori_loop(0, n_blocks, finish, 0)
    for b in range(n_blocks):
        write_out(b).wait()


def run_experts(lst, wl, cnt, h, act, sig, shd, wg, wu, wd):
    n_tok, dim = h.shape
    n_local, width, _ = wg.shape
    n_chunk = dim // LANES
    big = TILES[-1]
    max_tiles = n_local * ((n_tok + big - 1) // big)
    smem = pl.BlockSpec(memory_space=pltpu.SMEM)
    vmem = pl.BlockSpec(memory_space=pltpu.VMEM)
    hbm = pl.BlockSpec(memory_space=pl.ANY)
    return pl.pallas_call(
        expert_kernel,
        out_shape=jax.ShapeDtypeStruct((n_tok, dim), BF16),
        in_specs=[smem] * 3 + [hbm] + [vmem] * 3 + [hbm] * 3,
        out_specs=hbm,
        scratch_shapes=[
            pltpu.VMEM((n_tok // LANES, LANES, dim), BF16),
            pltpu.VMEM(((n_tok + 1) * PITCH, LANES), F32),
            pltpu.VMEM(((n_tok + 1) * PITCH, LANES), F32),
            pltpu.VMEM((SLOTS, width, dim), BF16),
            pltpu.VMEM((SLOTS, width, dim), BF16),
            pltpu.VMEM((SLOTS, width, dim), BF16),
            pltpu.VMEM((n_chunk * (big + PAD), LANES), F32),
            pltpu.VMEM((big, dim), BF16),
            pltpu.VMEM((2 * n_chunk * (big + PAD), LANES), F32),
            pltpu.SMEM((n_local,), jnp.int32),
            pltpu.SMEM((max_tiles,), jnp.int32),
            pltpu.SMEM((max_tiles,), jnp.int32),
            pltpu.SMEM((max_tiles,), jnp.int32),
            pltpu.SMEM((max_tiles,), jnp.int32),
            pltpu.SemaphoreType.DMA((n_tok // LANES,)),
            pltpu.SemaphoreType.DMA((SLOTS, 3)),
            pltpu.SemaphoreType.DMA((n_tok // LANES,)),
        ],
        compiler_params=pltpu.CompilerParams(vmem_limit_bytes=67_000_000),
        name="experts",
    )(lst.reshape(-1), wl.reshape(-1), cnt, h, act, sig, shd, wg, wu, wd)


def reduce_kernel(groups, p_hbm, x_ref, out_ref, mate, own, ra, rb, rc, sems):
    x, core, y, n_x, n_y = place()
    rows, dim = x_ref.shape
    part = rows // n_y
    s_in, s_d, r_d, s_a, r_a, s_b, r_b, s_c, r_c, s_e, r_e = sems

    def at(v, n):
        return lax.rem(v + n, n)

    xs = [at(x + d, n_x) for d in range(4)]
    ys = [at(y + d, n_y) for d in range(4)]
    to_mate = peer(x, 1 - core, y)
    x_peers = [None] + [peer(xs[d], core, y) for d in range(1, 4)]
    y_peers = [None] + [peer(x, core, ys[d]) for d in range(1, 4)]
    mine = pl.ds(pl.multiple_of(y * part, part), part)
    started = []

    def go(c):
        c.start()
        started.append(c)
        return c

    loads, mates = [], []
    for g, (kind, lo, w) in enumerate(groups):
        c = pltpu.make_async_copy(p_hbm.at[:, core, :, lo:lo + w], own[g], s_in.at[g])
        c.start()
        loads.append(c)
    meet([to_mate] + x_peers[1:] + y_peers[1:])
    for g, (kind, lo, w) in enumerate(groups):
        mates.append(go(remote(p_hbm.at[:, 1 - core, :, lo:lo + w], mate[g], s_d.at[g], r_d.at[g], to_mate)))

    def unit(g, d, lo, n):
        if groups[g][0] == "x":
            return own[g].at[xs[d], lo:lo + n, :]
        return own[g].at[:, pl.ds(pl.multiple_of(ys[d] * part, part) + lo, n), :]

    def land(g, k, lo, n):
        return rb[g].at[k, lo:lo + n, :] if groups[g][0] == "x" else rb[g].at[k, :, lo:lo + n, :]

    def first_peers(g):
        return x_peers if groups[g][0] == "x" else y_peers

    def half(g):
        return (rows if groups[g][0] == "x" else part) // 2

    a, b_ind, b_dep, c_sent, e_sent = {}, {}, {}, {}, {}

    def add_mate(g):
        loads[g].wait()
        mates[g].wait_recv()
        own[g][...] = (own[g][...].astype(F32) + mate[g][...].astype(F32)).astype(BF16)
        h = half(g)
        for k, (lo, d) in enumerate(((0, 1), (h, 3))):
            a[g, k] = go(remote(unit(g, 2, lo, h), ra[g].at[k], s_a.at[g, k], r_a.at[g, k], first_peers(g)[d]))

    def send_near(g):
        h = half(g)
        for k, (lo, d) in enumerate(((h, 1), (0, 3))):
            b_ind[g, k] = go(remote(unit(g, d, lo, h), land(g, k, lo, h), s_b.at[g, k, 0], r_b.at[g, k, 0],
                                    first_peers(g)[d]))

    def add_far(g):
        h = half(g)
        for k, (lo, d) in enumerate(((0, 1), (h, 3))):
            a[g, k].wait_recv()
            ref = unit(g, d, lo, h)
            ref[...] = (ref[...].astype(F32) + ra[g][k].astype(F32)).astype(BF16)
            b_dep[g, k] = go(remote(ref, land(g, k, lo, h), s_b.at[g, k, 1], r_b.at[g, k, 1], first_peers(g)[d]))

    def second_axis(g):
        for k in range(2):
            b_ind[g, k].wait_recv()
            b_dep[g, k].wait_recv()
        ref = unit(g, 0, 0, 2 * half(g))
        ref[...] = (ref[...].astype(F32) + rb[g][0].astype(F32) + rb[g][1].astype(F32)).astype(BF16)
        for d in (2, 1, 3):
            if groups[g][0] == "x":
                src = own[g].at[x, pl.ds(pl.multiple_of(ys[d] * part, part), part), :]
                where = y_peers[d]
            else:
                src = own[g].at[xs[d], mine, :]
                where = x_peers[d]
            c_sent[g, d] = go(remote(src, rc[g].at[d - 1], s_c.at[g, d - 1], r_c.at[g, d - 1], where))

    def finish(g):
        kind, lo, w = groups[g]
        total = own[g][x, mine, :].astype(F32)
        for d in (1, 3, 2):
            c_sent[g, d].wait_recv()
            total = total + rc[g][d - 1].astype(F32)
        cols = slice(lo, lo + w)
        out_ref[mine, cols] = (x_ref[mine, cols].astype(F32) + total).astype(BF16)
        for d in (2, 1, 3):
            ref = out_ref.at[mine, cols]
            e_sent[g, d] = go(remote(ref, ref, s_e.at[g, d - 1], r_e.at[g, d - 1], y_peers[d]))

    order = ((add_mate, 0), (send_near, 0), (add_mate, 1), (send_near, 1), (add_mate, 2), (add_far, 0), (send_near, 2),
             (add_far, 1), (add_mate, 3), (add_far, 2), (second_axis, 1), (send_near, 3), (second_axis, 0),
             (add_mate, 4), (add_far, 3), (finish, 1), (send_near, 4), (second_axis, 2), (finish, 0), (add_far, 4),
             (second_axis, 3), (finish, 2), (second_axis, 4), (finish, 3), (finish, 4))
    for step, g in order:
        step(g)
    for g in range(len(groups)):
        for d in range(1, 4):
            e_sent[g, d].wait_recv()
    for c in started:
        c.wait_send()


def run_reduce(partial, hidden, n_x, n_y):
    rows, dim = hidden.shape
    q = dim // 8
    groups = (("x", 0, 2 * q), ("y", 2 * q, 2 * q), ("x", 4 * q, 2 * q), ("x", 6 * q, q), ("x", 7 * q, q))
    n_g = len(groups)
    part = rows // n_y
    dma = pltpu.SemaphoreType.DMA

    def per_group(of):
        return [pltpu.VMEM(of(kind, w), BF16) for kind, _, w in groups]

    def kernel(p, xr, o, *rest):
        lists = [rest[k * n_g:(k + 1) * n_g] for k in range(5)]
        reduce_kernel(groups, p, xr, o, *lists, rest[5 * n_g:])

    return pl.pallas_call(
        kernel,
        out_shape=jax.ShapeDtypeStruct((rows, dim), BF16),
        in_specs=[pl.BlockSpec(memory_space=pl.ANY), pl.BlockSpec(memory_space=pltpu.VMEM)],
        out_specs=pl.BlockSpec(memory_space=pltpu.VMEM),
        scratch_shapes=(
            per_group(lambda kind, w: (n_x, rows, w)) + per_group(lambda kind, w: (n_x, rows, w))
            + per_group(lambda kind, w: (2, rows // 2, w) if kind == "x" else (2, n_x, part // 2, w))
            + per_group(lambda kind, w: (2, rows, w) if kind == "x" else (2, n_x, part, w))
            + per_group(lambda kind, w: (3, part, w))
            + [dma((n_g,)), dma((n_g,)), dma((n_g,)), dma((n_g, 2)), dma((n_g, 2)), dma((n_g, 2, 2)),
               dma((n_g, 2, 2)), dma((n_g, 3)), dma((n_g, 3)), dma((n_g, 3)), dma((n_g, 3))]),
        compiler_params=pltpu.CompilerParams(collective_id=1, has_side_effects=True, vmem_limit_bytes=67_000_000),
        name="reduce",
    )(partial.reshape(n_x, 2, rows, dim), hidden)


def solution(mesh):
    tok_spec = P(('dp', 'ep'), None)
    in_specs = (tok_spec, tok_spec, P(None), P(None, None), P(None, None),
                P('ep', None, 'tp'), P('ep', None, 'tp'), P('ep', 'tp', None),
                P(None, ('tp', 'ep')), P(None, ('tp', 'ep')), P(('tp', 'ep'), None))
    n_x, n_y = mesh.shape['ep'] // 2, mesh.shape['tp']
    assert n_x == 4 and n_y == 4

    def local_step(hidden_in, topk_idx, norm_gain, router_w, shared_sig_w, exp_gate, exp_up, exp_down,
                   sh_gate, sh_up, sh_down):
        h, act, sig, lst, wl, cnt = run_gather(
            hidden_in, topk_idx.T, norm_gain, router_w.T, shared_sig_w.T, sh_gate.T, sh_up.T,
            exp_gate.shape[0], n_x)
        partial = run_experts(lst, wl, cnt, h, act, sig, sh_down,
                              jnp.swapaxes(exp_gate, 1, 2), jnp.swapaxes(exp_up, 1, 2), exp_down)
        return run_reduce(partial, hidden_in, n_x, n_y)

    return jax.shard_map(local_step, mesh=mesh, in_specs=in_specs, out_specs=tok_spec, check_vma=False)
```

```python
import functools

import jax
import jax.numpy as jnp
from jax import lax
from jax.experimental import pallas as pl
from jax.experimental.pallas import tpu as pltpu
from jax.sharding import PartitionSpec as P

RMS_EPS = 1e-6
LANES = 128
PITCH = 20
PAD = 4
TILES = (64, 256, 320, 384, 512)
SLOTS = 3
F32 = jnp.float32
BF16 = jnp.bfloat16
NT = (((1,), (1,)), ((), ()))
TN = (((0,), (0,)), ((), ()))
MESH = pl.DeviceIdType.MESH


def place():
    ep, y = lax.axis_index("ep"), lax.axis_index("tp")
    return ep // 2, ep % 2, y, lax.axis_size("ep") // 2, lax.axis_size("tp")


def peer(x, core, y):
    return {"ep": 2 * x + core, "tp": y}


def remote(src, dst, send, recv, where):
    return pltpu.make_async_remote_copy(src_ref=src, dst_ref=dst, send_sem=send, recv_sem=recv,
                                        device_id=where, device_id_type=MESH)


def meet(peers):
    barrier = pltpu.get_barrier_semaphore()
    for p in peers:
        pl.semaphore_signal(barrier, inc=1, device_id=p, device_id_type=MESH)
    pl.semaphore_wait(barrier, len(peers))


def token_pair(x, gain, sigw, cols_ref, n_exp, width, up_at):
    xf = x.astype(F32)
    inv = lax.rsqrt(jnp.mean(xf * xf, axis=-1, keepdims=True) + RMS_EPS)
    h = (xf * inv * gain.astype(F32)).astype(BF16)
    sig = jax.nn.sigmoid(jnp.sum(h.astype(F32) * sigw.astype(F32), axis=-1, keepdims=True))
    return h, sig


def pair_dots(h, cols_ref, n_exp, width, up_at):
    out = lax.dot_general(cols_ref[...], h, NT, preferred_element_type=F32)
    logits = out[:n_exp]
    ex = jnp.exp(logits - jnp.max(logits, axis=0, keepdims=True))
    prob = ex / jnp.sum(ex, axis=0, keepdims=True)
    act = (jax.nn.silu(out[n_exp:n_exp + width]) * out[up_at:up_at + width]).astype(BF16)
    return prob, act


def routing_lists(idx_t, first, n_local, lst_ref, cnt_ref):
    n_tok = idx_t.shape[1]
    n_hi = n_tok // LANES
    sub = lax.broadcasted_iota(jnp.int32, (n_local, n_tok), 0)
    member = jnp.zeros((n_local, n_tok), F32)
    for e in range(n_local):
        hit = jnp.sum((idx_t == first + e).astype(F32), axis=0, keepdims=True)
        member = jnp.where(sub == e, hit, member)
    tri = (lax.broadcasted_iota(jnp.int32, (LANES, LANES), 0)
           < lax.broadcasted_iota(jnp.int32, (LANES, LANES), 1)).astype(F32).astype(BF16)
    base = jnp.zeros((n_local, 1), F32)
    parts = []
    for b in range(n_hi):
        m_b = member[:, b * LANES:(b + 1) * LANES]
        parts.append(jnp.dot(m_b.astype(BF16), tri, preferred_element_type=F32) + base)
        base = base + jnp.sum(m_b, axis=-1, keepdims=True)
    pos = jnp.concatenate(parts, axis=1).astype(jnp.int32)
    cnt_ref[...] = jnp.broadcast_to(base, cnt_ref.shape).astype(jnp.int32)
    tok = lax.broadcasted_iota(jnp.int32, (n_hi, n_tok), 1)
    hi_id = lax.broadcasted_iota(jnp.int32, (n_hi, n_tok), 0)
    lo_id = lax.broadcasted_iota(jnp.int32, (LANES, n_tok), 0)
    row_id = (lax.broadcasted_iota(jnp.int32, (n_hi, LANES), 0) * LANES
              + lax.broadcasted_iota(jnp.int32, (n_hi, LANES), 1))
    tok_hi = (tok >> 3).astype(F32)
    tok_lo = (tok & 7).astype(F32)
    for e in range(n_local):
        p_e = pos[e:e + 1, :]
        here = ((p_e >> 7) == hi_id) & (member[e:e + 1, :] > 0.0)
        lo_hot = jnp.where((p_e & (LANES - 1)) == lo_id, 1.0, 0.0).astype(BF16)
        lhs = jnp.concatenate([jnp.where(here, v, 0.0) for v in (tok_hi, tok_lo)], axis=0).astype(BF16)
        got = lax.dot_general(lhs, lo_hot, NT, preferred_element_type=F32)
        t_of = (got[:n_hi] * 8.0 + got[n_hi:]).astype(jnp.int32)
        valid = row_id < base[e:e + 1, :].astype(jnp.int32)
        lst_ref[e * n_hi:(e + 1) * n_hi, :] = jnp.where(valid, t_of, n_tok)


def gather_kernel(n_local, x_hbm, idx_hbm, gain_hbm, rw_hbm, sigw_hbm, shg_hbm, shu_hbm,
                  h_hbm, act_ref, sigv_ref, lst_ref, wl_ref, cnt_ref,
                  tok, idx, cols, gain_ref, sigw_ref, prob, hbuf, in_sem, send, recv, isend, irecv, out_sem):
    x, core, y, n_x, n_y = place()
    n_exp, width = rw_hbm.shape[0], shg_hbm.shape[0]
    up_at = n_exp + (width + 15) // 16 * 16
    rows = x_hbm.shape[0]
    half, piece = rows // 2, rows // 8
    own = 2 * x + core
    load_x = pltpu.make_async_copy(x_hbm, tok.at[own], in_sem.at[0])
    load_i = pltpu.make_async_copy(idx_hbm, idx.at[own], in_sem.at[1])
    load_x.start()
    load_i.start()
    small = [pltpu.make_async_copy(src, dst, in_sem.at[2 + k]) for k, (src, dst) in enumerate((
        (rw_hbm, cols.at[0:n_exp, :]), (shg_hbm, cols.at[n_exp:n_exp + width, :]),
        (shu_hbm, cols.at[up_at:up_at + width, :]), (gain_hbm, gain_ref), (sigw_hbm, sigw_ref)))]

    def at(v, n):
        return lax.rem(v + n, n)

    right, left, far = at(x + 1, n_x), at(x - 1, n_x), at(x + 2, n_x)
    up, down = at(y + 1, n_y), at(y - 1, n_y)
    meet([peer(x, 1 - core, y), peer(right, core, y), peer(left, core, y), peer(x, core, up), peer(x, core, down)])
    load_x.wait()
    load_i.wait()

    started = []
    count = [0]

    def copy(block, row, n_rows, where):
        k = count[0]
        count[0] += 1
        row = pl.multiple_of(row, piece)
        ref = tok.at[block, pl.ds(row, n_rows), :]
        c = remote(ref, ref, send.at[k], recv.at[k], where)
        return c

    def go(c):
        c.start()
        started.append(c)
        return c

    mine = (y % 2) * half
    m = [mine + k * piece for k in range(4)]
    o = [half - mine + k * piece for k in range(4)]
    to_right, to_left = peer(right, core, y), peer(left, core, y)
    to_up, to_down, to_mate = peer(x, core, up), peer(x, core, down), peer(x, 1 - core, y)
    from_left, from_right = {}, {}
    for k in range(4):
        from_left[k] = go(copy(own, m[k], piece, to_right))
        from_right[k ^ 2] = go(copy(own, m[k ^ 2], piece, to_left))
    s_mate = go(copy(own, 0, rows, to_mate))
    icopies = []

    def send_idx(block, where):
        k = len(icopies)
        c = remote(idx.at[block], idx.at[block], isend.at[k], irecv.at[k], where)
        c.start()
        icopies.append(c)
        return c

    i_left, i_right, i_own = send_idx(own, to_right), send_idx(own, to_left), send_idx(own, to_mate)
    cols[n_exp + width - width % 8:up_at, :] = jnp.zeros((up_at - n_exp - width + width % 8, cols.shape[1]), BF16)
    tail = up_at + width - width % 8
    cols[tail:, :] = jnp.zeros((cols.shape[0] - tail, cols.shape[1]), BF16)
    for c in small:
        c.start()

    outs = []

    def pair(slot, px):
        for c in range(2):
            h, sig = token_pair(tok[2 * px + c], gain_ref[...].astype(F32).reshape(1, -1), sigw_ref[...], cols, n_exp, width, up_at)
            hbuf[slot, c * rows:(c + 1) * rows, :] = h
            sigv_ref[pl.ds(pl.multiple_of((2 * px + c) * rows, rows), rows), :] = sig
        out = pltpu.make_async_copy(hbuf.at[slot], h_hbm.at[pl.ds(pl.multiple_of(2 * px * rows, 2 * rows), 2 * rows), :],
                                    out_sem.at[slot])
        p, a = pair_dots(hbuf[slot], cols, n_exp, width, up_at)
        prob[px] = p
        act_ref[:, pl.ds(pl.multiple_of(px * 2 * rows, 2 * rows), 2 * rows)] = a
        out.start()
        outs.append(out)

    lb, rb, fb = 2 * left + core, 2 * right + core, 2 * far + core
    mate = {lb_name: [] for lb_name in "lrf"}
    along_y, forward = {}, {}

    def relay(name, block, k, arrived, onward=None):
        arrived.wait_recv()
        if onward is not None:
            forward[k] = go(copy(block, m[k], piece, onward))
        along_y[name, k] = go(copy(block, m[k], piece, to_up if k < 2 else to_down))
        mate[name].append(go(copy(block, m[k], piece, to_mate)))

    def pass_on(name, block, k):
        along_y[name, k].wait_recv()
        mate[name].append(go(copy(block, o[k], piece, to_mate)))

    def arrived_all(name):
        for c in mate[name]:
            c.wait_recv()

    relay("l", lb, 0, from_left[0], to_right)
    relay("r", rb, 2, from_right[2], to_left)
    relay("l", lb, 1, from_left[1], to_right)
    relay("r", rb, 3, from_right[3], to_left)
    i_left.wait_recv()
    i_far = send_idx(lb, to_right)
    i_mates = [send_idx(lb, to_mate)]
    i_right.wait_recv()
    i_mates.append(send_idx(rb, to_mate))
    s_mate.wait_recv()
    for c in small:
        c.wait()
    pair(0, x)
    i_far.wait_recv()
    i_mates.append(send_idx(fb, to_mate))
    relay("l", lb, 2, from_left[2])
    relay("r", rb, 0, from_right[0])
    pass_on("l", lb, 0)
    pass_on("r", rb, 2)
    relay("l", lb, 3, from_left[3])
    relay("r", rb, 1, from_right[1])
    pass_on("l", lb, 1)
    pass_on("r", rb, 3)
    relay("f", fb, 0, forward[0])
    relay("f", fb, 2, forward[2])
    pass_on("l", lb, 2)
    pass_on("r", rb, 0)
    relay("f", fb, 1, forward[1])
    relay("f", fb, 3, forward[3])
    pass_on("l", lb, 3)
    pass_on("r", rb, 1)
    arrived_all("l")
    pair(1, left)
    pass_on("f", fb, 0)
    pass_on("f", fb, 2)
    arrived_all("r")
    pair(2, right)
    pass_on("f", fb, 1)
    pass_on("f", fb, 3)
    first = pl.multiple_of(own * n_local, n_local)
    lst_rows = 2 * n_x * rows // LANES
    lst_ref[n_local * lst_rows:, :] = jnp.full((lst_ref.shape[0] - n_local * lst_rows, LANES), 2 * n_x * rows, jnp.int32)
    for c in [i_own] + i_mates:
        c.wait_recv()
    routing_lists(jnp.concatenate([idx[b] for b in range(2 * n_x)], axis=1), first, n_local, lst_ref, cnt_ref)
    arrived_all("f")
    pair(3, far)
    n_hi = 2 * n_x * rows // LANES
    wl_ref[...] = jnp.zeros_like(wl_ref)
    for b in range(n_x):
        wt = prob[b, pl.ds(first, n_local), :]
        for e in range(n_local):
            for c in range(2):
                wl_ref[e * (n_hi + 1) + 2 * b + c:e * (n_hi + 1) + 2 * b + c + 1, :] = (
                    wt[e:e + 1, c * LANES:(c + 1) * LANES])
    for c in started + icopies:
        c.wait_send()
    for c in outs:
        c.wait()


def run_gather(hidden, idx_t, gain, rw_t, sig_t, shg_t, shu_t, n_local, n_x):
    rows, dim = hidden.shape
    n_tok = rows * 2 * n_x
    n_hi = n_tok // LANES
    n_exp, width = rw_t.shape[0], shg_t.shape[0]
    pad = (width + 15) // 16 * 16
    n_copy = 8 + 1 + 4 + 2 * 12 + 12
    n_idx = 3 + 1 + 3
    vmem = pl.BlockSpec(memory_space=pltpu.VMEM)
    hbm = pl.BlockSpec(memory_space=pl.ANY)
    return pl.pallas_call(
        functools.partial(gather_kernel, n_local),
        out_shape=(jax.ShapeDtypeStruct((n_tok, dim), BF16),
                   jax.ShapeDtypeStruct((width, n_tok), BF16),
                   jax.ShapeDtypeStruct((n_tok, 1), F32),
                   jax.ShapeDtypeStruct(((n_local + 1) * n_hi, LANES), jnp.int32),
                   jax.ShapeDtypeStruct((n_local * (n_hi + 1), LANES), F32),
                   jax.ShapeDtypeStruct((n_local, LANES), jnp.int32)),
        in_specs=[hbm] * 7,
        out_specs=[hbm] + [vmem] * 5,
        scratch_shapes=[
            pltpu.VMEM((2 * n_x, rows, dim), BF16),
            pltpu.VMEM((2 * n_x,) + idx_t.shape, jnp.int32),
            pltpu.VMEM((n_exp + 2 * pad, dim), BF16),
            pltpu.VMEM((dim,), BF16),
            pltpu.VMEM((1, dim), BF16),
            pltpu.VMEM((n_x, n_exp, 2 * rows), F32),
            pltpu.VMEM((n_x, 2 * rows, dim), BF16),
            pltpu.SemaphoreType.DMA((7,)),
            pltpu.SemaphoreType.DMA((n_copy,)),
            pltpu.SemaphoreType.DMA((n_copy,)),
            pltpu.SemaphoreType.DMA((n_idx,)),
            pltpu.SemaphoreType.DMA((n_idx,)),
            pltpu.SemaphoreType.DMA((n_x,)),
        ],
        compiler_params=pltpu.CompilerParams(collective_id=0, has_side_effects=True, vmem_limit_bytes=67_000_000),
        name="gather",
    )(hidden, idx_t, gain, rw_t, sig_t, shg_t, shu_t)


def expert_kernel(lst_hbm, wl_hbm, cnt_hbm, h_hbm, act_hbm, sig_hbm, shd_hbm, wg_hbm, wu_hbm, wd_hbm, out_hbm,
                  lst, wl, cnt, act_ref, sig_ref, shd_ref, h_in, table, acc, wg, wu, wd, xt, xb, fb, active, tile_e, tile_s, tile_r, tile_n,
                  in_sem, w_sem, out_sem, small_sem):
    n_tok, dim = h_hbm.shape
    n_local = wg_hbm.shape[0]
    n_chunk = dim // LANES
    n_blocks = n_tok // LANES
    big = TILES[-1]
    stride = big + PAD

    def fetch_h(b):
        return pltpu.make_async_copy(h_hbm.at[pl.ds(b * LANES, LANES), :], h_in.at[b], in_sem.at[b])

    def weight_copies(e, s):
        return (pltpu.make_async_copy(wg_hbm.at[e], wg.at[s], w_sem.at[s, 0]),
                pltpu.make_async_copy(wu_hbm.at[e], wu.at[s], w_sem.at[s, 1]),
                pltpu.make_async_copy(wd_hbm.at[e], wd.at[s], w_sem.at[s, 2]))

    small = [pltpu.make_async_copy(src, dst, small_sem.at[k]) for k, (src, dst) in enumerate((
        (cnt_hbm, cnt), (lst_hbm, lst), (wl_hbm, wl), (act_hbm, act_ref), (sig_hbm, sig_ref), (shd_hbm, shd_ref)))]
    for c in small:
        c.start()
    for b in range(n_blocks):
        fetch_h(b).start()
    small[0].wait()

    def note(e, carry):
        n, tiles = carry
        total = cnt[e, 0]

        @pl.when(total > 0)
        def _():
            active[n] = e

        def tile(k, t):
            tile_e[t] = e
            tile_s[t] = n
            tile_r[t] = k * big
            tile_n[t] = jnp.minimum(total - k * big, big)
            return t + 1

        return n + jnp.where(total > 0, 1, 0), lax.fori_loop(0, (total + big - 1) // big, tile, tiles)

    n_active, n_tiles = lax.fori_loop(0, n_local, note, (0, 0))
    for s in range(SLOTS - 1):
        @pl.when(s < n_active)
        def _():
            for c in weight_copies(active[s], s):
                c.start()

    acc[n_tok * PITCH:, :] = jnp.zeros((acc.shape[0] - n_tok * PITCH, LANES), F32)
    table[n_tok * PITCH:, :] = jnp.zeros((table.shape[0] - n_tok * PITCH, LANES), F32)

    def shared(b, carry):
        rows = pl.ds(pl.multiple_of(b * LANES, LANES), LANES)
        sig = sig_ref[rows, :]
        for c in range(0, n_chunk, 2):
            sh = sig * lax.dot_general(act_ref[:, rows], shd_ref[:, c * LANES:(c + 2) * LANES], TN,
                                       preferred_element_type=F32)
            for d in range(2):
                acc[pl.ds(b * LANES * PITCH + c + d, LANES, stride=PITCH), :] = sh[:, d * LANES:(d + 1) * LANES]
        return carry

    for c in small[1:]:
        c.wait()
    lax.fori_loop(0, n_blocks, shared, 0)

    def spread(b, carry):
        fetch_h(b).wait()
        for c in range(n_chunk):
            table[pl.ds(b * LANES * PITCH + c, LANES, stride=PITCH), :] = (
                h_in[b, :, c * LANES:(c + 1) * LANES].astype(F32))
        return carry

    lax.fori_loop(0, n_blocks, spread, 0)

    def gather8(base, g):
        for i in range(8):
            row = pl.multiple_of(lst[base + g * 8 + i] * PITCH, 4)
            xt[pl.ds(g * 8 + i, n_chunk, stride=stride), :] = table[pl.ds(row, n_chunk), :]

    def scatter8(f_at, w_at, base, g):
        where, weight, old, new = [], [], [], []
        for i in range(8):
            t = lst[base + g * 8 + i]
            where.append(pl.multiple_of(t * PITCH, 4))
            weight.append(wl[w_at + t])
            old.append(acc[pl.ds(where[i], n_chunk), :])
        for i in range(8):
            new.append(old[i] + weight[i] * fb[pl.ds(f_at + g * 8 + i, n_chunk, stride=stride), :])
        for i in range(8):
            acc[pl.ds(where[i], n_chunk), :] = new[i]

    def ffn(m, s, f_at, moves):
        for c in range(n_chunk):
            xb[:m, c * LANES:(c + 1) * LANES] = xt[c * stride:c * stride + m, :].astype(BF16)
        n_move = len(moves)
        done = 0

        def some(upto):
            nonlocal done
            while done < upto:
                moves[done]()
                done += 1

        gate = lax.dot_general(wg[s], xb[:m, :], NT, preferred_element_type=F32)
        some(n_move * 3 // 10)
        up = lax.dot_general(wu[s], xb[:m, :], NT, preferred_element_type=F32)
        some(n_move * 6 // 10)
        act = (jax.nn.silu(gate) * up).astype(BF16)
        for c in range(0, n_chunk, 2):
            f = lax.dot_general(act, wd[s, :, c * LANES:(c + 2) * LANES], TN, preferred_element_type=F32)
            yield_at = n_move * 6 // 10 + (n_move - n_move * 6 // 10) * (c + 2) // n_chunk
            for d in range(2):
                fb[pl.ds(f_at + (c + d) * stride, m), :] = f[:, d * LANES:(d + 1) * LANES]
            some(yield_at)

    @pl.when(n_tiles > 0)
    def _():
        def first(g, carry):
            gather8(tile_e[0] * n_tok + tile_r[0], g)
            return carry

        lax.fori_loop(0, (tile_n[0] + 7) // 8, first, 0)

    def tile_step(i, carry):
        e, k, r0, n = tile_e[i], tile_s[i], tile_r[i], tile_n[i]
        s = lax.rem(k, SLOTS)

        @pl.when(r0 == 0)
        def _():
            ahead = k + SLOTS - 1

            @pl.when(ahead < n_active)
            def _():
                for c in weight_copies(active[ahead], lax.rem(ahead, SLOTS)):
                    c.start()

            for c in weight_copies(e, s):
                c.wait()

        f_size = n_chunk * stride
        f_at = pl.multiple_of(lax.rem(i, 2) * f_size, 8)
        f_prev = pl.multiple_of(lax.rem(i + 1, 2) * f_size, 8)
        before, after = jnp.maximum(i - 1, 0), jnp.minimum(i + 1, n_tiles - 1)
        e1 = tile_e[before]
        w1 = e1 * (n_tok + LANES)
        base1 = jnp.where(i > 0, e1 * n_tok + tile_r[before], n_local * n_tok)
        n1 = jnp.where(i > 0, tile_n[before], 0)
        base2 = tile_e[after] * n_tok + tile_r[after]
        n2 = jnp.where(i + 1 < n_tiles, tile_n[after], 0)
        below = 0
        for m in TILES:
            @pl.when((n > below) & (n <= m))
            def _(m=m):
                moves = []
                for g in range(m // 8):
                    moves.append(functools.partial(gather8, base2, g))
                    moves.append(functools.partial(scatter8, f_prev, w1, base1, g))
                ffn(m, s, f_at, moves)

                def more_in(g, c2):
                    gather8(base2, g)
                    return c2

                def more_out(g, c2):
                    scatter8(f_prev, w1, base1, g)
                    return c2

                lax.fori_loop(m // 8, (n2 + 7) // 8, more_in, 0)
                lax.fori_loop(m // 8, (n1 + 7) // 8, more_out, 0)
            below = m

        return carry

    lax.fori_loop(0, n_tiles, tile_step, 0)

    @pl.when(n_tiles > 0)
    def _():
        i = n_tiles - 1
        f_at = pl.multiple_of(lax.rem(i, 2) * (n_chunk * stride), 8)

        def last(g, carry):
            scatter8(f_at, tile_e[i] * (n_tok + LANES), tile_e[i] * n_tok + tile_r[i], g)
            return carry

        lax.fori_loop(0, (tile_n[i] + 7) // 8, last, 0)

    def write_out(b):
        return pltpu.make_async_copy(h_in.at[b], out_hbm.at[pl.ds(b * LANES, LANES), :], out_sem.at[b])

    def finish(b, carry):
        for c in range(n_chunk):
            h_in[b, :, c * LANES:(c + 1) * LANES] = (
                acc[pl.ds(b * LANES * PITCH + c, LANES, stride=PITCH), :].astype(BF16))
        write_out(b).start()
        return carry

    lax.fori_loop(0, n_blocks, finish, 0)
    for b in range(n_blocks):
        write_out(b).wait()


def run_experts(lst, wl, cnt, h, act, sig, shd, wg, wu, wd):
    n_tok, dim = h.shape
    n_local, width, _ = wg.shape
    n_chunk = dim // LANES
    big = TILES[-1]
    max_tiles = n_local * ((n_tok + big - 1) // big)
    hbm = pl.BlockSpec(memory_space=pl.ANY)
    return pl.pallas_call(
        expert_kernel,
        out_shape=jax.ShapeDtypeStruct((n_tok, dim), BF16),
        in_specs=[hbm] * 10,
        out_specs=hbm,
        scratch_shapes=[
            pltpu.SMEM((lst.size,), jnp.int32),
            pltpu.SMEM((wl.size,), F32),
            pltpu.SMEM(cnt.shape, jnp.int32),
            pltpu.VMEM(act.shape, BF16),
            pltpu.VMEM(sig.shape, F32),
            pltpu.VMEM(shd.shape, BF16),
            pltpu.VMEM((n_tok // LANES, LANES, dim), BF16),
            pltpu.VMEM(((n_tok + 1) * PITCH, LANES), F32),
            pltpu.VMEM(((n_tok + 1) * PITCH, LANES), F32),
            pltpu.VMEM((SLOTS, width, dim), BF16),
            pltpu.VMEM((SLOTS, width, dim), BF16),
            pltpu.VMEM((SLOTS, width, dim), BF16),
            pltpu.VMEM((n_chunk * (big + PAD), LANES), F32),
            pltpu.VMEM((big, dim), BF16),
            pltpu.VMEM((2 * n_chunk * (big + PAD), LANES), F32),
            pltpu.SMEM((n_local,), jnp.int32),
            pltpu.SMEM((max_tiles,), jnp.int32),
            pltpu.SMEM((max_tiles,), jnp.int32),
            pltpu.SMEM((max_tiles,), jnp.int32),
            pltpu.SMEM((max_tiles,), jnp.int32),
            pltpu.SemaphoreType.DMA((n_tok // LANES,)),
            pltpu.SemaphoreType.DMA((SLOTS, 3)),
            pltpu.SemaphoreType.DMA((n_tok // LANES,)),
            pltpu.SemaphoreType.DMA((6,)),
        ],
        compiler_params=pltpu.CompilerParams(vmem_limit_bytes=67_000_000),
        name="experts",
    )(lst.reshape(-1), wl.reshape(-1), cnt, h, act, sig, shd, wg, wu, wd)


def reduce_kernel(groups, p_hbm, x_hbm, out_ref, x_ref, last, mate, own, ra, rb, rc, sems):
    x, core, y, n_x, n_y = place()
    rows, dim = x_ref.shape
    part = rows // n_y
    load_x = pltpu.make_async_copy(x_hbm, x_ref, sems[-1])
    s_in, s_d, r_d, s_a, r_a, s_b, r_b, s_c, r_c, s_e, r_e = sems[:-1]

    def at(v, n):
        return lax.rem(v + n, n)

    xs = [at(x + d, n_x) for d in range(4)]
    ys = [at(y + d, n_y) for d in range(4)]
    to_mate = peer(x, 1 - core, y)
    x_peers = [None] + [peer(xs[d], core, y) for d in range(1, 4)]
    y_peers = [None] + [peer(x, core, ys[d]) for d in range(1, 4)]
    mine = pl.ds(pl.multiple_of(y * part, part), part)
    started = []

    def go(c):
        c.start()
        started.append(c)
        return c

    loads, mates = [], []
    for g, (kind, lo, w) in enumerate(groups):
        c = pltpu.make_async_copy(p_hbm.at[:, core, :, lo:lo + w], own[g], s_in.at[g])
        c.start()
        loads.append(c)
    load_x.start()
    meet([to_mate] + x_peers[1:] + y_peers[1:])
    for g, (kind, lo, w) in enumerate(groups):
        mates.append(go(remote(p_hbm.at[:, 1 - core, :, lo:lo + w], mate[g], s_d.at[g], r_d.at[g], to_mate)))

    def unit(g, d, lo, n):
        if groups[g][0] == "x":
            return own[g].at[xs[d], lo:lo + n, :]
        return own[g].at[:, pl.ds(pl.multiple_of(ys[d] * part, part) + lo, n), :]

    def land(g, k, lo, n):
        return rb[g].at[k, lo:lo + n, :] if groups[g][0] == "x" else rb[g].at[k, :, lo:lo + n, :]

    def first_peers(g):
        return x_peers if groups[g][0] == "x" else y_peers

    def half(g):
        return (rows if groups[g][0] == "x" else part) // 2

    a, b_ind, b_dep, c_sent, e_sent = {}, {}, {}, {}, {}

    def add_mate(g):
        loads[g].wait()
        mates[g].wait_recv()
        own[g][...] = (own[g][...].astype(F32) + mate[g][...].astype(F32)).astype(BF16)
        h = half(g)
        for k, (lo, d) in enumerate(((0, 1), (h, 3))):
            a[g, k] = go(remote(unit(g, 2, lo, h), ra[g].at[k], s_a.at[g, k], r_a.at[g, k], first_peers(g)[d]))

    def send_near(g):
        h = half(g)
        for k, (lo, d) in enumerate(((h, 1), (0, 3))):
            b_ind[g, k] = go(remote(unit(g, d, lo, h), land(g, k, lo, h), s_b.at[g, k, 0], r_b.at[g, k, 0],
                                    first_peers(g)[d]))

    def add_far(g):
        h = half(g)
        for k, (lo, d) in enumerate(((0, 1), (h, 3))):
            a[g, k].wait_recv()
            ref = unit(g, d, lo, h)
            ref[...] = (ref[...].astype(F32) + ra[g][k].astype(F32)).astype(BF16)
            b_dep[g, k] = go(remote(ref, land(g, k, lo, h), s_b.at[g, k, 1], r_b.at[g, k, 1], first_peers(g)[d]))

    def second_axis(g):
        for k in range(2):
            b_ind[g, k].wait_recv()
            b_dep[g, k].wait_recv()
        ref = unit(g, 0, 0, 2 * half(g))
        ref[...] = (ref[...].astype(F32) + rb[g][0].astype(F32) + rb[g][1].astype(F32)).astype(BF16)
        for d in (2, 1, 3):
            if groups[g][0] == "x":
                src = own[g].at[x, pl.ds(pl.multiple_of(ys[d] * part, part), part), :]
                where = y_peers[d]
            else:
                src = own[g].at[xs[d], mine, :]
                where = x_peers[d]
            c_sent[g, d] = go(remote(src, rc[g].at[d - 1], s_c.at[g, d - 1], r_c.at[g, d - 1], where))

    def finish(g):
        kind, lo, w = groups[g]
        if g == 0:
            load_x.wait()
        total = own[g][x, mine, :].astype(F32)
        for d in (1, 3, 2):
            c_sent[g, d].wait_recv()
            total = total + rc[g][d - 1].astype(F32)
        cols = slice(lo, lo + w)
        out_ref[mine, cols] = (x_ref[mine, cols].astype(F32) + total).astype(BF16)
        for d in (2, 1, 3):
            ref = out_ref.at[mine, cols]
            e_sent[g, d] = go(remote(ref, ref, s_e.at[g, d - 1], r_e.at[g, d - 1], y_peers[d]))

    def exchange(g):
        for k in range(2):
            b_ind[g, k].wait_recv()
            b_dep[g, k].wait_recv()
        last[y] = (own[g][x].astype(F32) + rb[g][0].astype(F32) + rb[g][1].astype(F32)).astype(BF16)
        for d in (2, 1, 3):
            c_sent[g, d] = go(remote(last.at[y], last.at[y], s_c.at[g, d - 1], r_c.at[g, d - 1], y_peers[d]))

    def close(g):
        _, lo, w = groups[g]
        for d in (1, 3, 2):
            c_sent[g, d].wait_recv()
        total = last[0].astype(F32)
        for k in range(1, 4):
            total = total + last[k].astype(F32)
        out_ref[:, lo:lo + w] = (x_ref[:, lo:lo + w].astype(F32) + total).astype(BF16)

    order = ((add_mate, 0), (send_near, 0), (add_mate, 1), (send_near, 1), (add_mate, 2), (send_near, 2), (add_far, 0),
             (add_far, 1), (add_mate, 3), (add_far, 2), (second_axis, 0), (send_near, 3), (second_axis, 2),
             (add_mate, 4), (second_axis, 1), (add_far, 3), (send_near, 4), (finish, 0), (finish, 2), (add_far, 4),
             (finish, 1), (second_axis, 3), (exchange, 4), (finish, 3), (close, 4))
    for step, g in order:
        step(g)
    for g in range(len(groups) - 1):
        for d in range(1, 4):
            e_sent[g, d].wait_recv()
    for c in started:
        c.wait_send()


def run_reduce(partial, hidden, n_x, n_y):
    rows, dim = hidden.shape
    q = dim // 8
    groups = (("x", 0, q), ("x", q, 2 * q), ("y", 3 * q, 2 * q), ("x", 5 * q, 2 * q), ("x", 7 * q, q))
    n_g = len(groups)
    part = rows // n_y
    dma = pltpu.SemaphoreType.DMA

    def per_group(of):
        return [pltpu.VMEM(of(kind, w), BF16) for kind, _, w in groups]

    def kernel(p, xh, o, xr, last, *rest):
        lists = [rest[k * n_g:(k + 1) * n_g] for k in range(5)]
        reduce_kernel(groups, p, xh, o, xr, last, *lists, rest[5 * n_g:])

    return pl.pallas_call(
        kernel,
        out_shape=jax.ShapeDtypeStruct((rows, dim), BF16),
        in_specs=[pl.BlockSpec(memory_space=pltpu.HBM)] * 2,
        out_specs=pl.BlockSpec(memory_space=pltpu.VMEM),
        scratch_shapes=(
            [pltpu.VMEM((rows, dim), BF16), pltpu.VMEM((n_y, rows, groups[-1][2]), BF16)] +
            per_group(lambda kind, w: (n_x, rows, w)) + per_group(lambda kind, w: (n_x, rows, w))
            + per_group(lambda kind, w: (2, rows // 2, w) if kind == "x" else (2, n_x, part // 2, w))
            + per_group(lambda kind, w: (2, rows, w) if kind == "x" else (2, n_x, part, w))
            + per_group(lambda kind, w: (3, part, w))
            + [dma((n_g,)), dma((n_g,)), dma((n_g,)), dma((n_g, 2)), dma((n_g, 2)), dma((n_g, 2, 2)),
               dma((n_g, 2, 2)), dma((n_g, 3)), dma((n_g, 3)), dma((n_g, 3)), dma((n_g, 3)), dma]),
        compiler_params=pltpu.CompilerParams(collective_id=1, has_side_effects=True, vmem_limit_bytes=60_000_000),
        name="reduce",
    )(partial.reshape(n_x, 2, rows, dim), hidden)


def solution(mesh):
    tok_spec = P(('dp', 'ep'), None)
    in_specs = (tok_spec, tok_spec, P(None), P(None, None), P(None, None),
                P('ep', None, 'tp'), P('ep', None, 'tp'), P('ep', 'tp', None),
                P(None, ('tp', 'ep')), P(None, ('tp', 'ep')), P(('tp', 'ep'), None))
    n_x, n_y = mesh.shape['ep'] // 2, mesh.shape['tp']
    assert n_x == 4 and n_y == 4

    def local_step(hidden_in, topk_idx, norm_gain, router_w, shared_sig_w, exp_gate, exp_up, exp_down,
                   sh_gate, sh_up, sh_down):
        h, act, sig, lst, wl, cnt = run_gather(
            hidden_in, topk_idx.T, norm_gain, router_w.T, shared_sig_w.T, sh_gate.T, sh_up.T,
            exp_gate.shape[0], n_x)
        partial = run_experts(lst, wl, cnt, h, act, sig, sh_down,
                              jnp.swapaxes(exp_gate, 1, 2), jnp.swapaxes(exp_up, 1, 2), exp_down)
        return run_reduce(partial, hidden_in, n_x, n_y)

    return jax.shard_map(local_step, mesh=mesh, in_specs=in_specs, out_specs=tok_spec, check_vma=False)
```

```python
import functools

import jax
import jax.numpy as jnp
from jax import lax
from jax.experimental import pallas as pl
from jax.experimental.pallas import tpu as pltpu
from jax.sharding import PartitionSpec as P

RMS_EPS = 1e-6
LANES = 128
PITCH = 20
PAD = 4
TILES = (64, 256, 320, 384, 512)
SLOTS = 3
F32 = jnp.float32
BF16 = jnp.bfloat16
NT = (((1,), (1,)), ((), ()))
TN = (((0,), (0,)), ((), ()))
MESH = pl.DeviceIdType.MESH


def place():
    ep, y = lax.axis_index("ep"), lax.axis_index("tp")
    return ep // 2, ep % 2, y, lax.axis_size("ep") // 2, lax.axis_size("tp")


def peer(x, core, y):
    return {"ep": 2 * x + core, "tp": y}


def remote(src, dst, send, recv, where):
    return pltpu.make_async_remote_copy(src_ref=src, dst_ref=dst, send_sem=send, recv_sem=recv,
                                        device_id=where, device_id_type=MESH)


def meet(peers):
    barrier = pltpu.get_barrier_semaphore()
    for p in peers:
        pl.semaphore_signal(barrier, inc=1, device_id=p, device_id_type=MESH)
    pl.semaphore_wait(barrier, len(peers))


def token_pair(x, gain, sigw, cols_ref, n_exp, width, up_at):
    xf = x.astype(F32)
    inv = lax.rsqrt(jnp.mean(xf * xf, axis=-1, keepdims=True) + RMS_EPS)
    h = (xf * inv * gain.astype(F32)).astype(BF16)
    sig = jax.nn.sigmoid(jnp.sum(h.astype(F32) * sigw.astype(F32), axis=-1, keepdims=True))
    return h, sig


def pair_dots(h, cols_ref, n_exp, width, up_at):
    out = lax.dot_general(cols_ref[...], h, NT, preferred_element_type=F32)
    logits = out[:n_exp]
    ex = jnp.exp(logits - jnp.max(logits, axis=0, keepdims=True))
    prob = ex / jnp.sum(ex, axis=0, keepdims=True)
    act = (jax.nn.silu(out[n_exp:n_exp + width]) * out[up_at:up_at + width]).astype(BF16)
    return prob, act


def routing_lists(idx_t, first, n_local, lst_ref, cnt_ref):
    n_tok = idx_t.shape[1]
    n_hi = n_tok // LANES
    sub = lax.broadcasted_iota(jnp.int32, (n_local, n_tok), 0)
    member = jnp.zeros((n_local, n_tok), F32)
    for e in range(n_local):
        hit = jnp.sum((idx_t == first + e).astype(F32), axis=0, keepdims=True)
        member = jnp.where(sub == e, hit, member)
    tri = (lax.broadcasted_iota(jnp.int32, (LANES, LANES), 0)
           < lax.broadcasted_iota(jnp.int32, (LANES, LANES), 1)).astype(F32).astype(BF16)
    base = jnp.zeros((n_local, 1), F32)
    parts = []
    for b in range(n_hi):
        m_b = member[:, b * LANES:(b + 1) * LANES]
        parts.append(jnp.dot(m_b.astype(BF16), tri, preferred_element_type=F32) + base)
        base = base + jnp.sum(m_b, axis=-1, keepdims=True)
    pos = jnp.concatenate(parts, axis=1).astype(jnp.int32)
    cnt_ref[...] = jnp.broadcast_to(base, cnt_ref.shape).astype(jnp.int32)
    tok = lax.broadcasted_iota(jnp.int32, (n_hi, n_tok), 1)
    hi_id = lax.broadcasted_iota(jnp.int32, (n_hi, n_tok), 0)
    lo_id = lax.broadcasted_iota(jnp.int32, (LANES, n_tok), 0)
    row_id = (lax.broadcasted_iota(jnp.int32, (n_hi, LANES), 0) * LANES
              + lax.broadcasted_iota(jnp.int32, (n_hi, LANES), 1))
    tok_hi = (tok >> 3).astype(F32)
    tok_lo = (tok & 7).astype(F32)
    for e in range(n_local):
        p_e = pos[e:e + 1, :]
        here = ((p_e >> 7) == hi_id) & (member[e:e + 1, :] > 0.0)
        lo_hot = jnp.where((p_e & (LANES - 1)) == lo_id, 1.0, 0.0).astype(BF16)
        lhs = jnp.concatenate([jnp.where(here, v, 0.0) for v in (tok_hi, tok_lo)], axis=0).astype(BF16)
        got = lax.dot_general(lhs, lo_hot, NT, preferred_element_type=F32)
        t_of = (got[:n_hi] * 8.0 + got[n_hi:]).astype(jnp.int32)
        valid = row_id < base[e:e + 1, :].astype(jnp.int32)
        lst_ref[e * n_hi:(e + 1) * n_hi, :] = jnp.where(valid, t_of, n_tok)


def gather_kernel(n_local, x_hbm, idx_hbm, gain_hbm, rw_hbm, sigw_hbm, shg_hbm, shu_hbm,
                  h_hbm, act_ref, sigv_ref, lst_ref, wl_ref, cnt_ref,
                  tok, idx, cols, gain_ref, sigw_ref, prob, hbuf, in_sem, send, recv, isend, irecv, out_sem):
    x, core, y, n_x, n_y = place()
    n_exp, width = rw_hbm.shape[0], shg_hbm.shape[0]
    up_at = n_exp + (width + 15) // 16 * 16
    rows = x_hbm.shape[0]
    half, piece = rows // 2, rows // 4
    own = 2 * x + core
    load_x = pltpu.make_async_copy(x_hbm, tok.at[own], in_sem.at[0])
    load_i = pltpu.make_async_copy(idx_hbm, idx.at[own], in_sem.at[1])
    load_x.start()
    load_i.start()
    small = [pltpu.make_async_copy(src, dst, in_sem.at[2 + k]) for k, (src, dst) in enumerate((
        (rw_hbm, cols.at[0:n_exp, :]), (shg_hbm, cols.at[n_exp:n_exp + width, :]),
        (shu_hbm, cols.at[up_at:up_at + width, :]), (gain_hbm, gain_ref), (sigw_hbm, sigw_ref)))]

    def at(v, n):
        return lax.rem(v + n, n)

    right, left, far = at(x + 1, n_x), at(x - 1, n_x), at(x + 2, n_x)
    up, down = at(y + 1, n_y), at(y - 1, n_y)
    meet([peer(x, 1 - core, y), peer(right, core, y), peer(left, core, y), peer(x, core, up), peer(x, core, down)])
    load_x.wait()
    load_i.wait()

    started = []
    count = [0]

    def copy(block, row, n_rows, where):
        k = count[0]
        count[0] += 1
        row = pl.multiple_of(row, piece)
        ref = tok.at[block, pl.ds(row, n_rows), :]
        c = remote(ref, ref, send.at[k], recv.at[k], where)
        return c

    def go(c):
        c.start()
        started.append(c)
        return c

    mine = (y % 2) * half
    m = [mine, mine + piece]
    o = [half - mine, half - mine + piece]
    to_right, to_left = peer(right, core, y), peer(left, core, y)
    to_up, to_down, to_mate = peer(x, core, up), peer(x, core, down), peer(x, 1 - core, y)
    icopies = []

    def send_idx(block, where):
        k = len(icopies)
        c = remote(idx.at[block], idx.at[block], isend.at[k], irecv.at[k], where)
        c.start()
        icopies.append(c)
        return c

    i_left, i_right, i_own = send_idx(own, to_right), send_idx(own, to_left), send_idx(own, to_mate)
    from_left, from_right = {}, {}
    for k in range(2):
        from_left[k] = go(copy(own, m[k], piece, to_right))
        from_right[1 - k] = go(copy(own, m[1 - k], piece, to_left))
    s_mate = go(copy(own, 0, rows, to_mate))

    cols[n_exp + width - width % 8:up_at, :] = jnp.zeros((up_at - n_exp - width + width % 8, cols.shape[1]), BF16)
    tail = up_at + width - width % 8
    cols[tail:, :] = jnp.zeros((cols.shape[0] - tail, cols.shape[1]), BF16)
    for c in small:
        c.start()

    outs = []

    def pair(slot, px):
        for c in range(2):
            h, sig = token_pair(tok[2 * px + c], gain_ref[...].astype(F32).reshape(1, -1), sigw_ref[...], cols, n_exp, width, up_at)
            hbuf[slot, c * rows:(c + 1) * rows, :] = h
            sigv_ref[pl.ds(pl.multiple_of((2 * px + c) * rows, rows), rows), :] = sig
        out = pltpu.make_async_copy(hbuf.at[slot], h_hbm.at[pl.ds(pl.multiple_of(2 * px * rows, 2 * rows), 2 * rows), :],
                                    out_sem.at[slot])
        p, a = pair_dots(hbuf[slot], cols, n_exp, width, up_at)
        prob[px] = p
        act_ref[:, pl.ds(pl.multiple_of(px * 2 * rows, 2 * rows), 2 * rows)] = a
        out.start()
        outs.append(out)

    lb, rb, fb = 2 * left + core, 2 * right + core, 2 * far + core
    mate = {name: [] for name in "lrf"}
    along_y, forward = {}, {}

    def relay(name, block, k, arrived, onward=None):
        arrived.wait_recv()
        if onward is not None:
            forward[k] = go(copy(block, m[k], piece, onward))
        along_y[name, k] = go(copy(block, m[k], piece, to_up if k == 0 else to_down))

    def to_the_mate(name, block, row):
        mate[name].append(go(copy(block, row, half, to_mate)))

    def pass_on(name, block):
        for k in range(2):
            along_y[name, k].wait_recv()
        to_the_mate(name, block, o[0])

    def arrived_all(name):
        for c in mate[name]:
            c.wait_recv()

    i_left.wait_recv()
    i_far = send_idx(lb, to_right)
    i_mates = [send_idx(lb, to_mate)]
    i_right.wait_recv()
    i_mates.append(send_idx(rb, to_mate))
    relay("l", lb, 0, from_left[0], to_right)
    relay("r", rb, 1, from_right[1], to_left)
    s_mate.wait_recv()
    for c in small:
        c.wait()
    pair(0, x)
    relay("l", lb, 1, from_left[1])
    relay("r", rb, 0, from_right[0])
    to_the_mate("l", lb, m[0])
    to_the_mate("r", rb, m[0])
    i_far.wait_recv()
    i_mates.append(send_idx(fb, to_mate))
    relay("f", fb, 0, forward[0])
    relay("f", fb, 1, forward[1])
    to_the_mate("f", fb, m[0])
    pass_on("l", lb)
    pass_on("r", rb)
    arrived_all("l")
    pair(1, left)
    pass_on("f", fb)
    arrived_all("r")
    pair(2, right)
    first = pl.multiple_of(own * n_local, n_local)
    lst_rows = 2 * n_x * rows // LANES
    lst_ref[n_local * lst_rows:, :] = jnp.full((lst_ref.shape[0] - n_local * lst_rows, LANES), 2 * n_x * rows, jnp.int32)
    for c in [i_own] + i_mates:
        c.wait_recv()
    routing_lists(jnp.concatenate([idx[b] for b in range(2 * n_x)], axis=1), first, n_local, lst_ref, cnt_ref)
    arrived_all("f")
    pair(3, far)
    n_hi = 2 * n_x * rows // LANES
    wl_ref[...] = jnp.zeros_like(wl_ref)
    for b in range(n_x):
        wt = prob[b, pl.ds(first, n_local), :]
        for e in range(n_local):
            for c in range(2):
                wl_ref[e * (n_hi + 1) + 2 * b + c:e * (n_hi + 1) + 2 * b + c + 1, :] = (
                    wt[e:e + 1, c * LANES:(c + 1) * LANES])
    for c in started + icopies:
        c.wait_send()
    for c in outs:
        c.wait()


def run_gather(hidden, idx_t, gain, rw_t, sig_t, shg_t, shu_t, n_local, n_x):
    rows, dim = hidden.shape
    n_tok = rows * 2 * n_x
    n_hi = n_tok // LANES
    n_exp, width = rw_t.shape[0], shg_t.shape[0]
    pad = (width + 15) // 16 * 16
    n_copy = 4 + 1 + 2 + 6 + 6
    n_idx = 3 + 1 + 3
    vmem = pl.BlockSpec(memory_space=pltpu.VMEM)
    hbm = pl.BlockSpec(memory_space=pl.ANY)
    return pl.pallas_call(
        functools.partial(gather_kernel, n_local),
        out_shape=(jax.ShapeDtypeStruct((n_tok, dim), BF16),
                   jax.ShapeDtypeStruct((width, n_tok), BF16),
                   jax.ShapeDtypeStruct((n_tok, 1), F32),
                   jax.ShapeDtypeStruct(((n_local + 1) * n_hi, LANES), jnp.int32),
                   jax.ShapeDtypeStruct((n_local * (n_hi + 1), LANES), F32),
                   jax.ShapeDtypeStruct((n_local, LANES), jnp.int32)),
        in_specs=[hbm] * 7,
        out_specs=[hbm] + [vmem] * 5,
        scratch_shapes=[
            pltpu.VMEM((2 * n_x, rows, dim), BF16),
            pltpu.VMEM((2 * n_x,) + idx_t.shape, jnp.int32),
            pltpu.VMEM((n_exp + 2 * pad, dim), BF16),
            pltpu.VMEM((dim,), BF16),
            pltpu.VMEM((1, dim), BF16),
            pltpu.VMEM((n_x, n_exp, 2 * rows), F32),
            pltpu.VMEM((n_x, 2 * rows, dim), BF16),
            pltpu.SemaphoreType.DMA((7,)),
            pltpu.SemaphoreType.DMA((n_copy,)),
            pltpu.SemaphoreType.DMA((n_copy,)),
            pltpu.SemaphoreType.DMA((n_idx,)),
            pltpu.SemaphoreType.DMA((n_idx,)),
            pltpu.SemaphoreType.DMA((n_x,)),
        ],
        compiler_params=pltpu.CompilerParams(collective_id=0, has_side_effects=True, vmem_limit_bytes=67_000_000),
        name="gather",
    )(hidden, idx_t, gain, rw_t, sig_t, shg_t, shu_t)


def expert_kernel(lst_hbm, wl_hbm, cnt_hbm, h_hbm, act_hbm, sig_hbm, shd_hbm, wg_hbm, wu_hbm, wd_hbm, out_hbm,
                  lst, wl, cnt, act_ref, sig_ref, shd_ref, h_in, table, acc, wg, wu, wd, xt, xb, fb, active, tile_e, tile_s, tile_r, tile_n,
                  in_sem, w_sem, out_sem, small_sem):
    n_tok, dim = h_hbm.shape
    n_local = wg_hbm.shape[0]
    n_chunk = dim // LANES
    n_blocks = n_tok // LANES
    big = TILES[-1]
    stride = big + PAD

    def fetch_h(b):
        return pltpu.make_async_copy(h_hbm.at[pl.ds(b * LANES, LANES), :], h_in.at[b], in_sem.at[b])

    def weight_copies(e, s):
        return (pltpu.make_async_copy(wg_hbm.at[e], wg.at[s], w_sem.at[s, 0]),
                pltpu.make_async_copy(wu_hbm.at[e], wu.at[s], w_sem.at[s, 1]),
                pltpu.make_async_copy(wd_hbm.at[e], wd.at[s], w_sem.at[s, 2]))

    small = [pltpu.make_async_copy(src, dst, small_sem.at[k]) for k, (src, dst) in enumerate((
        (cnt_hbm, cnt), (lst_hbm, lst), (wl_hbm, wl), (act_hbm, act_ref), (sig_hbm, sig_ref), (shd_hbm, shd_ref)))]
    for c in small:
        c.start()
    for b in range(n_blocks):
        fetch_h(b).start()
    small[0].wait()

    def note(e, carry):
        n, tiles = carry
        total = cnt[e, 0]

        @pl.when(total > 0)
        def _():
            active[n] = e

        def tile(k, t):
            tile_e[t] = e
            tile_s[t] = n
            tile_r[t] = k * big
            tile_n[t] = jnp.minimum(total - k * big, big)
            return t + 1

        return n + jnp.where(total > 0, 1, 0), lax.fori_loop(0, (total + big - 1) // big, tile, tiles)

    n_active, n_tiles = lax.fori_loop(0, n_local, note, (0, 0))
    for s in range(SLOTS - 1):
        @pl.when(s < n_active)
        def _():
            for c in weight_copies(active[s], s):
                c.start()

    acc[n_tok * PITCH:, :] = jnp.zeros((acc.shape[0] - n_tok * PITCH, LANES), F32)
    table[n_tok * PITCH:, :] = jnp.zeros((table.shape[0] - n_tok * PITCH, LANES), F32)

    def shared(b, carry):
        rows = pl.ds(pl.multiple_of(b * LANES, LANES), LANES)
        sig = sig_ref[rows, :]
        for c in range(0, n_chunk, 2):
            sh = sig * lax.dot_general(act_ref[:, rows], shd_ref[:, c * LANES:(c + 2) * LANES], TN,
                                       preferred_element_type=F32)
            for d in range(2):
                acc[pl.ds(b * LANES * PITCH + c + d, LANES, stride=PITCH), :] = sh[:, d * LANES:(d + 1) * LANES]
        return carry

    for c in small[1:]:
        c.wait()
    lax.fori_loop(0, n_blocks, shared, 0)

    def spread(b, carry):
        fetch_h(b).wait()
        for c in range(n_chunk):
            table[pl.ds(b * LANES * PITCH + c, LANES, stride=PITCH), :] = (
                h_in[b, :, c * LANES:(c + 1) * LANES].astype(F32))
        return carry

    lax.fori_loop(0, n_blocks, spread, 0)

    def gather8(base, g):
        for i in range(8):
            row = pl.multiple_of(lst[base + g * 8 + i] * PITCH, 4)
            xt[pl.ds(g * 8 + i, n_chunk, stride=stride), :] = table[pl.ds(row, n_chunk), :]

    def scatter8(f_at, w_at, base, g):
        where, weight, old, new = [], [], [], []
        for i in range(8):
            t = lst[base + g * 8 + i]
            where.append(pl.multiple_of(t * PITCH, 4))
            weight.append(wl[w_at + t])
            old.append(acc[pl.ds(where[i], n_chunk), :])
        for i in range(8):
            new.append(old[i] + weight[i] * fb[pl.ds(f_at + g * 8 + i, n_chunk, stride=stride), :])
        for i in range(8):
            acc[pl.ds(where[i], n_chunk), :] = new[i]

    def ffn(m, s, f_at, moves):
        for c in range(n_chunk):
            xb[:m, c * LANES:(c + 1) * LANES] = xt[c * stride:c * stride + m, :].astype(BF16)
        n_move = len(moves)
        done = 0

        def some(upto):
            nonlocal done
            while done < upto:
                moves[done]()
                done += 1

        gate = lax.dot_general(wg[s], xb[:m, :], NT, preferred_element_type=F32)
        some(n_move * 3 // 10)
        up = lax.dot_general(wu[s], xb[:m, :], NT, preferred_element_type=F32)
        some(n_move * 6 // 10)
        act = (jax.nn.silu(gate) * up).astype(BF16)
        for c in range(0, n_chunk, 2):
            f = lax.dot_general(act, wd[s, :, c * LANES:(c + 2) * LANES], TN, preferred_element_type=F32)
            yield_at = n_move * 6 // 10 + (n_move - n_move * 6 // 10) * (c + 2) // n_chunk
            for d in range(2):
                fb[pl.ds(f_at + (c + d) * stride, m), :] = f[:, d * LANES:(d + 1) * LANES]
            some(yield_at)

    @pl.when(n_tiles > 0)
    def _():
        def first(g, carry):
            gather8(tile_e[0] * n_tok + tile_r[0], g)
            return carry

        lax.fori_loop(0, (tile_n[0] + 7) // 8, first, 0)

    def tile_step(i, carry):
        e, k, r0, n = tile_e[i], tile_s[i], tile_r[i], tile_n[i]
        s = lax.rem(k, SLOTS)

        @pl.when(r0 == 0)
        def _():
            ahead = k + SLOTS - 1

            @pl.when(ahead < n_active)
            def _():
                for c in weight_copies(active[ahead], lax.rem(ahead, SLOTS)):
                    c.start()

            for c in weight_copies(e, s):
                c.wait()

        f_size = n_chunk * stride
        f_at = pl.multiple_of(lax.rem(i, 2) * f_size, 8)
        f_prev = pl.multiple_of(lax.rem(i + 1, 2) * f_size, 8)
        before, after = jnp.maximum(i - 1, 0), jnp.minimum(i + 1, n_tiles - 1)
        e1 = tile_e[before]
        w1 = e1 * (n_tok + LANES)
        base1 = jnp.where(i > 0, e1 * n_tok + tile_r[before], n_local * n_tok)
        n1 = jnp.where(i > 0, tile_n[before], 0)
        base2 = tile_e[after] * n_tok + tile_r[after]
        n2 = jnp.where(i + 1 < n_tiles, tile_n[after], 0)
        below = 0
        for m in TILES:
            @pl.when((n > below) & (n <= m))
            def _(m=m):
                moves = []
                for g in range(m // 8):
                    moves.append(functools.partial(gather8, base2, g))
                    moves.append(functools.partial(scatter8, f_prev, w1, base1, g))
                ffn(m, s, f_at, moves)

                def more_in(g, c2):
                    gather8(base2, g)
                    return c2

                def more_out(g, c2):
                    scatter8(f_prev, w1, base1, g)
                    return c2

                lax.fori_loop(m // 8, (n2 + 7) // 8, more_in, 0)
                lax.fori_loop(m // 8, (n1 + 7) // 8, more_out, 0)
            below = m

        return carry

    lax.fori_loop(0, n_tiles, tile_step, 0)

    @pl.when(n_tiles > 0)
    def _():
        i = n_tiles - 1
        f_at = pl.multiple_of(lax.rem(i, 2) * (n_chunk * stride), 8)

        def last(g, carry):
            scatter8(f_at, tile_e[i] * (n_tok + LANES), tile_e[i] * n_tok + tile_r[i], g)
            return carry

        lax.fori_loop(0, (tile_n[i] + 7) // 8, last, 0)

    def write_out(b):
        return pltpu.make_async_copy(h_in.at[b], out_hbm.at[pl.ds(b * LANES, LANES), :], out_sem.at[b])

    def finish(b, carry):
        for c in range(n_chunk):
            h_in[b, :, c * LANES:(c + 1) * LANES] = (
                acc[pl.ds(b * LANES * PITCH + c, LANES, stride=PITCH), :].astype(BF16))
        write_out(b).start()
        return carry

    lax.fori_loop(0, n_blocks, finish, 0)
    for b in range(n_blocks):
        write_out(b).wait()


def run_experts(lst, wl, cnt, h, act, sig, shd, wg, wu, wd):
    n_tok, dim = h.shape
    n_local, width, _ = wg.shape
    n_chunk = dim // LANES
    big = TILES[-1]
    max_tiles = n_local * ((n_tok + big - 1) // big)
    hbm = pl.BlockSpec(memory_space=pl.ANY)
    return pl.pallas_call(
        expert_kernel,
        out_shape=jax.ShapeDtypeStruct((n_tok, dim), BF16),
        in_specs=[hbm] * 10,
        out_specs=hbm,
        scratch_shapes=[
            pltpu.SMEM((lst.size,), jnp.int32),
            pltpu.SMEM((wl.size,), F32),
            pltpu.SMEM(cnt.shape, jnp.int32),
            pltpu.VMEM(act.shape, BF16),
            pltpu.VMEM(sig.shape, F32),
            pltpu.VMEM(shd.shape, BF16),
            pltpu.VMEM((n_tok // LANES, LANES, dim), BF16),
            pltpu.VMEM(((n_tok + 1) * PITCH, LANES), F32),
            pltpu.VMEM(((n_tok + 1) * PITCH, LANES), F32),
            pltpu.VMEM((SLOTS, width, dim), BF16),
            pltpu.VMEM((SLOTS, width, dim), BF16),
            pltpu.VMEM((SLOTS, width, dim), BF16),
            pltpu.VMEM((n_chunk * (big + PAD), LANES), F32),
            pltpu.VMEM((big, dim), BF16),
            pltpu.VMEM((2 * n_chunk * (big + PAD), LANES), F32),
            pltpu.SMEM((n_local,), jnp.int32),
            pltpu.SMEM((max_tiles,), jnp.int32),
            pltpu.SMEM((max_tiles,), jnp.int32),
            pltpu.SMEM((max_tiles,), jnp.int32),
            pltpu.SMEM((max_tiles,), jnp.int32),
            pltpu.SemaphoreType.DMA((n_tok // LANES,)),
            pltpu.SemaphoreType.DMA((SLOTS, 3)),
            pltpu.SemaphoreType.DMA((n_tok // LANES,)),
            pltpu.SemaphoreType.DMA((6,)),
        ],
        compiler_params=pltpu.CompilerParams(vmem_limit_bytes=67_000_000),
        name="experts",
    )(lst.reshape(-1), wl.reshape(-1), cnt, h, act, sig, shd, wg, wu, wd)


def reduce_kernel(groups, p_hbm, x_hbm, out_ref, x_ref, last, mate, own, ra, rb, rc, sems):
    x, core, y, n_x, n_y = place()
    rows, dim = x_ref.shape
    part = rows // n_y
    load_x = pltpu.make_async_copy(x_hbm, x_ref, sems[-1])
    s_in, s_d, r_d, s_a, r_a, s_b, r_b, s_c, r_c, s_e, r_e = sems[:-1]

    def at(v, n):
        return lax.rem(v + n, n)

    xs = [at(x + d, n_x) for d in range(4)]
    ys = [at(y + d, n_y) for d in range(4)]
    to_mate = peer(x, 1 - core, y)
    x_peers = [None] + [peer(xs[d], core, y) for d in range(1, 4)]
    y_peers = [None] + [peer(x, core, ys[d]) for d in range(1, 4)]
    mine = pl.ds(pl.multiple_of(y * part, part), part)
    started = []

    def go(c):
        c.start()
        started.append(c)
        return c

    loads, mates = [], []
    for g, (kind, lo, w) in enumerate(groups):
        c = pltpu.make_async_copy(p_hbm.at[:, core, :, lo:lo + w], own[g], s_in.at[g])
        c.start()
        loads.append(c)
    load_x.start()
    meet([to_mate] + x_peers[1:] + y_peers[1:])
    for g, (kind, lo, w) in enumerate(groups):
        mates.append(go(remote(p_hbm.at[:, 1 - core, :, lo:lo + w], mate[g], s_d.at[g], r_d.at[g], to_mate)))

    def unit(g, d, lo, n):
        if groups[g][0] == "x":
            return own[g].at[xs[d], lo:lo + n, :]
        return own[g].at[:, pl.ds(pl.multiple_of(ys[d] * part, part) + lo, n), :]

    def land(g, k, lo, n):
        return rb[g].at[k, lo:lo + n, :] if groups[g][0] == "x" else rb[g].at[k, :, lo:lo + n, :]

    def first_peers(g):
        return x_peers if groups[g][0] == "x" else y_peers

    def half(g):
        return (rows if groups[g][0] == "x" else part) // 2

    a, b_ind, b_dep, c_sent, e_sent = {}, {}, {}, {}, {}

    def add_mate(g):
        loads[g].wait()
        mates[g].wait_recv()
        own[g][...] = (own[g][...].astype(F32) + mate[g][...].astype(F32)).astype(BF16)
        h = half(g)
        for k, (lo, d) in enumerate(((0, 1), (h, 3))):
            a[g, k] = go(remote(unit(g, 2, lo, h), ra[g].at[k], s_a.at[g, k], r_a.at[g, k], first_peers(g)[d]))

    def send_near(g):
        h = half(g)
        for k, (lo, d) in enumerate(((h, 1), (0, 3))):
            b_ind[g, k] = go(remote(unit(g, d, lo, h), land(g, k, lo, h), s_b.at[g, k, 0], r_b.at[g, k, 0],
                                    first_peers(g)[d]))

    def add_far(g):
        h = half(g)
        for k, (lo, d) in enumerate(((0, 1), (h, 3))):
            a[g, k].wait_recv()
            ref = unit(g, d, lo, h)
            ref[...] = (ref[...].astype(F32) + ra[g][k].astype(F32)).astype(BF16)
            b_dep[g, k] = go(remote(ref, land(g, k, lo, h), s_b.at[g, k, 1], r_b.at[g, k, 1], first_peers(g)[d]))

    def second_axis(g):
        for k in range(2):
            b_ind[g, k].wait_recv()
            b_dep[g, k].wait_recv()
        ref = unit(g, 0, 0, 2 * half(g))
        ref[...] = (ref[...].astype(F32) + rb[g][0].astype(F32) + rb[g][1].astype(F32)).astype(BF16)
        for d in (2, 1, 3):
            if groups[g][0] == "x":
                src = own[g].at[x, pl.ds(pl.multiple_of(ys[d] * part, part), part), :]
                where = y_peers[d]
            else:
                src = own[g].at[xs[d], mine, :]
                where = x_peers[d]
            c_sent[g, d] = go(remote(src, rc[g].at[d - 1], s_c.at[g, d - 1], r_c.at[g, d - 1], where))

    def finish(g):
        kind, lo, w = groups[g]
        if g == 0:
            load_x.wait()
        total = own[g][x, mine, :].astype(F32)
        for d in (1, 3, 2):
            c_sent[g, d].wait_recv()
            total = total + rc[g][d - 1].astype(F32)
        cols = slice(lo, lo + w)
        out_ref[mine, cols] = (x_ref[mine, cols].astype(F32) + total).astype(BF16)
        for d in (2, 1, 3):
            ref = out_ref.at[mine, cols]
            e_sent[g, d] = go(remote(ref, ref, s_e.at[g, d - 1], r_e.at[g, d - 1], y_peers[d]))

    def exchange(g):
        for k in range(2):
            b_ind[g, k].wait_recv()
            b_dep[g, k].wait_recv()
        last[y] = (own[g][x].astype(F32) + rb[g][0].astype(F32) + rb[g][1].astype(F32)).astype(BF16)
        for d in (2, 1, 3):
            c_sent[g, d] = go(remote(last.at[y], last.at[y], s_c.at[g, d - 1], r_c.at[g, d - 1], y_peers[d]))

    def close(g):
        _, lo, w = groups[g]
        for d in (1, 3, 2):
            c_sent[g, d].wait_recv()
        total = last[0].astype(F32)
        for k in range(1, 4):
            total = total + last[k].astype(F32)
        out_ref[:, lo:lo + w] = (x_ref[:, lo:lo + w].astype(F32) + total).astype(BF16)

    order = ((add_mate, 0), (send_near, 0), (add_mate, 1), (send_near, 1), (add_mate, 2), (send_near, 2), (add_far, 0),
             (add_far, 1), (add_mate, 3), (add_far, 2), (second_axis, 0), (send_near, 3), (second_axis, 2),
             (add_mate, 4), (second_axis, 1), (add_far, 3), (send_near, 4), (finish, 0), (finish, 2), (add_far, 4),
             (finish, 1), (second_axis, 3), (exchange, 4), (finish, 3), (close, 4))
    for step, g in order:
        step(g)
    for g in range(len(groups) - 1):
        for d in range(1, 4):
            e_sent[g, d].wait_recv()
    for c in started:
        c.wait_send()


def run_reduce(partial, hidden, n_x, n_y):
    rows, dim = hidden.shape
    q = dim // 8
    groups = (("x", 0, q), ("x", q, 2 * q), ("y", 3 * q, 2 * q), ("x", 5 * q, 2 * q), ("x", 7 * q, q))
    n_g = len(groups)
    part = rows // n_y
    dma = pltpu.SemaphoreType.DMA

    def per_group(of):
        return [pltpu.VMEM(of(kind, w), BF16) for kind, _, w in groups]

    def kernel(p, xh, o, xr, last, *rest):
        lists = [rest[k * n_g:(k + 1) * n_g] for k in range(5)]
        reduce_kernel(groups, p, xh, o, xr, last, *lists, rest[5 * n_g:])

    return pl.pallas_call(
        kernel,
        out_shape=jax.ShapeDtypeStruct((rows, dim), BF16),
        in_specs=[pl.BlockSpec(memory_space=pltpu.HBM)] * 2,
        out_specs=pl.BlockSpec(memory_space=pltpu.VMEM),
        scratch_shapes=(
            [pltpu.VMEM((rows, dim), BF16), pltpu.VMEM((n_y, rows, groups[-1][2]), BF16)] +
            per_group(lambda kind, w: (n_x, rows, w)) + per_group(lambda kind, w: (n_x, rows, w))
            + per_group(lambda kind, w: (2, rows // 2, w) if kind == "x" else (2, n_x, part // 2, w))
            + per_group(lambda kind, w: (2, rows, w) if kind == "x" else (2, n_x, part, w))
            + per_group(lambda kind, w: (3, part, w))
            + [dma((n_g,)), dma((n_g,)), dma((n_g,)), dma((n_g, 2)), dma((n_g, 2)), dma((n_g, 2, 2)),
               dma((n_g, 2, 2)), dma((n_g, 3)), dma((n_g, 3)), dma((n_g, 3)), dma((n_g, 3)), dma]),
        compiler_params=pltpu.CompilerParams(collective_id=1, has_side_effects=True, vmem_limit_bytes=60_000_000),
        name="reduce",
    )(partial.reshape(n_x, 2, rows, dim), hidden)


def solution(mesh):
    tok_spec = P(('dp', 'ep'), None)
    in_specs = (tok_spec, tok_spec, P(None), P(None, None), P(None, None),
                P('ep', None, 'tp'), P('ep', None, 'tp'), P('ep', 'tp', None),
                P(None, ('tp', 'ep')), P(None, ('tp', 'ep')), P(('tp', 'ep'), None))
    n_x, n_y = mesh.shape['ep'] // 2, mesh.shape['tp']
    assert n_x == 4 and n_y == 4

    def local_step(hidden_in, topk_idx, norm_gain, router_w, shared_sig_w, exp_gate, exp_up, exp_down,
                   sh_gate, sh_up, sh_down):
        h, act, sig, lst, wl, cnt = run_gather(
            hidden_in, topk_idx.T, norm_gain, router_w.T, shared_sig_w.T, sh_gate.T, sh_up.T,
            exp_gate.shape[0], n_x)
        partial = run_experts(lst, wl, cnt, h, act, sig, sh_down,
                              jnp.swapaxes(exp_gate, 1, 2), jnp.swapaxes(exp_up, 1, 2), exp_down)
        return run_reduce(partial, hidden_in, n_x, n_y)

    return jax.shard_map(local_step, mesh=mesh, in_specs=in_specs, out_specs=tok_spec, check_vma=False)
```

```python
import functools

import jax
import jax.numpy as jnp
from jax import lax
from jax.experimental import pallas as pl
from jax.experimental.pallas import tpu as pltpu
from jax.sharding import PartitionSpec as P

RMS_EPS = 1e-6
LANES = 128
PITCH = 20
PAD = 4
TILES = (64, 256, 320, 384, 512)
SLOTS = 3
F32 = jnp.float32
BF16 = jnp.bfloat16
NT = (((1,), (1,)), ((), ()))
TN = (((0,), (0,)), ((), ()))
MESH = pl.DeviceIdType.MESH


def place():
    ep, y = lax.axis_index("ep"), lax.axis_index("tp")
    return ep // 2, ep % 2, y, lax.axis_size("ep") // 2, lax.axis_size("tp")


def peer(x, core, y):
    return {"ep": 2 * x + core, "tp": y}


def remote(src, dst, send, recv, where):
    return pltpu.make_async_remote_copy(src_ref=src, dst_ref=dst, send_sem=send, recv_sem=recv,
                                        device_id=where, device_id_type=MESH)


def meet(peers):
    barrier = pltpu.get_barrier_semaphore()
    for p in peers:
        pl.semaphore_signal(barrier, inc=1, device_id=p, device_id_type=MESH)
    pl.semaphore_wait(barrier, len(peers))


def token_pair(x, gain, sigw, cols_ref, n_exp, width, up_at):
    xf = x.astype(F32)
    inv = lax.rsqrt(jnp.mean(xf * xf, axis=-1, keepdims=True) + RMS_EPS)
    h = (xf * inv * gain.astype(F32)).astype(BF16)
    sig = jax.nn.sigmoid(jnp.sum(h.astype(F32) * sigw.astype(F32), axis=-1, keepdims=True))
    return h, sig


def pair_dots(h, cols_ref, n_exp, width, up_at):
    out = lax.dot_general(cols_ref[...], h, NT, preferred_element_type=F32)
    logits = out[:n_exp]
    ex = jnp.exp(logits - jnp.max(logits, axis=0, keepdims=True))
    prob = ex / jnp.sum(ex, axis=0, keepdims=True)
    act = (jax.nn.silu(out[n_exp:n_exp + width]) * out[up_at:up_at + width]).astype(BF16)
    return prob, act


def routing_lists(idx_t, first, n_local, lst_ref, cnt_ref):
    n_tok = idx_t.shape[1]
    n_hi = n_tok // LANES
    sub = lax.broadcasted_iota(jnp.int32, (n_local, n_tok), 0)
    member = jnp.zeros((n_local, n_tok), F32)
    for e in range(n_local):
        hit = jnp.sum((idx_t == first + e).astype(F32), axis=0, keepdims=True)
        member = jnp.where(sub == e, hit, member)
    tri = (lax.broadcasted_iota(jnp.int32, (LANES, LANES), 0)
           < lax.broadcasted_iota(jnp.int32, (LANES, LANES), 1)).astype(F32).astype(BF16)
    base = jnp.zeros((n_local, 1), F32)
    parts = []
    for b in range(n_hi):
        m_b = member[:, b * LANES:(b + 1) * LANES]
        parts.append(jnp.dot(m_b.astype(BF16), tri, preferred_element_type=F32) + base)
        base = base + jnp.sum(m_b, axis=-1, keepdims=True)
    pos = jnp.concatenate(parts, axis=1).astype(jnp.int32)
    cnt_ref[...] = jnp.broadcast_to(base, cnt_ref.shape).astype(jnp.int32)
    tok = lax.broadcasted_iota(jnp.int32, (n_hi, n_tok), 1)
    hi_id = lax.broadcasted_iota(jnp.int32, (n_hi, n_tok), 0)
    lo_id = lax.broadcasted_iota(jnp.int32, (LANES, n_tok), 0)
    row_id = (lax.broadcasted_iota(jnp.int32, (n_hi, LANES), 0) * LANES
              + lax.broadcasted_iota(jnp.int32, (n_hi, LANES), 1))
    tok_hi = (tok >> 3).astype(F32)
    tok_lo = (tok & 7).astype(F32)
    for e in range(n_local):
        p_e = pos[e:e + 1, :]
        here = ((p_e >> 7) == hi_id) & (member[e:e + 1, :] > 0.0)
        lo_hot = jnp.where((p_e & (LANES - 1)) == lo_id, 1.0, 0.0).astype(BF16)
        lhs = jnp.concatenate([jnp.where(here, v, 0.0) for v in (tok_hi, tok_lo)], axis=0).astype(BF16)
        got = lax.dot_general(lhs, lo_hot, NT, preferred_element_type=F32)
        t_of = (got[:n_hi] * 8.0 + got[n_hi:]).astype(jnp.int32)
        valid = row_id < base[e:e + 1, :].astype(jnp.int32)
        lst_ref[e * n_hi:(e + 1) * n_hi, :] = jnp.where(valid, t_of, n_tok)


def gather_kernel(n_local, x_hbm, idx_hbm, gain_hbm, rw_hbm, sigw_hbm, shg_hbm, shu_hbm,
                  h_hbm, act_ref, sigv_ref, lst_ref, wl_ref, cnt_ref,
                  tok, idx, cols, gain_ref, sigw_ref, prob, hbuf, in_sem, send, recv, isend, irecv, out_sem):
    x, core, y, n_x, n_y = place()
    n_exp, width = rw_hbm.shape[0], shg_hbm.shape[0]
    up_at = n_exp + (width + 15) // 16 * 16
    rows = x_hbm.shape[0]
    half, piece = rows // 2, rows // 4
    own = 2 * x + core
    load_x = pltpu.make_async_copy(x_hbm, tok.at[own], in_sem.at[0])
    load_i = pltpu.make_async_copy(idx_hbm, idx.at[own], in_sem.at[1])
    load_x.start()
    load_i.start()
    small = [pltpu.make_async_copy(src, dst, in_sem.at[2 + k]) for k, (src, dst) in enumerate((
        (rw_hbm, cols.at[0:n_exp, :]), (shg_hbm, cols.at[n_exp:n_exp + width, :]),
        (shu_hbm, cols.at[up_at:up_at + width, :]), (gain_hbm, gain_ref), (sigw_hbm, sigw_ref)))]

    def at(v, n):
        return lax.rem(v + n, n)

    right, left, far = at(x + 1, n_x), at(x - 1, n_x), at(x + 2, n_x)
    up, down = at(y + 1, n_y), at(y - 1, n_y)
    meet([peer(x, 1 - core, y), peer(right, core, y), peer(left, core, y), peer(x, core, up), peer(x, core, down)])
    load_x.wait()
    load_i.wait()

    started = []
    count = [0]

    def copy(block, row, n_rows, where):
        k = count[0]
        count[0] += 1
        row = pl.multiple_of(row, piece)
        ref = tok.at[block, pl.ds(row, n_rows), :]
        c = remote(ref, ref, send.at[k], recv.at[k], where)
        return c

    def go(c):
        c.start()
        started.append(c)
        return c

    mine = (y % 2) * half
    m = [mine, mine + piece]
    o = [half - mine, half - mine + piece]
    to_right, to_left = peer(right, core, y), peer(left, core, y)
    to_up, to_down, to_mate = peer(x, core, up), peer(x, core, down), peer(x, 1 - core, y)
    icopies = []

    def send_idx(block, where):
        k = len(icopies)
        c = remote(idx.at[block], idx.at[block], isend.at[k], irecv.at[k], where)
        c.start()
        icopies.append(c)
        return c

    i_left, i_right, i_own = send_idx(own, to_right), send_idx(own, to_left), send_idx(own, to_mate)
    from_left, from_right = {}, {}
    for k in range(2):
        from_left[k] = go(copy(own, m[k], piece, to_right))
        from_right[1 - k] = go(copy(own, m[1 - k], piece, to_left))
    s_mate = go(copy(own, 0, rows, to_mate))

    cols[n_exp + width - width % 8:up_at, :] = jnp.zeros((up_at - n_exp - width + width % 8, cols.shape[1]), BF16)
    tail = up_at + width - width % 8
    cols[tail:, :] = jnp.zeros((cols.shape[0] - tail, cols.shape[1]), BF16)
    for c in small:
        c.start()

    outs = []

    def pair(slot, px):
        for c in range(2):
            h, sig = token_pair(tok[2 * px + c], gain_ref[...].astype(F32).reshape(1, -1), sigw_ref[...], cols, n_exp, width, up_at)
            hbuf[slot, c * rows:(c + 1) * rows, :] = h
            sigv_ref[pl.ds(pl.multiple_of((2 * px + c) * rows, rows), rows), :] = sig
        out = pltpu.make_async_copy(hbuf.at[slot], h_hbm.at[pl.ds(pl.multiple_of(2 * px * rows, 2 * rows), 2 * rows), :],
                                    out_sem.at[slot])
        p, a = pair_dots(hbuf[slot], cols, n_exp, width, up_at)
        prob[px] = p
        act_ref[:, pl.ds(pl.multiple_of(px * 2 * rows, 2 * rows), 2 * rows)] = a
        out.start()
        outs.append(out)

    lb, rb, fb = 2 * left + core, 2 * right + core, 2 * far + core
    mate = {name: [] for name in "lrf"}
    along_y, forward = {}, {}

    def relay(name, block, k, arrived, onward=None):
        arrived.wait_recv()
        if onward is not None:
            forward[k] = go(copy(block, m[k], piece, onward))
        along_y[name, k] = go(copy(block, m[k], piece, to_up if k == 0 else to_down))

    def to_the_mate(name, block, row):
        mate[name].append(go(copy(block, row, half, to_mate)))

    def pass_on(name, block):
        for k in range(2):
            along_y[name, k].wait_recv()
        to_the_mate(name, block, o[0])

    def arrived_all(name):
        for c in mate[name]:
            c.wait_recv()

    i_left.wait_recv()
    i_far = send_idx(lb, to_right)
    i_mates = [send_idx(lb, to_mate)]
    i_right.wait_recv()
    i_mates.append(send_idx(rb, to_mate))
    relay("l", lb, 0, from_left[0], to_right)
    relay("r", rb, 1, from_right[1], to_left)
    s_mate.wait_recv()
    for c in small:
        c.wait()
    pair(0, x)
    relay("l", lb, 1, from_left[1])
    relay("r", rb, 0, from_right[0])
    to_the_mate("l", lb, m[0])
    to_the_mate("r", rb, m[0])
    i_far.wait_recv()
    i_mates.append(send_idx(fb, to_mate))
    relay("f", fb, 0, forward[0])
    relay("f", fb, 1, forward[1])
    to_the_mate("f", fb, m[0])
    pass_on("l", lb)
    pass_on("r", rb)
    arrived_all("l")
    pair(1, left)
    pass_on("f", fb)
    arrived_all("r")
    pair(2, right)
    first = pl.multiple_of(own * n_local, n_local)
    lst_rows = 2 * n_x * rows // LANES
    lst_ref[n_local * lst_rows:, :] = jnp.full((lst_ref.shape[0] - n_local * lst_rows, LANES), 2 * n_x * rows, jnp.int32)
    for c in [i_own] + i_mates:
        c.wait_recv()
    routing_lists(jnp.concatenate([idx[b] for b in range(2 * n_x)], axis=1), first, n_local, lst_ref, cnt_ref)
    arrived_all("f")
    pair(3, far)
    n_hi = 2 * n_x * rows // LANES
    wl_ref[...] = jnp.zeros_like(wl_ref)
    for b in range(n_x):
        wt = prob[b, pl.ds(first, n_local), :]
        for e in range(n_local):
            for c in range(2):
                wl_ref[e * (n_hi + 1) + 2 * b + c:e * (n_hi + 1) + 2 * b + c + 1, :] = (
                    wt[e:e + 1, c * LANES:(c + 1) * LANES])
    for c in started + icopies:
        c.wait_send()
    for c in outs:
        c.wait()


def run_gather(hidden, idx_t, gain, rw_t, sig_t, shg_t, shu_t, n_local, n_x):
    rows, dim = hidden.shape
    n_tok = rows * 2 * n_x
    n_hi = n_tok // LANES
    n_exp, width = rw_t.shape[0], shg_t.shape[0]
    pad = (width + 15) // 16 * 16
    n_copy = 4 + 1 + 2 + 6 + 6
    n_idx = 3 + 1 + 3
    vmem = pl.BlockSpec(memory_space=pltpu.VMEM)
    hbm = pl.BlockSpec(memory_space=pl.ANY)
    return pl.pallas_call(
        functools.partial(gather_kernel, n_local),
        out_shape=(jax.ShapeDtypeStruct((n_tok, dim), BF16),
                   jax.ShapeDtypeStruct((width, n_tok), BF16),
                   jax.ShapeDtypeStruct((n_tok, 1), F32),
                   jax.ShapeDtypeStruct(((n_local + 1) * n_hi, LANES), jnp.int32),
                   jax.ShapeDtypeStruct((n_local * (n_hi + 1), LANES), F32),
                   jax.ShapeDtypeStruct((n_local, LANES), jnp.int32)),
        in_specs=[hbm] * 7,
        out_specs=[hbm] + [vmem] * 5,
        scratch_shapes=[
            pltpu.VMEM((2 * n_x, rows, dim), BF16),
            pltpu.VMEM((2 * n_x,) + idx_t.shape, jnp.int32),
            pltpu.VMEM((n_exp + 2 * pad, dim), BF16),
            pltpu.VMEM((dim,), BF16),
            pltpu.VMEM((1, dim), BF16),
            pltpu.VMEM((n_x, n_exp, 2 * rows), F32),
            pltpu.VMEM((n_x, 2 * rows, dim), BF16),
            pltpu.SemaphoreType.DMA((7,)),
            pltpu.SemaphoreType.DMA((n_copy,)),
            pltpu.SemaphoreType.DMA((n_copy,)),
            pltpu.SemaphoreType.DMA((n_idx,)),
            pltpu.SemaphoreType.DMA((n_idx,)),
            pltpu.SemaphoreType.DMA((n_x,)),
        ],
        compiler_params=pltpu.CompilerParams(collective_id=0, has_side_effects=True, vmem_limit_bytes=67_000_000),
        name="gather",
    )(hidden, idx_t, gain, rw_t, sig_t, shg_t, shu_t)


def expert_kernel(lst_hbm, wl_hbm, cnt_hbm, h_hbm, act_hbm, sig_hbm, shd_hbm, wg_hbm, wu_hbm, wd_hbm, out_hbm,
                  lst, wl, cnt, act_ref, sig_ref, shd_ref, h_in, table, acc, wg, wu, wd, xt, xb, fb, active, tile_e, tile_s, tile_r, tile_n,
                  in_sem, w_sem, out_sem, small_sem):
    n_tok, dim = h_hbm.shape
    n_local = wg_hbm.shape[0]
    n_chunk = dim // LANES
    n_blocks = n_tok // LANES
    big = TILES[-1]
    stride = big + PAD

    def fetch_h(b):
        return pltpu.make_async_copy(h_hbm.at[pl.ds(b * LANES, LANES), :], h_in.at[b], in_sem.at[b])

    def weight_copies(e, s):
        return (pltpu.make_async_copy(wg_hbm.at[e], wg.at[s], w_sem.at[s, 0]),
                pltpu.make_async_copy(wu_hbm.at[e], wu.at[s], w_sem.at[s, 1]),
                pltpu.make_async_copy(wd_hbm.at[e], wd.at[s], w_sem.at[s, 2]))

    small = [pltpu.make_async_copy(src, dst, small_sem.at[k]) for k, (src, dst) in enumerate((
        (cnt_hbm, cnt), (lst_hbm, lst), (wl_hbm, wl), (act_hbm, act_ref), (sig_hbm, sig_ref), (shd_hbm, shd_ref)))]
    for c in small:
        c.start()
    for b in range(n_blocks):
        fetch_h(b).start()
    small[0].wait()

    def note(e, carry):
        n, tiles = carry
        total = cnt[e, 0]

        @pl.when(total > 0)
        def _():
            active[n] = e

        def tile(k, t):
            tile_e[t] = e
            tile_s[t] = n
            tile_r[t] = k * big
            tile_n[t] = jnp.minimum(total - k * big, big)
            return t + 1

        return n + jnp.where(total > 0, 1, 0), lax.fori_loop(0, (total + big - 1) // big, tile, tiles)

    n_active, n_tiles = lax.fori_loop(0, n_local, note, (0, 0))
    for s in range(SLOTS - 1):
        @pl.when(s < n_active)
        def _():
            for c in weight_copies(active[s], s):
                c.start()

    acc[n_tok * PITCH:, :] = jnp.zeros((acc.shape[0] - n_tok * PITCH, LANES), F32)
    table[n_tok * PITCH:, :] = jnp.zeros((table.shape[0] - n_tok * PITCH, LANES), F32)

    def shared(b, carry):
        rows = pl.ds(pl.multiple_of(b * LANES, LANES), LANES)
        sig = sig_ref[rows, :]
        for c in range(0, n_chunk, 2):
            sh = sig * lax.dot_general(act_ref[:, rows], shd_ref[:, c * LANES:(c + 2) * LANES], TN,
                                       preferred_element_type=F32)
            for d in range(2):
                acc[pl.ds(b * LANES * PITCH + c + d, LANES, stride=PITCH), :] = sh[:, d * LANES:(d + 1) * LANES]
        return carry

    for c in small[1:]:
        c.wait()
    lax.fori_loop(0, n_blocks, shared, 0)

    def spread(b, carry):
        fetch_h(b).wait()
        for c in range(n_chunk):
            table[pl.ds(b * LANES * PITCH + c, LANES, stride=PITCH), :] = (
                h_in[b, :, c * LANES:(c + 1) * LANES].astype(F32))
        return carry

    lax.fori_loop(0, n_blocks, spread, 0)

    def gather8(base, g):
        for i in range(8):
            row = pl.multiple_of(lst[base + g * 8 + i] * PITCH, 4)
            xt[pl.ds(g * 8 + i, n_chunk, stride=stride), :] = table[pl.ds(row, n_chunk), :]

    def scatter8(f_at, w_at, base, g):
        where, weight, old, new = [], [], [], []
        for i in range(8):
            t = lst[base + g * 8 + i]
            where.append(pl.multiple_of(t * PITCH, 4))
            weight.append(wl[w_at + t])
            old.append(acc[pl.ds(where[i], n_chunk), :])
        for i in range(8):
            new.append(old[i] + weight[i] * fb[pl.ds(f_at + g * 8 + i, n_chunk, stride=stride), :])
        for i in range(8):
            acc[pl.ds(where[i], n_chunk), :] = new[i]

    def ffn(m, s, f_at, moves):
        for c in range(n_chunk):
            xb[:m, c * LANES:(c + 1) * LANES] = xt[c * stride:c * stride + m, :].astype(BF16)
        n_move = len(moves)
        done = 0

        def some(upto):
            nonlocal done
            while done < upto:
                moves[done]()
                done += 1

        gate = lax.dot_general(wg[s], xb[:m, :], NT, preferred_element_type=F32)
        some(n_move * 3 // 10)
        up = lax.dot_general(wu[s], xb[:m, :], NT, preferred_element_type=F32)
        some(n_move * 6 // 10)
        act = (jax.nn.silu(gate) * up).astype(BF16)
        for c in range(0, n_chunk, 2):
            f = lax.dot_general(act, wd[s, :, c * LANES:(c + 2) * LANES], TN, preferred_element_type=F32)
            yield_at = n_move * 6 // 10 + (n_move - n_move * 6 // 10) * (c + 2) // n_chunk
            for d in range(2):
                fb[pl.ds(f_at + (c + d) * stride, m), :] = f[:, d * LANES:(d + 1) * LANES]
            some(yield_at)

    @pl.when(n_tiles > 0)
    def _():
        def first(g, carry):
            gather8(tile_e[0] * n_tok + tile_r[0], g)
            return carry

        lax.fori_loop(0, (tile_n[0] + 7) // 8, first, 0)

    def tile_step(i, carry):
        e, k, r0, n = tile_e[i], tile_s[i], tile_r[i], tile_n[i]
        s = lax.rem(k, SLOTS)

        @pl.when(r0 == 0)
        def _():
            ahead = k + SLOTS - 1

            @pl.when(ahead < n_active)
            def _():
                for c in weight_copies(active[ahead], lax.rem(ahead, SLOTS)):
                    c.start()

            for c in weight_copies(e, s):
                c.wait()

        f_size = n_chunk * stride
        f_at = pl.multiple_of(lax.rem(i, 2) * f_size, 8)
        f_prev = pl.multiple_of(lax.rem(i + 1, 2) * f_size, 8)
        before, after = jnp.maximum(i - 1, 0), jnp.minimum(i + 1, n_tiles - 1)
        e1 = tile_e[before]
        w1 = e1 * (n_tok + LANES)
        base1 = jnp.where(i > 0, e1 * n_tok + tile_r[before], n_local * n_tok)
        n1 = jnp.where(i > 0, tile_n[before], 0)
        base2 = tile_e[after] * n_tok + tile_r[after]
        n2 = jnp.where(i + 1 < n_tiles, tile_n[after], 0)
        below = 0
        for m in TILES:
            @pl.when((n > below) & (n <= m))
            def _(m=m):
                moves = []
                for g in range(m // 8):
                    moves.append(functools.partial(gather8, base2, g))
                    moves.append(functools.partial(scatter8, f_prev, w1, base1, g))
                ffn(m, s, f_at, moves)

                def more_in(g, c2):
                    gather8(base2, g)
                    return c2

                def more_out(g, c2):
                    scatter8(f_prev, w1, base1, g)
                    return c2

                lax.fori_loop(m // 8, (n2 + 7) // 8, more_in, 0)
                lax.fori_loop(m // 8, (n1 + 7) // 8, more_out, 0)
            below = m

        return carry

    lax.fori_loop(0, n_tiles, tile_step, 0)

    @pl.when(n_tiles > 0)
    def _():
        i = n_tiles - 1
        f_at = pl.multiple_of(lax.rem(i, 2) * (n_chunk * stride), 8)

        def last(g, carry):
            scatter8(f_at, tile_e[i] * (n_tok + LANES), tile_e[i] * n_tok + tile_r[i], g)
            return carry

        lax.fori_loop(0, (tile_n[i] + 7) // 8, last, 0)

    def write_out(b):
        return pltpu.make_async_copy(h_in.at[b], out_hbm.at[pl.ds(b * LANES, LANES), :], out_sem.at[b])

    def finish(b, carry):
        for c in range(n_chunk):
            h_in[b, :, c * LANES:(c + 1) * LANES] = (
                acc[pl.ds(b * LANES * PITCH + c, LANES, stride=PITCH), :].astype(BF16))
        write_out(b).start()
        return carry

    lax.fori_loop(0, n_blocks, finish, 0)
    for b in range(n_blocks):
        write_out(b).wait()


def run_experts(lst, wl, cnt, h, act, sig, shd, wg, wu, wd):
    n_tok, dim = h.shape
    n_local, width, _ = wg.shape
    n_chunk = dim // LANES
    big = TILES[-1]
    max_tiles = n_local * ((n_tok + big - 1) // big)
    hbm = pl.BlockSpec(memory_space=pl.ANY)
    return pl.pallas_call(
        expert_kernel,
        out_shape=jax.ShapeDtypeStruct((n_tok, dim), BF16),
        in_specs=[hbm] * 10,
        out_specs=hbm,
        scratch_shapes=[
            pltpu.SMEM((lst.size,), jnp.int32),
            pltpu.SMEM((wl.size,), F32),
            pltpu.SMEM(cnt.shape, jnp.int32),
            pltpu.VMEM(act.shape, BF16),
            pltpu.VMEM(sig.shape, F32),
            pltpu.VMEM(shd.shape, BF16),
            pltpu.VMEM((n_tok // LANES, LANES, dim), BF16),
            pltpu.VMEM(((n_tok + 1) * PITCH, LANES), F32),
            pltpu.VMEM(((n_tok + 1) * PITCH, LANES), F32),
            pltpu.VMEM((SLOTS, width, dim), BF16),
            pltpu.VMEM((SLOTS, width, dim), BF16),
            pltpu.VMEM((SLOTS, width, dim), BF16),
            pltpu.VMEM((n_chunk * (big + PAD), LANES), F32),
            pltpu.VMEM((big, dim), BF16),
            pltpu.VMEM((2 * n_chunk * (big + PAD), LANES), F32),
            pltpu.SMEM((n_local,), jnp.int32),
            pltpu.SMEM((max_tiles,), jnp.int32),
            pltpu.SMEM((max_tiles,), jnp.int32),
            pltpu.SMEM((max_tiles,), jnp.int32),
            pltpu.SMEM((max_tiles,), jnp.int32),
            pltpu.SemaphoreType.DMA((n_tok // LANES,)),
            pltpu.SemaphoreType.DMA((SLOTS, 3)),
            pltpu.SemaphoreType.DMA((n_tok // LANES,)),
            pltpu.SemaphoreType.DMA((6,)),
        ],
        compiler_params=pltpu.CompilerParams(vmem_limit_bytes=67_000_000),
        name="experts",
    )(lst.reshape(-1), wl.reshape(-1), cnt, h, act, sig, shd, wg, wu, wd)


def reduce_kernel(groups, p_hbm, x_hbm, out_ref, x_ref, last, mate, own, ra, rb, rc, sems):
    x, core, y, n_x, n_y = place()
    rows, dim = x_ref.shape
    part = rows // n_y
    load_x = pltpu.make_async_copy(x_hbm, x_ref, sems[-1])
    s_in, s_d, r_d, s_a, r_a, s_b, r_b, s_c, r_c, s_e, r_e = sems[:-1]

    def at(v, n):
        return lax.rem(v + n, n)

    xs = [at(x + d, n_x) for d in range(4)]
    ys = [at(y + d, n_y) for d in range(4)]
    to_mate = peer(x, 1 - core, y)
    x_peers = [None] + [peer(xs[d], core, y) for d in range(1, 4)]
    y_peers = [None] + [peer(x, core, ys[d]) for d in range(1, 4)]
    mine = pl.ds(pl.multiple_of(y * part, part), part)
    started = []

    def go(c):
        c.start()
        started.append(c)
        return c

    loads, mates = [], []
    for g, (kind, lo, w) in enumerate(groups):
        c = pltpu.make_async_copy(p_hbm.at[:, core, :, lo:lo + w], own[g], s_in.at[g])
        c.start()
        loads.append(c)
    load_x.start()
    meet([to_mate] + x_peers[1:] + y_peers[1:])
    for g, (kind, lo, w) in enumerate(groups):
        mates.append(go(remote(p_hbm.at[:, 1 - core, :, lo:lo + w], mate[g], s_d.at[g], r_d.at[g], to_mate)))

    def unit(g, d, lo, n):
        if groups[g][0] == "x":
            return own[g].at[xs[d], lo:lo + n, :]
        return own[g].at[:, pl.ds(pl.multiple_of(ys[d] * part, part) + lo, n), :]

    def land(g, k, lo, n):
        return rb[g].at[k, lo:lo + n, :] if groups[g][0] == "x" else rb[g].at[k, :, lo:lo + n, :]

    def first_peers(g):
        return x_peers if groups[g][0] == "x" else y_peers

    def half(g):
        return (rows if groups[g][0] == "x" else part) // 2

    a, b_ind, b_dep, c_sent, e_sent = {}, {}, {}, {}, {}

    def add_mate(g):
        loads[g].wait()
        mates[g].wait_recv()
        own[g][...] = (own[g][...].astype(F32) + mate[g][...].astype(F32)).astype(BF16)
        h = half(g)
        for k, (lo, d) in enumerate(((0, 1), (h, 3))):
            a[g, k] = go(remote(unit(g, 2, lo, h), ra[g].at[k], s_a.at[g, k], r_a.at[g, k], first_peers(g)[d]))

    def send_near(g):
        h = half(g)
        for k, (lo, d) in enumerate(((h, 1), (0, 3))):
            b_ind[g, k] = go(remote(unit(g, d, lo, h), land(g, k, lo, h), s_b.at[g, k, 0], r_b.at[g, k, 0],
                                    first_peers(g)[d]))

    def add_far(g):
        h = half(g)
        for k, (lo, d) in enumerate(((0, 1), (h, 3))):
            a[g, k].wait_recv()
            ref = unit(g, d, lo, h)
            ref[...] = (ref[...].astype(F32) + ra[g][k].astype(F32)).astype(BF16)
            b_dep[g, k] = go(remote(ref, land(g, k, lo, h), s_b.at[g, k, 1], r_b.at[g, k, 1], first_peers(g)[d]))

    def second_axis(g):
        for k in range(2):
            b_ind[g, k].wait_recv()
            b_dep[g, k].wait_recv()
        ref = unit(g, 0, 0, 2 * half(g))
        ref[...] = (ref[...].astype(F32) + rb[g][0].astype(F32) + rb[g][1].astype(F32)).astype(BF16)
        for d in (2, 1, 3):
            if groups[g][0] == "x":
                src = own[g].at[x, pl.ds(pl.multiple_of(ys[d] * part, part), part), :]
                where = y_peers[d]
            else:
                src = own[g].at[xs[d], mine, :]
                where = x_peers[d]
            c_sent[g, d] = go(remote(src, rc[g].at[d - 1], s_c.at[g, d - 1], r_c.at[g, d - 1], where))

    def finish(g):
        kind, lo, w = groups[g]
        if g == 0:
            load_x.wait()
        total = own[g][x, mine, :].astype(F32)
        for d in (1, 3, 2):
            c_sent[g, d].wait_recv()
            total = total + rc[g][d - 1].astype(F32)
        cols = slice(lo, lo + w)
        out_ref[mine, cols] = (x_ref[mine, cols].astype(F32) + total).astype(BF16)
        for d in (2, 1, 3):
            ref = out_ref.at[mine, cols]
            e_sent[g, d] = go(remote(ref, ref, s_e.at[g, d - 1], r_e.at[g, d - 1], y_peers[d]))

    def exchange(g):
        for k in range(2):
            b_ind[g, k].wait_recv()
            b_dep[g, k].wait_recv()
        last[y] = (own[g][x].astype(F32) + rb[g][0].astype(F32) + rb[g][1].astype(F32)).astype(BF16)
        for d in (2, 1, 3):
            c_sent[g, d] = go(remote(last.at[y], last.at[y], s_c.at[g, d - 1], r_c.at[g, d - 1], y_peers[d]))

    def close(g):
        _, lo, w = groups[g]
        for d in (1, 3, 2):
            c_sent[g, d].wait_recv()
        total = last[0].astype(F32)
        for k in range(1, 4):
            total = total + last[k].astype(F32)
        out_ref[:, lo:lo + w] = (x_ref[:, lo:lo + w].astype(F32) + total).astype(BF16)

    order = ((add_mate, 0), (send_near, 0), (add_mate, 1), (send_near, 1), (add_mate, 2), (add_far, 0), (send_near, 2),
             (add_far, 1), (add_mate, 3), (add_far, 2), (second_axis, 0), (second_axis, 1), (send_near, 3),
             (add_far, 3), (finish, 0), (second_axis, 2), (finish, 1), (exchange, 3), (finish, 2), (close, 3))
    for step, g in order:
        step(g)
    for g in range(len(groups) - 1):
        for d in range(1, 4):
            e_sent[g, d].wait_recv()
    for c in started:
        c.wait_send()


def run_reduce(partial, hidden, n_x, n_y):
    rows, dim = hidden.shape
    q = dim // 8
    groups = (("x", 0, 2 * q), ("y", 2 * q, 2 * q), ("x", 4 * q, 3 * q), ("x", 7 * q, q))
    n_g = len(groups)
    part = rows // n_y
    dma = pltpu.SemaphoreType.DMA

    def per_group(of):
        return [pltpu.VMEM(of(kind, w), BF16) for kind, _, w in groups]

    def kernel(p, xh, o, xr, last, *rest):
        lists = [rest[k * n_g:(k + 1) * n_g] for k in range(5)]
        reduce_kernel(groups, p, xh, o, xr, last, *lists, rest[5 * n_g:])

    return pl.pallas_call(
        kernel,
        out_shape=jax.ShapeDtypeStruct((rows, dim), BF16),
        in_specs=[pl.BlockSpec(memory_space=pltpu.HBM)] * 2,
        out_specs=pl.BlockSpec(memory_space=pltpu.VMEM),
        scratch_shapes=(
            [pltpu.VMEM((rows, dim), BF16), pltpu.VMEM((n_y, rows, groups[-1][2]), BF16)] +
            per_group(lambda kind, w: (n_x, rows, w)) + per_group(lambda kind, w: (n_x, rows, w))
            + per_group(lambda kind, w: (2, rows // 2, w) if kind == "x" else (2, n_x, part // 2, w))
            + per_group(lambda kind, w: (2, rows, w) if kind == "x" else (2, n_x, part, w))
            + per_group(lambda kind, w: (3, part, w))
            + [dma((n_g,)), dma((n_g,)), dma((n_g,)), dma((n_g, 2)), dma((n_g, 2)), dma((n_g, 2, 2)),
               dma((n_g, 2, 2)), dma((n_g, 3)), dma((n_g, 3)), dma((n_g, 3)), dma((n_g, 3)), dma]),
        compiler_params=pltpu.CompilerParams(collective_id=1, has_side_effects=True, vmem_limit_bytes=56_000_000),
        name="reduce",
    )(partial.reshape(n_x, 2, rows, dim), hidden)


def solution(mesh):
    tok_spec = P(('dp', 'ep'), None)
    in_specs = (tok_spec, tok_spec, P(None), P(None, None), P(None, None),
                P('ep', None, 'tp'), P('ep', None, 'tp'), P('ep', 'tp', None),
                P(None, ('tp', 'ep')), P(None, ('tp', 'ep')), P(('tp', 'ep'), None))
    n_x, n_y = mesh.shape['ep'] // 2, mesh.shape['tp']
    assert n_x == 4 and n_y == 4

    def local_step(hidden_in, topk_idx, norm_gain, router_w, shared_sig_w, exp_gate, exp_up, exp_down,
                   sh_gate, sh_up, sh_down):
        h, act, sig, lst, wl, cnt = run_gather(
            hidden_in, topk_idx.T, norm_gain, router_w.T, shared_sig_w.T, sh_gate.T, sh_up.T,
            exp_gate.shape[0], n_x)
        partial = run_experts(lst, wl, cnt, h, act, sig, sh_down,
                              jnp.swapaxes(exp_gate, 1, 2), jnp.swapaxes(exp_up, 1, 2), exp_down)
        return run_reduce(partial, hidden_in, n_x, n_y)

    return jax.shard_map(local_step, mesh=mesh, in_specs=in_specs, out_specs=tok_spec, check_vma=False)
```

```python
import functools

import jax
import jax.numpy as jnp
from jax import lax
from jax.experimental import pallas as pl
from jax.experimental.pallas import tpu as pltpu
from jax.sharding import PartitionSpec as P

RMS_EPS = 1e-6
LANES = 128
PITCH = 20
PAD = 4
TILES = (64, 256, 320, 384, 512)
SLOTS = 3
F32 = jnp.float32
BF16 = jnp.bfloat16
NT = (((1,), (1,)), ((), ()))
TN = (((0,), (0,)), ((), ()))
MESH = pl.DeviceIdType.MESH


def place():
    ep, y = lax.axis_index("ep"), lax.axis_index("tp")
    return ep // 2, ep % 2, y, lax.axis_size("ep") // 2, lax.axis_size("tp")


def peer(x, core, y):
    return {"ep": 2 * x + core, "tp": y}


def remote(src, dst, send, recv, where):
    return pltpu.make_async_remote_copy(src_ref=src, dst_ref=dst, send_sem=send, recv_sem=recv,
                                        device_id=where, device_id_type=MESH)


def meet(peers):
    barrier = pltpu.get_barrier_semaphore()
    for p in peers:
        pl.semaphore_signal(barrier, inc=1, device_id=p, device_id_type=MESH)
    pl.semaphore_wait(barrier, len(peers))


def token_pair(x, gain, sigw, cols_ref, n_exp, width, up_at):
    xf = x.astype(F32)
    inv = lax.rsqrt(jnp.mean(xf * xf, axis=-1, keepdims=True) + RMS_EPS)
    h = (xf * inv * gain.astype(F32)).astype(BF16)
    sig = jax.nn.sigmoid(jnp.sum(h.astype(F32) * sigw.astype(F32), axis=-1, keepdims=True))
    return h, sig


def pair_dots(h, cols_ref, n_exp, width, up_at):
    out = lax.dot_general(cols_ref[...], h, NT, preferred_element_type=F32)
    logits = out[:n_exp]
    ex = jnp.exp(logits - jnp.max(logits, axis=0, keepdims=True))
    prob = ex / jnp.sum(ex, axis=0, keepdims=True)
    act = (jax.nn.silu(out[n_exp:n_exp + width]) * out[up_at:up_at + width]).astype(BF16)
    return prob, act


def routing_lists(idx_t, first, n_local, lst_ref, cnt_ref):
    n_tok = idx_t.shape[1]
    n_hi = n_tok // LANES
    sub = lax.broadcasted_iota(jnp.int32, (n_local, n_tok), 0)
    member = jnp.zeros((n_local, n_tok), F32)
    for e in range(n_local):
        hit = jnp.sum((idx_t == first + e).astype(F32), axis=0, keepdims=True)
        member = jnp.where(sub == e, hit, member)
    tri = (lax.broadcasted_iota(jnp.int32, (LANES, LANES), 0)
           < lax.broadcasted_iota(jnp.int32, (LANES, LANES), 1)).astype(F32).astype(BF16)
    base = jnp.zeros((n_local, 1), F32)
    parts = []
    for b in range(n_hi):
        m_b = member[:, b * LANES:(b + 1) * LANES]
        parts.append(jnp.dot(m_b.astype(BF16), tri, preferred_element_type=F32) + base)
        base = base + jnp.sum(m_b, axis=-1, keepdims=True)
    pos = jnp.concatenate(parts, axis=1).astype(jnp.int32)
    cnt_ref[...] = jnp.broadcast_to(base, cnt_ref.shape).astype(jnp.int32)
    tok = lax.broadcasted_iota(jnp.int32, (n_hi, n_tok), 1)
    hi_id = lax.broadcasted_iota(jnp.int32, (n_hi, n_tok), 0)
    lo_id = lax.broadcasted_iota(jnp.int32, (LANES, n_tok), 0)
    row_id = (lax.broadcasted_iota(jnp.int32, (n_hi, LANES), 0) * LANES
              + lax.broadcasted_iota(jnp.int32, (n_hi, LANES), 1))
    tok_hi = (tok >> 3).astype(F32)
    tok_lo = (tok & 7).astype(F32)
    for e in range(n_local):
        p_e = pos[e:e + 1, :]
        here = ((p_e >> 7) == hi_id) & (member[e:e + 1, :] > 0.0)
        lo_hot = jnp.where((p_e & (LANES - 1)) == lo_id, 1.0, 0.0).astype(BF16)
        lhs = jnp.concatenate([jnp.where(here, v, 0.0) for v in (tok_hi, tok_lo)], axis=0).astype(BF16)
        got = lax.dot_general(lhs, lo_hot, NT, preferred_element_type=F32)
        t_of = (got[:n_hi] * 8.0 + got[n_hi:]).astype(jnp.int32)
        valid = row_id < base[e:e + 1, :].astype(jnp.int32)
        lst_ref[e * n_hi:(e + 1) * n_hi, :] = jnp.where(valid, t_of, n_tok)


def gather_kernel(n_local, x_hbm, idx_hbm, gain_hbm, rw_hbm, sigw_hbm, shg_hbm, shu_hbm,
                  h_hbm, act_ref, sigv_ref, lst_ref, wl_ref, cnt_ref,
                  tok, idx, cols, gain_ref, sigw_ref, prob, hbuf, in_sem, send, recv, isend, irecv, out_sem):
    x, core, y, n_x, n_y = place()
    n_exp, width = rw_hbm.shape[0], shg_hbm.shape[0]
    up_at = n_exp + (width + 15) // 16 * 16
    rows = x_hbm.shape[0]
    half, piece = rows // 2, rows // 4
    own = 2 * x + core
    load_x = pltpu.make_async_copy(x_hbm, tok.at[own], in_sem.at[0])
    load_i = pltpu.make_async_copy(idx_hbm, idx.at[own], in_sem.at[1])
    load_x.start()
    load_i.start()
    small = [pltpu.make_async_copy(src, dst, in_sem.at[2 + k]) for k, (src, dst) in enumerate((
        (rw_hbm, cols.at[0:n_exp, :]), (shg_hbm, cols.at[n_exp:n_exp + width, :]),
        (shu_hbm, cols.at[up_at:up_at + width, :]), (gain_hbm, gain_ref), (sigw_hbm, sigw_ref)))]

    def at(v, n):
        return lax.rem(v + n, n)

    right, left, far = at(x + 1, n_x), at(x - 1, n_x), at(x + 2, n_x)
    up, down = at(y + 1, n_y), at(y - 1, n_y)
    meet([peer(x, 1 - core, y), peer(right, core, y), peer(left, core, y), peer(x, core, up), peer(x, core, down)])
    load_x.wait()
    load_i.wait()

    started = []
    count = [0]

    def copy(block, row, n_rows, where):
        k = count[0]
        count[0] += 1
        row = pl.multiple_of(row, piece)
        ref = tok.at[block, pl.ds(row, n_rows), :]
        c = remote(ref, ref, send.at[k], recv.at[k], where)
        return c

    def go(c):
        c.start()
        started.append(c)
        return c

    mine = (y % 2) * half
    m = [mine, mine + piece]
    o = [half - mine, half - mine + piece]
    to_right, to_left = peer(right, core, y), peer(left, core, y)
    to_up, to_down, to_mate = peer(x, core, up), peer(x, core, down), peer(x, 1 - core, y)
    icopies = []

    def send_idx(block, where):
        k = len(icopies)
        c = remote(idx.at[block], idx.at[block], isend.at[k], irecv.at[k], where)
        c.start()
        icopies.append(c)
        return c

    i_left, i_right, i_own = send_idx(own, to_right), send_idx(own, to_left), send_idx(own, to_mate)
    from_left, from_right = {}, {}
    for k in range(2):
        from_left[k] = go(copy(own, m[k], piece, to_right))
        from_right[1 - k] = go(copy(own, m[1 - k], piece, to_left))
    s_mate = go(copy(own, 0, rows, to_mate))

    cols[n_exp + width - width % 8:up_at, :] = jnp.zeros((up_at - n_exp - width + width % 8, cols.shape[1]), BF16)
    tail = up_at + width - width % 8
    cols[tail:, :] = jnp.zeros((cols.shape[0] - tail, cols.shape[1]), BF16)
    for c in small:
        c.start()

    outs = []

    def pair(slot, px):
        for c in range(2):
            h, sig = token_pair(tok[2 * px + c], gain_ref[...].astype(F32).reshape(1, -1), sigw_ref[...], cols, n_exp, width, up_at)
            hbuf[slot, c * rows:(c + 1) * rows, :] = h
            sigv_ref[pl.ds(pl.multiple_of((2 * px + c) * rows, rows), rows), :] = sig
        out = pltpu.make_async_copy(hbuf.at[slot], h_hbm.at[pl.ds(pl.multiple_of(2 * px * rows, 2 * rows), 2 * rows), :],
                                    out_sem.at[slot])
        p, a = pair_dots(hbuf[slot], cols, n_exp, width, up_at)
        prob[px] = p
        act_ref[:, pl.ds(pl.multiple_of(px * 2 * rows, 2 * rows), 2 * rows)] = a
        out.start()
        outs.append(out)

    lb, rb, fb = 2 * left + core, 2 * right + core, 2 * far + core
    mate = {name: [] for name in "lrf"}
    along_y, forward = {}, {}

    def relay(name, block, k, arrived, onward=None):
        arrived.wait_recv()
        if onward is not None:
            forward[k] = go(copy(block, m[k], piece, onward))
        along_y[name, k] = go(copy(block, m[k], piece, to_up if k == 0 else to_down))

    def to_the_mate(name, block, row):
        mate[name].append(go(copy(block, row, half, to_mate)))

    def pass_on(name, block):
        for k in range(2):
            along_y[name, k].wait_recv()
        to_the_mate(name, block, o[0])

    def arrived_all(name):
        for c in mate[name]:
            c.wait_recv()

    i_left.wait_recv()
    i_far = send_idx(lb, to_right)
    i_mates = [send_idx(lb, to_mate)]
    i_right.wait_recv()
    i_mates.append(send_idx(rb, to_mate))
    relay("l", lb, 0, from_left[0], to_right)
    relay("r", rb, 1, from_right[1], to_left)
    s_mate.wait_recv()
    for c in small:
        c.wait()
    pair(0, x)
    relay("l", lb, 1, from_left[1])
    relay("r", rb, 0, from_right[0])
    to_the_mate("l", lb, m[0])
    to_the_mate("r", rb, m[0])
    i_far.wait_recv()
    i_mates.append(send_idx(fb, to_mate))
    relay("f", fb, 0, forward[0])
    relay("f", fb, 1, forward[1])
    to_the_mate("f", fb, m[0])
    pass_on("l", lb)
    pass_on("r", rb)
    arrived_all("l")
    pair(1, left)
    first = pl.multiple_of(own * n_local, n_local)
    lst_rows = 2 * n_x * rows // LANES
    lst_ref[n_local * lst_rows:, :] = jnp.full((lst_ref.shape[0] - n_local * lst_rows, LANES), 2 * n_x * rows, jnp.int32)
    for c in [i_own] + i_mates:
        c.wait_recv()
    routing_lists(jnp.concatenate([idx[b] for b in range(2 * n_x)], axis=1), first, n_local, lst_ref, cnt_ref)
    pass_on("f", fb)
    arrived_all("r")
    pair(2, right)
    arrived_all("f")
    pair(3, far)
    n_hi = 2 * n_x * rows // LANES
    wl_ref[...] = jnp.zeros_like(wl_ref)
    for b in range(n_x):
        wt = prob[b, pl.ds(first, n_local), :]
        for e in range(n_local):
            for c in range(2):
                wl_ref[e * (n_hi + 1) + 2 * b + c:e * (n_hi + 1) + 2 * b + c + 1, :] = (
                    wt[e:e + 1, c * LANES:(c + 1) * LANES])
    for c in started + icopies:
        c.wait_send()
    for c in outs:
        c.wait()


def run_gather(hidden, idx_t, gain, rw_t, sig_t, shg_t, shu_t, n_local, n_x):
    rows, dim = hidden.shape
    n_tok = rows * 2 * n_x
    n_hi = n_tok // LANES
    n_exp, width = rw_t.shape[0], shg_t.shape[0]
    pad = (width + 15) // 16 * 16
    n_copy = 4 + 1 + 2 + 6 + 6
    n_idx = 3 + 1 + 3
    vmem = pl.BlockSpec(memory_space=pltpu.VMEM)
    hbm = pl.BlockSpec(memory_space=pl.ANY)
    return pl.pallas_call(
        functools.partial(gather_kernel, n_local),
        out_shape=(jax.ShapeDtypeStruct((n_tok, dim), BF16),
                   jax.ShapeDtypeStruct((width, n_tok), BF16),
                   jax.ShapeDtypeStruct((n_tok, 1), F32),
                   jax.ShapeDtypeStruct(((n_local + 1) * n_hi, LANES), jnp.int32),
                   jax.ShapeDtypeStruct((n_local * (n_hi + 1), LANES), F32),
                   jax.ShapeDtypeStruct((n_local, LANES), jnp.int32)),
        in_specs=[hbm] * 7,
        out_specs=[hbm] + [vmem] * 5,
        scratch_shapes=[
            pltpu.VMEM((2 * n_x, rows, dim), BF16),
            pltpu.VMEM((2 * n_x,) + idx_t.shape, jnp.int32),
            pltpu.VMEM((n_exp + 2 * pad, dim), BF16),
            pltpu.VMEM((dim,), BF16),
            pltpu.VMEM((1, dim), BF16),
            pltpu.VMEM((n_x, n_exp, 2 * rows), F32),
            pltpu.VMEM((n_x, 2 * rows, dim), BF16),
            pltpu.SemaphoreType.DMA((7,)),
            pltpu.SemaphoreType.DMA((n_copy,)),
            pltpu.SemaphoreType.DMA((n_copy,)),
            pltpu.SemaphoreType.DMA((n_idx,)),
            pltpu.SemaphoreType.DMA((n_idx,)),
            pltpu.SemaphoreType.DMA((n_x,)),
        ],
        compiler_params=pltpu.CompilerParams(collective_id=0, has_side_effects=True, vmem_limit_bytes=67_000_000),
        name="gather",
    )(hidden, idx_t, gain, rw_t, sig_t, shg_t, shu_t)


def expert_kernel(lst_hbm, wl_hbm, cnt_hbm, h_hbm, act_hbm, sig_hbm, shd_hbm, wg_hbm, wu_hbm, wd_hbm, out_hbm,
                  lst, wl, cnt, act_ref, sig_ref, shd_ref, h_in, table, acc, wg, wu, wd, xt, xb, fb, active, tile_e, tile_s, tile_r, tile_n,
                  in_sem, w_sem, out_sem, small_sem):
    n_tok, dim = h_hbm.shape
    n_local = wg_hbm.shape[0]
    n_chunk = dim // LANES
    n_blocks = n_tok // LANES
    big = TILES[-1]
    stride = big + PAD

    def fetch_h(b):
        return pltpu.make_async_copy(h_hbm.at[pl.ds(b * LANES, LANES), :], h_in.at[b], in_sem.at[b])

    def weight_copies(e, s):
        return (pltpu.make_async_copy(wg_hbm.at[e], wg.at[s], w_sem.at[s, 0]),
                pltpu.make_async_copy(wu_hbm.at[e], wu.at[s], w_sem.at[s, 1]),
                pltpu.make_async_copy(wd_hbm.at[e], wd.at[s], w_sem.at[s, 2]))

    small = [pltpu.make_async_copy(src, dst, small_sem.at[k]) for k, (src, dst) in enumerate((
        (cnt_hbm, cnt), (lst_hbm, lst), (wl_hbm, wl), (act_hbm, act_ref), (sig_hbm, sig_ref), (shd_hbm, shd_ref)))]
    for c in small:
        c.start()
    for b in range(n_blocks):
        fetch_h(b).start()
    small[0].wait()

    def note(e, carry):
        n, tiles = carry
        total = cnt[e, 0]

        @pl.when(total > 0)
        def _():
            active[n] = e

        def tile(k, t):
            tile_e[t] = e
            tile_s[t] = n
            tile_r[t] = k * big
            tile_n[t] = jnp.minimum(total - k * big, big)
            return t + 1

        return n + jnp.where(total > 0, 1, 0), lax.fori_loop(0, (total + big - 1) // big, tile, tiles)

    n_active, n_tiles = lax.fori_loop(0, n_local, note, (0, 0))
    for s in range(SLOTS - 1):
        @pl.when(s < n_active)
        def _():
            for c in weight_copies(active[s], s):
                c.start()

    acc[n_tok * PITCH:, :] = jnp.zeros((acc.shape[0] - n_tok * PITCH, LANES), F32)
    table[n_tok * PITCH:, :] = jnp.zeros((table.shape[0] - n_tok * PITCH, LANES), F32)

    def shared(b, carry):
        rows = pl.ds(pl.multiple_of(b * LANES, LANES), LANES)
        sig = sig_ref[rows, :]
        for c in range(0, n_chunk, 2):
            sh = sig * lax.dot_general(act_ref[:, rows], shd_ref[:, c * LANES:(c + 2) * LANES], TN,
                                       preferred_element_type=F32)
            for d in range(2):
                acc[pl.ds(b * LANES * PITCH + c + d, LANES, stride=PITCH), :] = sh[:, d * LANES:(d + 1) * LANES]
        return carry

    for c in small[1:]:
        c.wait()
    lax.fori_loop(0, n_blocks, shared, 0)

    def spread(b, carry):
        fetch_h(b).wait()
        for c in range(n_chunk):
            table[pl.ds(b * LANES * PITCH + c, LANES, stride=PITCH), :] = (
                h_in[b, :, c * LANES:(c + 1) * LANES].astype(F32))
        return carry

    lax.fori_loop(0, n_blocks, spread, 0)

    def gather8(base, g):
        for i in range(8):
            row = pl.multiple_of(lst[base + g * 8 + i] * PITCH, 4)
            xt[pl.ds(g * 8 + i, n_chunk, stride=stride), :] = table[pl.ds(row, n_chunk), :]

    def scatter8(f_at, w_at, base, g):
        where, weight, old, new = [], [], [], []
        for i in range(8):
            t = lst[base + g * 8 + i]
            where.append(pl.multiple_of(t * PITCH, 4))
            weight.append(wl[w_at + t])
            old.append(acc[pl.ds(where[i], n_chunk), :])
        for i in range(8):
            new.append(old[i] + weight[i] * fb[pl.ds(f_at + g * 8 + i, n_chunk, stride=stride), :])
        for i in range(8):
            acc[pl.ds(where[i], n_chunk), :] = new[i]

    def ffn(m, s, f_at, moves):
        for c in range(n_chunk):
            xb[:m, c * LANES:(c + 1) * LANES] = xt[c * stride:c * stride + m, :].astype(BF16)
        n_move = len(moves)
        done = 0

        def some(upto):
            nonlocal done
            while done < upto:
                moves[done]()
                done += 1

        gate = lax.dot_general(wg[s], xb[:m, :], NT, preferred_element_type=F32)
        some(n_move * 3 // 10)
        up = lax.dot_general(wu[s], xb[:m, :], NT, preferred_element_type=F32)
        some(n_move * 6 // 10)
        act = (jax.nn.silu(gate) * up).astype(BF16)
        for c in range(0, n_chunk, 2):
            f = lax.dot_general(act, wd[s, :, c * LANES:(c + 2) * LANES], TN, preferred_element_type=F32)
            yield_at = n_move * 6 // 10 + (n_move - n_move * 6 // 10) * (c + 2) // n_chunk
            for d in range(2):
                fb[pl.ds(f_at + (c + d) * stride, m), :] = f[:, d * LANES:(d + 1) * LANES]
            some(yield_at)

    @pl.when(n_tiles > 0)
    def _():
        def first(g, carry):
            gather8(tile_e[0] * n_tok + tile_r[0], g)
            return carry

        lax.fori_loop(0, (tile_n[0] + 7) // 8, first, 0)

    def tile_step(i, carry):
        e, k, r0, n = tile_e[i], tile_s[i], tile_r[i], tile_n[i]
        s = lax.rem(k, SLOTS)

        @pl.when(r0 == 0)
        def _():
            ahead = k + SLOTS - 1

            @pl.when(ahead < n_active)
            def _():
                for c in weight_copies(active[ahead], lax.rem(ahead, SLOTS)):
                    c.start()

            for c in weight_copies(e, s):
                c.wait()

        f_size = n_chunk * stride
        f_at = pl.multiple_of(lax.rem(i, 2) * f_size, 8)
        f_prev = pl.multiple_of(lax.rem(i + 1, 2) * f_size, 8)
        before, after = jnp.maximum(i - 1, 0), jnp.minimum(i + 1, n_tiles - 1)
        e1 = tile_e[before]
        w1 = e1 * (n_tok + LANES)
        base1 = jnp.where(i > 0, e1 * n_tok + tile_r[before], n_local * n_tok)
        n1 = jnp.where(i > 0, tile_n[before], 0)
        base2 = tile_e[after] * n_tok + tile_r[after]
        n2 = jnp.where(i + 1 < n_tiles, tile_n[after], 0)
        below = 0
        for m in TILES:
            @pl.when((n > below) & (n <= m))
            def _(m=m):
                moves = []
                for g in range(m // 8):
                    moves.append(functools.partial(gather8, base2, g))
                    moves.append(functools.partial(scatter8, f_prev, w1, base1, g))
                ffn(m, s, f_at, moves)

                def more_in(g, c2):
                    gather8(base2, g)
                    return c2

                def more_out(g, c2):
                    scatter8(f_prev, w1, base1, g)
                    return c2

                lax.fori_loop(m // 8, (n2 + 7) // 8, more_in, 0)
                lax.fori_loop(m // 8, (n1 + 7) // 8, more_out, 0)
            below = m

        return carry

    lax.fori_loop(0, n_tiles, tile_step, 0)

    @pl.when(n_tiles > 0)
    def _():
        i = n_tiles - 1
        f_at = pl.multiple_of(lax.rem(i, 2) * (n_chunk * stride), 8)

        def last(g, carry):
            scatter8(f_at, tile_e[i] * (n_tok + LANES), tile_e[i] * n_tok + tile_r[i], g)
            return carry

        lax.fori_loop(0, (tile_n[i] + 7) // 8, last, 0)

    def write_out(b):
        return pltpu.make_async_copy(h_in.at[b], out_hbm.at[pl.ds(b * LANES, LANES), :], out_sem.at[b])

    def finish(b, carry):
        for c in range(n_chunk):
            h_in[b, :, c * LANES:(c + 1) * LANES] = (
                acc[pl.ds(b * LANES * PITCH + c, LANES, stride=PITCH), :].astype(BF16))
        write_out(b).start()
        return carry

    lax.fori_loop(0, n_blocks, finish, 0)
    for b in range(n_blocks):
        write_out(b).wait()


def run_experts(lst, wl, cnt, h, act, sig, shd, wg, wu, wd):
    n_tok, dim = h.shape
    n_local, width, _ = wg.shape
    n_chunk = dim // LANES
    big = TILES[-1]
    max_tiles = n_local * ((n_tok + big - 1) // big)
    hbm = pl.BlockSpec(memory_space=pl.ANY)
    return pl.pallas_call(
        expert_kernel,
        out_shape=jax.ShapeDtypeStruct((n_tok, dim), BF16),
        in_specs=[hbm] * 10,
        out_specs=hbm,
        scratch_shapes=[
            pltpu.SMEM((lst.size,), jnp.int32),
            pltpu.SMEM((wl.size,), F32),
            pltpu.SMEM(cnt.shape, jnp.int32),
            pltpu.VMEM(act.shape, BF16),
            pltpu.VMEM(sig.shape, F32),
            pltpu.VMEM(shd.shape, BF16),
            pltpu.VMEM((n_tok // LANES, LANES, dim), BF16),
            pltpu.VMEM(((n_tok + 1) * PITCH, LANES), F32),
            pltpu.VMEM(((n_tok + 1) * PITCH, LANES), F32),
            pltpu.VMEM((SLOTS, width, dim), BF16),
            pltpu.VMEM((SLOTS, width, dim), BF16),
            pltpu.VMEM((SLOTS, width, dim), BF16),
            pltpu.VMEM((n_chunk * (big + PAD), LANES), F32),
            pltpu.VMEM((big, dim), BF16),
            pltpu.VMEM((2 * n_chunk * (big + PAD), LANES), F32),
            pltpu.SMEM((n_local,), jnp.int32),
            pltpu.SMEM((max_tiles,), jnp.int32),
            pltpu.SMEM((max_tiles,), jnp.int32),
            pltpu.SMEM((max_tiles,), jnp.int32),
            pltpu.SMEM((max_tiles,), jnp.int32),
            pltpu.SemaphoreType.DMA((n_tok // LANES,)),
            pltpu.SemaphoreType.DMA((SLOTS, 3)),
            pltpu.SemaphoreType.DMA((n_tok // LANES,)),
            pltpu.SemaphoreType.DMA((6,)),
        ],
        compiler_params=pltpu.CompilerParams(vmem_limit_bytes=67_000_000),
        name="experts",
    )(lst.reshape(-1), wl.reshape(-1), cnt, h, act, sig, shd, wg, wu, wd)


def reduce_kernel(groups, p_hbm, x_hbm, out_ref, x_ref, last, mate, own, ra, rb, rc, sems):
    x, core, y, n_x, n_y = place()
    rows, dim = x_ref.shape
    part = rows // n_y
    load_x = pltpu.make_async_copy(x_hbm, x_ref, sems[-1])
    s_in, s_d, r_d, s_a, r_a, s_b, r_b, s_c, r_c, s_e, r_e = sems[:-1]

    def at(v, n):
        return lax.rem(v + n, n)

    xs = [at(x + d, n_x) for d in range(4)]
    ys = [at(y + d, n_y) for d in range(4)]
    to_mate = peer(x, 1 - core, y)
    x_peers = [None] + [peer(xs[d], core, y) for d in range(1, 4)]
    y_peers = [None] + [peer(x, core, ys[d]) for d in range(1, 4)]
    mine = pl.ds(pl.multiple_of(y * part, part), part)
    started = []

    def go(c):
        c.start()
        started.append(c)
        return c

    loads, mates = [], []
    for g, (kind, lo, w) in enumerate(groups):
        c = pltpu.make_async_copy(p_hbm.at[:, core, :, lo:lo + w], own[g], s_in.at[g])
        c.start()
        loads.append(c)
    load_x.start()
    meet([to_mate] + x_peers[1:] + y_peers[1:])
    for g, (kind, lo, w) in enumerate(groups):
        mates.append(go(remote(p_hbm.at[:, 1 - core, :, lo:lo + w], mate[g], s_d.at[g], r_d.at[g], to_mate)))

    def unit(g, d, lo, n):
        if groups[g][0] == "x":
            return own[g].at[xs[d], lo:lo + n, :]
        return own[g].at[:, pl.ds(pl.multiple_of(ys[d] * part, part) + lo, n), :]

    def land(g, k, lo, n):
        return rb[g].at[k, lo:lo + n, :] if groups[g][0] == "x" else rb[g].at[k, :, lo:lo + n, :]

    def first_peers(g):
        return x_peers if groups[g][0] == "x" else y_peers

    def half(g):
        return (rows if groups[g][0] == "x" else part) // 2

    a, b_ind, b_dep, c_sent, e_sent = {}, {}, {}, {}, {}

    def add_mate(g):
        loads[g].wait()
        mates[g].wait_recv()
        own[g][...] = (own[g][...].astype(F32) + mate[g][...].astype(F32)).astype(BF16)
        h = half(g)
        for k, (lo, d) in enumerate(((0, 1), (h, 3))):
            a[g, k] = go(remote(unit(g, 2, lo, h), ra[g].at[k], s_a.at[g, k], r_a.at[g, k], first_peers(g)[d]))

    def send_near(g):
        h = half(g)
        for k, (lo, d) in enumerate(((h, 1), (0, 3))):
            b_ind[g, k] = go(remote(unit(g, d, lo, h), land(g, k, lo, h), s_b.at[g, k, 0], r_b.at[g, k, 0],
                                    first_peers(g)[d]))

    def add_far(g):
        h = half(g)
        for k, (lo, d) in enumerate(((0, 1), (h, 3))):
            a[g, k].wait_recv()
            ref = unit(g, d, lo, h)
            ref[...] = (ref[...].astype(F32) + ra[g][k].astype(F32)).astype(BF16)
            b_dep[g, k] = go(remote(ref, land(g, k, lo, h), s_b.at[g, k, 1], r_b.at[g, k, 1], first_peers(g)[d]))

    def second_axis(g):
        for k in range(2):
            b_ind[g, k].wait_recv()
            b_dep[g, k].wait_recv()
        ref = unit(g, 0, 0, 2 * half(g))
        ref[...] = (ref[...].astype(F32) + rb[g][0].astype(F32) + rb[g][1].astype(F32)).astype(BF16)
        for d in (2, 1, 3):
            if groups[g][0] == "x":
                src = own[g].at[x, pl.ds(pl.multiple_of(ys[d] * part, part), part), :]
                where = y_peers[d]
            else:
                src = own[g].at[xs[d], mine, :]
                where = x_peers[d]
            c_sent[g, d] = go(remote(src, rc[g].at[d - 1], s_c.at[g, d - 1], r_c.at[g, d - 1], where))

    def finish(g):
        kind, lo, w = groups[g]
        if g == 0:
            load_x.wait()
        total = own[g][x, mine, :].astype(F32)
        for d in (1, 3, 2):
            c_sent[g, d].wait_recv()
            total = total + rc[g][d - 1].astype(F32)
        cols = slice(lo, lo + w)
        out_ref[mine, cols] = (x_ref[mine, cols].astype(F32) + total).astype(BF16)
        for d in (2, 1, 3):
            ref = out_ref.at[mine, cols]
            e_sent[g, d] = go(remote(ref, ref, s_e.at[g, d - 1], r_e.at[g, d - 1], y_peers[d]))

    def exchange(g):
        for k in range(2):
            b_ind[g, k].wait_recv()
            b_dep[g, k].wait_recv()
        last[y] = (own[g][x].astype(F32) + rb[g][0].astype(F32) + rb[g][1].astype(F32)).astype(BF16)
        for d in (2, 1, 3):
            c_sent[g, d] = go(remote(last.at[y], last.at[y], s_c.at[g, d - 1], r_c.at[g, d - 1], y_peers[d]))

    def close(g):
        _, lo, w = groups[g]
        for d in (1, 3, 2):
            c_sent[g, d].wait_recv()
        total = last[0].astype(F32)
        for k in range(1, 4):
            total = total + last[k].astype(F32)
        out_ref[:, lo:lo + w] = (x_ref[:, lo:lo + w].astype(F32) + total).astype(BF16)

    order = ((add_mate, 0), (send_near, 0), (add_mate, 1), (send_near, 1), (add_mate, 2), (add_far, 0), (send_near, 2),
             (add_far, 1), (add_mate, 3), (add_far, 2), (second_axis, 0), (second_axis, 1), (send_near, 3),
             (add_far, 3), (finish, 0), (second_axis, 2), (finish, 1), (exchange, 3), (finish, 2), (close, 3))
    for step, g in order:
        step(g)
    for g in range(len(groups) - 1):
        for d in range(1, 4):
            e_sent[g, d].wait_recv()
    for c in started:
        c.wait_send()


def run_reduce(partial, hidden, n_x, n_y):
    rows, dim = hidden.shape
    q = dim // 8
    groups = (("x", 0, 2 * q), ("y", 2 * q, 2 * q), ("x", 4 * q, 3 * q), ("x", 7 * q, q))
    n_g = len(groups)
    part = rows // n_y
    dma = pltpu.SemaphoreType.DMA

    def per_group(of):
        return [pltpu.VMEM(of(kind, w), BF16) for kind, _, w in groups]

    def kernel(p, xh, o, xr, last, *rest):
        lists = [rest[k * n_g:(k + 1) * n_g] for k in range(5)]
        reduce_kernel(groups, p, xh, o, xr, last, *lists, rest[5 * n_g:])

    return pl.pallas_call(
        kernel,
        out_shape=jax.ShapeDtypeStruct((rows, dim), BF16),
        in_specs=[pl.BlockSpec(memory_space=pltpu.HBM)] * 2,
        out_specs=pl.BlockSpec(memory_space=pltpu.VMEM),
        scratch_shapes=(
            [pltpu.VMEM((rows, dim), BF16), pltpu.VMEM((n_y, rows, groups[-1][2]), BF16)] +
            per_group(lambda kind, w: (n_x, rows, w)) + per_group(lambda kind, w: (n_x, rows, w))
            + per_group(lambda kind, w: (2, rows // 2, w) if kind == "x" else (2, n_x, part // 2, w))
            + per_group(lambda kind, w: (2, rows, w) if kind == "x" else (2, n_x, part, w))
            + per_group(lambda kind, w: (3, part, w))
            + [dma((n_g,)), dma((n_g,)), dma((n_g,)), dma((n_g, 2)), dma((n_g, 2)), dma((n_g, 2, 2)),
               dma((n_g, 2, 2)), dma((n_g, 3)), dma((n_g, 3)), dma((n_g, 3)), dma((n_g, 3)), dma]),
        compiler_params=pltpu.CompilerParams(collective_id=1, has_side_effects=True, vmem_limit_bytes=56_000_000),
        name="reduce",
    )(partial.reshape(n_x, 2, rows, dim), hidden)


def solution(mesh):
    tok_spec = P(('dp', 'ep'), None)
    in_specs = (tok_spec, tok_spec, P(None), P(None, None), P(None, None),
                P('ep', None, 'tp'), P('ep', None, 'tp'), P('ep', 'tp', None),
                P(None, ('tp', 'ep')), P(None, ('tp', 'ep')), P(('tp', 'ep'), None))
    n_x, n_y = mesh.shape['ep'] // 2, mesh.shape['tp']
    assert n_x == 4 and n_y == 4

    def local_step(hidden_in, topk_idx, norm_gain, router_w, shared_sig_w, exp_gate, exp_up, exp_down,
                   sh_gate, sh_up, sh_down):
        h, act, sig, lst, wl, cnt = run_gather(
            hidden_in, topk_idx.T, norm_gain, router_w.T, shared_sig_w.T, sh_gate.T, sh_up.T,
            exp_gate.shape[0], n_x)
        partial = run_experts(lst, wl, cnt, h, act, sig, sh_down,
                              jnp.swapaxes(exp_gate, 1, 2), jnp.swapaxes(exp_up, 1, 2), exp_down)
        return run_reduce(partial, hidden_in, n_x, n_y)

    return jax.shard_map(local_step, mesh=mesh, in_specs=in_specs, out_specs=tok_spec, check_vma=False)
```
